32 devices in a mesh: member: 4 (over y, core), lat: 8 (over z, x).
Axes of the slice: x: 2, y: 2, z: 4, core: 2. Of those that a mesh axis runs over, the one named last changes fastest.
Arguments:
- ensemble: float32 [640, 32, 256], P('member', 'lat'), may hold values from -6 to 6
- obs_cell: int32 [32, 128], P(('member', 'lat')), may hold values from 0 to 255
- obs_value: float32 [32, 128], P(('member', 'lat')), may hold values from -8 to 8
- obs_var: float32 [32, 128], P(('member', 'lat')), may hold values from 0.5 to 8
- patch_rows: int32 [32, 2], P(('member', 'lat')), may hold values from 1 to 24, 32 in all within a row
Outputs:
- analysis: float32 [640, 32, 256], P('member', 'lat')
The draws below stay inside these ranges and needn't reach their ends.
Inputs may be any that keep to these rules, and one draw needn't show every extreme that they name: `patch_rows`: each server's 2 patch lengths sum to 32.
All inputs are finite; a program needn't handle non-finite values. Where the reference program divides by a largest or mean magnitude, that divisor is 1e-20 or more.
Results may differ from the reference program's by a relative error of at most 0.0003.
Values sent between devices are 32-bit elements; how exact they have to be, the bound alone decides.
A program may use at most 64 MiB of HBM per device.

```python
import math
import jax
import jax.numpy as jnp
import numpy as np
from jax import lax

K = 640
LON_DEV = 8
OBS_DEV = 128
PATCH_DEV = 2
NS_ITERS = 3
STEPS = 4
NLAT = 32
NLON = 256
DEVICES = 32


def place_ends(drawn, own_key, low, top_value):
    longest = drawn.shape.index(max(drawn.shape))
    spots = []
    for shift in (0, 1):
        where = [jax.random.randint(jax.random.fold_in(own_key, axis), (), 0, length) for axis, length in enumerate(drawn.shape)]
        where[longest] = (where[longest] + shift) % drawn.shape[longest]
        spots.append(tuple(where))
    return drawn.at[spots[0]].set(low).at[spots[1]].set(top_value)


def steps_of(key, extent, shards, smallest, largest):
    level = 1.0
    for position, blocks in shards:
        draws = jax.random.uniform(jax.random.fold_in(jax.random.fold_in(key, 6), position), (blocks,), jnp.float32, smallest / len(shards), largest / len(shards))
        level = level * jnp.repeat(jnp.exp(draws), extent[position] // blocks).reshape((-1,) + (1,) * (len(extent) - 1 - position))
    return level


def profile(count, total, most, skew):
    portions = [(1 << 20) // math.isqrt(grade ** skew) + 1 for grade in range(2, count + 1)]
    rest, counts = total - most - (count - 1), [1] * (count - 1)
    while rest > 0:
        free = [i for i in range(count - 1) if counts[i] < most]
        pool, budget = sum([portions[i] for i in free]), rest
        for i in free:
            more = min(most - counts[i], max(1, budget * portions[i] // pool), rest)
            counts[i] = counts[i] + more
            rest = rest - more
    return np.array([most] + counts)


def ragged_sizes(own_key, amount, total, limit, skew):
    if amount == 2:
        one = jax.random.randint(own_key, (), max(1, total - limit), min(limit, total - 1) + 1)
        return jnp.stack([one, total - one])
    sizes = jnp.asarray(profile(amount, total, limit, skew), jnp.int32)
    twos = (amount - 1) // 2
    source_of, taker = sizes[1:1 + 2 * twos:2], sizes[2:2 + 2 * twos:2]
    slack = jnp.minimum(source_of - 1, limit - taker)
    shifted = jax.random.randint(jax.random.fold_in(own_key, 1), (twos,), 0, 1 << 20) % (slack + 1)
    sizes = sizes.at[1:1 + 2 * twos:2].set(source_of - shifted).at[2:2 + 2 * twos:2].set(taker + shifted)
    return sizes[jax.random.permutation(jax.random.fold_in(own_key, 2), amount)]


def gaussian(rng, shape, scale, limit, cuts=(), kind=jnp.bfloat16):
    values = jax.random.normal(rng, shape, jnp.float32) * scale
    if len(cuts) > 0:
        values = steps_of(rng, shape, cuts, -0.22, 0.18) * values
    return jnp.clip(values, min=-limit, max=limit).astype(kind)


def setup_inputs(seed: int = 0) -> dict:
    key_list = jax.random.split(jax.random.key(seed), 6)
    return {
        "ensemble": gaussian(key_list[0], (K, NLAT, NLON), 1.0, 6.0, ((0, 4), (1, 8)), jnp.float32),
        "obs_cell": place_ends(jax.random.randint(key_list[1], (DEVICES, OBS_DEV), 0, NLAT * LON_DEV), jax.random.fold_in(key_list[1], 1), 0, (NLAT * LON_DEV) - 1).astype(jnp.int32),
        "obs_value": gaussian(key_list[2], (DEVICES, OBS_DEV), 1.5, 8.0, ((0, 32),), jnp.float32),
        "obs_var": jnp.clip(jnp.exp(math.log(8.0) - 2.7725887 * jax.random.uniform(key_list[3], (DEVICES, OBS_DEV), jnp.float32) ** steps_of(key_list[3], (DEVICES, OBS_DEV), ((0, 32),), -0.2, 0.2)), 0.5, 8.0),
        "patch_rows": jax.vmap(lambda own: ragged_sizes(own, PATCH_DEV, NLAT, NLAT - NLAT // 4, 0))(jax.random.split(key_list[4], DEVICES)).reshape((DEVICES, PATCH_DEV)).astype(jnp.int32),
    }


lat_coeff = 0.4
lon_coeff = 0.05
advect_coeff = 0.1

def matmul(left, right):
    return jnp.dot(left, right, precision=lax.Precision.HIGHEST, preferred_element_type=jnp.float32)

def advance(padded):
    centre = padded[:, 1:-1]
    northern = padded[:, :-2]
    southern = padded[:, 2:]
    eastern = jnp.roll(centre, -1, axis=2)
    western = jnp.roll(centre, 1, axis=2)
    return centre + lat_coeff * (northern + southern - 2.0 * centre) + lon_coeff * (eastern + western - 2.0 * centre) - advect_coeff * centre * (eastern - western)

def observe(states, cell_index, values):
    observed = jnp.take(states, cell_index, axis=1)
    obs_mean = lax.optimization_barrier(jnp.mean(observed, axis=0))
    return (observed - obs_mean, values - obs_mean)

def localize(obs_rows, rel_cols, first_row, row_count, lat_scale, width_cols):
    lower = first_row.astype(jnp.float32)
    upper = lower + row_count.astype(jnp.float32) - 1.0
    lat_gap = jnp.maximum(jnp.maximum(lower - obs_rows, obs_rows - upper), 0.0) / lat_scale
    lon_gap = jnp.maximum(jnp.maximum(-rel_cols, rel_cols - (width_cols - 1.0)), 0.0) / width_cols
    return jnp.exp(-lat_gap * lat_gap - lon_gap * lon_gap)

def inverse_root(gram_matrix):
    bound = jnp.max(lax.optimization_barrier(jnp.sum(jnp.abs(gram_matrix), axis=1)))
    identity = jnp.eye(gram_matrix.shape[0], dtype=jnp.float32)
    iterate = gram_matrix / bound
    result = identity
    for turn_index in range(NS_ITERS):
        middle = 1.5 * identity - 0.5 * matmul(result, iterate)
        result = matmul(middle, result)
        if turn_index + 1 < NS_ITERS:
            iterate = matmul(iterate, middle)
    return result / jnp.sqrt(bound)

def analyse(states, spread, obs_meta, lengths, width_cols):
    members = states.shape[0]
    cell_total = states.shape[1]
    lat_total = cell_total // width_cols
    state_mean = lax.optimization_barrier(jnp.mean(states, axis=0))
    anomaly = states - state_mean
    starts = jnp.cumsum(lengths) - lengths
    cell_rows = jnp.arange(cell_total, dtype=jnp.int32) // width_cols
    identity = jnp.eye(members, dtype=jnp.float32)
    result = jnp.broadcast_to(state_mean, states.shape)
    for patch in range(lengths.shape[0]):
        weights = localize(obs_meta[2], obs_meta[3], starts[patch], lengths[patch], lat_total / 4.0, float(width_cols)) / obs_meta[1]
        weighted = spread * weights
        gram_matrix = (members - 1.0) * identity + matmul(weighted, spread.T)
        root = inverse_root(gram_matrix)
        drive = matmul(weighted, obs_meta[0])
        mean_weights = matmul(root, matmul(root, drive))
        transform = jnp.sqrt(members - 1.0) * root + mean_weights[:, None]
        update = matmul(transform.T, anomaly)
        cell_mask = (cell_rows >= starts[patch]) & (cell_rows < starts[patch] + lengths[patch])
        result = result + jnp.where(cell_mask[None, :], update, 0.0)
    return result

def reference(ensemble, obs_cell, obs_value, obs_var, patch_rows):
    fields = ensemble
    for _ in range(STEPS):
        fields = advance(jnp.pad(fields, ((0, 0), (1, 1), (0, 0))))
    servers = NLON // LON_DEV
    strips = fields.reshape(K, NLAT, servers, LON_DEV).transpose(2, 0, 1, 3).reshape(servers, K, NLAT * LON_DEV)

    def prepare(server):
        return observe(strips[server], obs_cell[server], obs_value[server])
    spreads, innovs = lax.map(prepare, jnp.arange(servers, dtype=jnp.int32))
    obs_rows = (obs_cell // LON_DEV).astype(jnp.float32)
    obs_cols = (obs_cell % LON_DEV).astype(jnp.float32)
    offsets = jnp.array([-1.0, 0.0, 1.0], jnp.float32)[:, None] * LON_DEV

    def solve(server):
        beside_all = jnp.stack([(server - 1) % servers, server, (server + 1) % servers]).astype(jnp.int32)
        near_spread = spreads[beside_all].transpose(1, 0, 2).reshape(K, 3 * OBS_DEV)
        obs_meta = jnp.stack([innovs[beside_all].reshape(-1), obs_var[beside_all].reshape(-1), obs_rows[beside_all].reshape(-1), (obs_cols[beside_all] + offsets).reshape(-1)])
        return analyse(strips[server], near_spread, obs_meta, patch_rows[server], LON_DEV)
    analysed = lax.map(solve, jnp.arange(servers, dtype=jnp.int32))
    return analysed.reshape(servers, K, NLAT, LON_DEV).transpose(1, 2, 0, 3).reshape(K, NLAT, NLON)
```

```python
import functools

import jax
import jax.numpy as jnp
from jax import lax
from jax.experimental import pallas as pl
from jax.experimental.pallas import tpu as pltpu
from jax.sharding import PartitionSpec as P

STEPS = 4

lat_coeff = 0.4
lon_coeff = 0.05
advect_coeff = 0.1

MESH = pl.DeviceIdType.MESH
LANES = 128


def with_halo(value, sides, width, wrap):
    for axis, dim in sides:
        size, length = (lax.axis_size(axis), value.shape[dim])
        up = [(i, (i + 1) % size) for i in range(size if wrap else size - 1)]
        down = [(j, i) for i, j in up]
        last = lax.slice_in_dim(value, length - width, length, axis=dim)
        initial = lax.slice_in_dim(value, 0, width, axis=dim)
        before = lax.ppermute(last, axis, up)
        after = lax.ppermute(initial, axis, down)
        value = jnp.concatenate([before, value, after], axis=dim)
    return value


def advance(padded):
    centre = padded[:, 1:-1]
    northern = padded[:, :-2]
    southern = padded[:, 2:]
    eastern = jnp.roll(centre, -1, axis=2)
    western = jnp.roll(centre, 1, axis=2)
    return (
        centre
        + lat_coeff * (northern + southern - 2.0 * centre)
        + lon_coeff * (eastern + western - 2.0 * centre)
        - advect_coeff * centre * (eastern - western)
    )


def localize(obs_rows, rel_cols, first_row, row_count, lat_scale, width_cols):
    lower = first_row.astype(jnp.float32)
    upper = lower + row_count.astype(jnp.float32) - 1.0
    lat_gap = jnp.maximum(jnp.maximum(lower - obs_rows, obs_rows - upper), 0.0) / lat_scale
    lon_gap = jnp.maximum(jnp.maximum(-rel_cols, rel_cols - (width_cols - 1.0)), 0.0) / width_cols
    return jnp.exp(-lat_gap * lat_gap - lon_gap * lon_gap)


def dot3(left, right):
    return jnp.matmul(left, right, precision=lax.Precision.HIGH, preferred_element_type=jnp.float32)


def analyse(anomaly, state_mean, spread, obs_meta, lengths, width_cols):
    cell_total, members = anomaly.shape
    lat_total = cell_total // width_cols
    near = spread.shape[0]
    starts = jnp.cumsum(lengths) - lengths
    cell_rows = jnp.arange(cell_total, dtype=jnp.int32) // width_cols
    identity = jnp.eye(members, dtype=jnp.float32)
    products = dot3(spread, jnp.concatenate([spread, anomaly], axis=0).T)
    common, crossed = products[:, :near], products[:, near:]
    innov = obs_meta[0]
    shrink = jnp.zeros((cell_total,), jnp.float32)
    shift = state_mean
    weights_all = jnp.zeros((near, cell_total), jnp.float32)
    for patch in range(lengths.shape[0]):
        weights = (
            localize(obs_meta[2], obs_meta[3], starts[patch], lengths[patch], lat_total / 4.0, float(width_cols))
            / obs_meta[1]
        )
        scale = jnp.sqrt(weights)
        gram_matrix = (members - 1.0) * identity + jnp.dot(
            (spread * weights[:, None]).T, spread, preferred_element_type=jnp.float32
        )
        bound = jnp.max(jnp.sum(jnp.abs(gram_matrix), axis=1))
        alpha = (members - 1.0) / bound
        x = common * scale[:, None] * (scale / bound)[None, :]
        c0 = 2.25 + alpha * (-2.4375 + alpha * (1.6875 + alpha * (-0.5625 + alpha * 0.0625)))
        c1 = -2.4375 + alpha * (3.375 + alpha * (-1.6875 + alpha * 0.25))
        c2 = 1.6875 + alpha * (-1.6875 + alpha * 0.375)
        c3 = -0.5625 + alpha * 0.25
        c4 = 0.0625
        x2 = dot3(x, x)
        x34 = dot3(x2, jnp.concatenate([x, x2], axis=1))
        x3, x4 = x34[:, :near], x34[:, near:]
        low = c2 * x + c3 * x2 + c4 * x3
        high = c1 * x + c2 * x2 + c3 * x3 + c4 * x4
        block = jnp.concatenate([crossed * scale[:, None], (scale * innov)[:, None]], axis=1)
        both = dot3(jnp.concatenate([low, high], axis=0), block)
        b1 = c1 * block + both[:near]
        b2 = c0 * block + both[near:]
        b3 = c0 * b2 + dot3(high, b2)
        mixed = alpha * c0 * b1 + b3
        got = 1.5 * b1 - 0.5 * (
            alpha * c0 * c0 * b1
            + c0 * mixed
            + dot3(high, mixed)
            + alpha * (c1 * b3 + dot3(low, b3))
        )
        base = c0 * (1.5 - 0.5 * alpha * c0 * c0)
        driven = base * block[:, -1] + jnp.sum(x * got[:, -1][None, :], axis=1)
        again = jnp.sum(x * driven[None, :], axis=1)
        mean_part = (
            jnp.sum(block[:, :-1] * (base * driven)[:, None] + got[:, :-1] * again[:, None], axis=0)
            / bound
        )
        cell_mask = (cell_rows >= starts[patch]) & (cell_rows < starts[patch] + lengths[patch])
        root_scale = jnp.sqrt((members - 1.0) / bound)
        shift = shift + jnp.where(cell_mask, mean_part, 0.0)
        shrink = jnp.where(cell_mask, root_scale * base, shrink)
        weights_all = jnp.where(
            cell_mask[None, :], got[:, :-1] * (scale * (root_scale / bound))[:, None], weights_all
        )
    return shift[:, None] + shrink[:, None] * anomaly + dot3(weights_all.T, spread)


def general_device(ensemble, obs_cell, obs_value, obs_var, patch_rows):
    members_dev, lat_rows, lon_cells = ensemble.shape
    lat_count = lax.axis_size("lat")
    member_count = lax.axis_size("member")
    servers = lat_count * member_count
    width_cols = lon_cells // servers
    padded = with_halo(ensemble, (("lat", 1),), STEPS, False)
    global_rows = (
        lax.axis_index("lat") * lat_rows + jnp.arange(lat_rows + 2 * STEPS, dtype=jnp.int32) - STEPS
    )
    inside = ((global_rows >= 0) & (global_rows < lat_rows * lat_count)).astype(jnp.float32)
    for step_index in range(STEPS):
        padded = advance(padded)
        keeper = inside[step_index + 1 : inside.shape[0] - step_index - 1]
        padded = padded * keeper[None, :, None]
    blocks = padded.reshape(1, members_dev, lat_rows, lon_cells)
    received = lax.all_to_all(blocks, ("member", "lat"), split_axis=3, concat_axis=0, tiled=True)
    strip = received.reshape(member_count, lat_count, members_dev, lat_rows, width_cols)
    members = member_count * members_dev
    lat_total = lat_count * lat_rows
    states = strip.transpose(1, 3, 4, 0, 2).reshape(lat_total * width_cols, members)
    cell_index = obs_cell[0]
    obs_count = cell_index.shape[0]
    state_mean = jnp.mean(states, axis=1)
    anomaly = states - state_mean[:, None]
    spread = jnp.take(anomaly, cell_index, axis=0)
    innov = obs_value[0] - jnp.take(state_mean, cell_index)
    obs_meta = jnp.stack(
        [
            innov,
            obs_var[0],
            (cell_index // width_cols).astype(jnp.float32),
            (cell_index % width_cols).astype(jnp.float32),
        ]
    )
    near_spread = with_halo(spread, ((("member", "lat"), 0),), obs_count, True)
    near_meta = with_halo(obs_meta, ((("member", "lat"), 1),), obs_count, True)
    shifts = jnp.repeat(jnp.array([-1.0, 0.0, 1.0], jnp.float32), obs_count) * width_cols
    near_meta = jnp.concatenate([near_meta[:3], (near_meta[3] + shifts)[None, :]], axis=0)
    analysed = analyse(anomaly, state_mean, near_spread, near_meta, patch_rows[0], width_cols)
    outgoing = analysed.reshape(lat_count, lat_rows, width_cols, member_count, members_dev)
    outgoing = outgoing.transpose(3, 0, 4, 1, 2).reshape(servers, members_dev, lat_rows, width_cols)
    returned = lax.all_to_all(outgoing, ("member", "lat"), split_axis=0, concat_axis=3, tiled=True)
    return returned.reshape(members_dev, lat_rows, lon_cells)


def place(block, lats):
    half = block // (lats // 2)
    return (1 - half) * (2 * block) + half * (2 * lats - 1 - 2 * block)


def block_at(lat, lats):
    odd = lat % 2
    return (1 - odd) * (lat // 2) + odd * (lats - 1 - lat // 2)


def member_of(block, q, members):
    odd = block % 2
    return (1 - odd) * q + odd * (members - 1 - q)


def strip_at(m, lat, lats, members):
    block = block_at(lat, lats)
    return block * members + member_of(block, m, members)


def home_of(strip, lats, members):
    block = strip // members
    return member_of(block, strip % members, members), place(block, lats)


def greet_all(lats, members):
    m, lat = lax.axis_index("member"), lax.axis_index("lat")
    barrier = pltpu.get_barrier_semaphore()
    for dm in range(members):
        for dl in range(lats):
            if dm == 0 and dl == 0:
                continue
            pl.semaphore_signal(
                barrier, inc=1, device_id=((m + dm) % members, (lat + dl) % lats), device_id_type=MESH
            )
    return barrier, lats * members - 1


def forecast(load, lats, rows, groups):
    fields = [load(l) for l in range(lats)]
    lane = lax.broadcasted_iota(jnp.int32, fields[0].shape, 1)
    first, last = lane < groups, lane >= LANES - groups
    count = fields[0].shape[0]
    zero = jnp.zeros_like(fields[0])
    for _ in range(STEPS):
        new = []
        for l in range(lats):
            c = fields[l]
            above = fields[l - 1] if l > 0 else zero
            below = fields[l + 1] if l + 1 < lats else zero
            north = pltpu.roll(jnp.where(last, above, c), groups, 1)
            south = pltpu.roll(jnp.where(first, below, c), LANES - groups, 1)
            east = pltpu.roll(c, count - 1, 0)
            west = pltpu.roll(c, 1, 0)
            new.append(
                c
                + lat_coeff * (north + south - 2.0 * c)
                + lon_coeff * (east + west - 2.0 * c)
                - advect_coeff * c * (east - west)
            )
        fields = new
    return fields


def forward_kernel(
    dims, x_ref, obs_ref, at_ref, mean_ref, yt_ref, meta_ref,
    s_buf, ra, f_buf, r_buf, obs_buf, a_send, a_recv, b_send, b_recv, o_send, o_recv, y_send, y_recv,
):
    lats, members, chunks, rows, width, group = dims
    cols = width * members
    m, lat = lax.axis_index("member"), lax.axis_index("lat")
    barrier, partners = greet_all(lats, members)
    edge = STEPS

    for kc in range(chunks):
        whole = jnp.concatenate([x_ref[kc * group : (kc + 1) * group, r, :] for r in range(rows)], axis=0)
        turned = whole.T
        lon = turned.shape[0]
        for b in range(lats):
            s_buf[kc, b, 0:cols] = turned[b * cols : (b + 1) * cols]
            east, west = ((b + 1) * cols) % lon, (b * cols - edge) % lon
            s_buf[kc, b, cols : cols + edge] = turned[east : east + edge]
            s_buf[kc, b, cols + edge : cols + 2 * edge] = turned[west : west + edge]

    pl.semaphore_wait(barrier, partners)

    target_m, target_l = home_of(m * lats + lat, lats, members)
    away = jnp.logical_or(target_m != m, target_l != lat)
    obs_copy = pltpu.make_async_remote_copy(
        src_ref=obs_ref, dst_ref=obs_buf, send_sem=o_send, recv_sem=o_recv,
        device_id=(target_m, target_l), device_id_type=MESH,
    )

    @pl.when(away)
    def _():
        obs_copy.start()

    @pl.when(jnp.logical_not(away))
    def _():
        obs_buf[...] = obs_ref[...]

    a_copies = []
    for kc in range(chunks):
        for d in range(1, lats):
            to = (lat + d) % lats
            copy = pltpu.make_async_remote_copy(
                src_ref=s_buf.at[kc, block_at(to, lats)], dst_ref=ra.at[kc, lat],
                send_sem=a_send.at[kc, d], recv_sem=a_recv.at[kc, d],
                device_id=(m, to), device_id_type=MESH,
            )
            copy.start()
            a_copies.append(copy)

    own = block_at(lat, lats)
    own_odd = own % 2
    b_copies = []
    for kc in range(chunks):
        ra[kc, lat] = s_buf[kc, own]
        for copy in a_copies[kc * (lats - 1) : (kc + 1) * (lats - 1)]:
            copy.wait_recv()
        fields = forecast(lambda l, kc=kc: ra[kc, l], lats, rows, group)
        for l in range(lats):
            for q in range(members):
                f_buf[kc, q, l] = fields[l][q * width : (q + 1) * width]
        for d in range(1, members):
            to = (m + d) % members
            copy = pltpu.make_async_remote_copy(
                src_ref=f_buf.at[kc, member_of(own, to, members)], dst_ref=r_buf.at[m, kc],
                send_sem=b_send.at[kc, d], recv_sem=b_recv.at[kc, d],
                device_id=(to, lat), device_id_type=MESH,
            )
            copy.start()
            b_copies.append(copy)
        r_buf[m, kc] = f_buf[kc, member_of(own, m, members)]

    @pl.when(away)
    def _():
        obs_copy.wait_recv()

    for copy in b_copies:
        copy.wait_recv()

    per = LANES // group
    lane_block = lax.broadcasted_iota(jnp.int32, (lats * width, LANES), 1) // group
    total = members * chunks // per
    for g in range(total):
        parts = []
        for j in range(per):
            c = g * per + j
            parts.append(r_buf[c // chunks, c % chunks].reshape(lats * width, LANES))
        for r in range(rows):
            out = None
            for j in range(per):
                shift = (group * (j - r)) % LANES
                piece = pltpu.roll(parts[j], shift, 1) if shift else parts[j]
                out = piece if out is None else jnp.where(lane_block == j, piece, out)
            for l in range(lats):
                at_ref[(l * rows + r) * width : (l * rows + r + 1) * width, g * LANES : (g + 1) * LANES] = out[
                    l * width : (l + 1) * width
                ]
    states = at_ref[...]
    cells, count = states.shape
    mean = jnp.sum(states, axis=1, keepdims=True) * (1.0 / count)
    anomaly = states - mean
    at_ref[...] = anomaly
    mean_ref[...] = jnp.broadcast_to(mean, mean_ref.shape)

    nobs = obs_buf.shape[1]
    eye = (
        lax.broadcasted_iota(jnp.int32, (nobs, nobs), 0) == lax.broadcasted_iota(jnp.int32, (nobs, nobs), 1)
    ).astype(jnp.float32)
    cell_col = jnp.sum(eye * obs_buf[0:1, :], axis=1, keepdims=True)
    onehot = (
        cell_col == lax.broadcasted_iota(jnp.int32, (nobs, cells), 1).astype(jnp.float32)
    ).astype(jnp.float32)
    spread = jnp.dot(onehot, anomaly, precision=lax.Precision.HIGHEST, preferred_element_type=jnp.float32)
    hit = jnp.sum(
        (lax.broadcasted_iota(jnp.int32, (cells, nobs), 0).astype(jnp.float32) == obs_buf[0:1, :]).astype(jnp.float32)
        * mean,
        axis=0,
        keepdims=True,
    )
    cell_row = obs_buf[0:1, :]
    row = jnp.floor(cell_row * (1.0 / width))
    yt_ref[1] = spread
    meta_ref[1, 0:1, :] = obs_buf[1:2, :] - hit
    meta_ref[1, 1:2, :] = obs_buf[2:3, :]
    meta_ref[1, 2:3, :] = row
    meta_ref[1, 3:4, :] = cell_row - width * row
    meta_ref[1, 4:5, :] = obs_buf[3:4, :]
    meta_ref[1, 5:8, :] = jnp.zeros((3, nobs), jnp.float32)

    strip = strip_at(m, lat, lats, members)
    count_strips = lats * members
    y_copies = []
    for side, slot in ((1, 0), (count_strips - 1, 2)):
        to_m, to_l = home_of((strip + side) % count_strips, lats, members)
        for i, ref in enumerate((yt_ref, meta_ref)):
            copy = pltpu.make_async_remote_copy(
                src_ref=ref.at[1], dst_ref=ref.at[slot],
                send_sem=y_send.at[slot, i], recv_sem=y_recv.at[slot, i],
                device_id=(to_m, to_l), device_id_type=MESH,
            )
            copy.start()
            y_copies.append(copy)
    for copy in y_copies:
        copy.wait_recv()

    for copy in a_copies + b_copies + y_copies:
        copy.wait_send()

    @pl.when(away)
    def _():
        obs_copy.wait_send()


def forward(ensemble, obs, dims):
    lats, members, chunks, rows, width, group = dims
    cells, total = lats * rows * width, members * chunks * group
    nobs = obs.shape[1]
    dma = pltpu.SemaphoreType.DMA
    vmem = pl.BlockSpec(memory_space=pltpu.VMEM)
    f32 = jnp.float32
    return pl.pallas_call(
        functools.partial(forward_kernel, dims),
        out_shape=(
            jax.ShapeDtypeStruct((cells, total), f32),
            jax.ShapeDtypeStruct((cells, LANES), f32),
            jax.ShapeDtypeStruct((3, nobs, total), f32),
            jax.ShapeDtypeStruct((3, 8, nobs), f32),
        ),
        in_specs=[vmem, vmem],
        out_specs=[vmem] * 4,
        scratch_shapes=[
            pltpu.VMEM((chunks, lats, members * width + 2 * STEPS, LANES), f32),
            pltpu.VMEM((chunks, lats, members * width + 2 * STEPS, LANES), f32),
            pltpu.VMEM((chunks, members, lats, width, LANES), f32),
            pltpu.VMEM((members, chunks, lats, width, LANES), f32),
            pltpu.VMEM((8, nobs), f32),
            dma((chunks, lats)),
            dma((chunks, lats)),
            dma((chunks, members)),
            dma((chunks, members)),
            dma,
            dma,
            dma((3, 2)),
            dma((3, 2)),
        ],
        compiler_params=pltpu.CompilerParams(
            collective_id=0, has_side_effects=True, vmem_limit_bytes=48 * 1024 * 1024
        ),
        name="forward",
    )(ensemble, obs)


def backward_kernel(dims, y_ref, z_ref, t_buf, send, recv):
    lats, members, chunks, rows, width, group = dims
    m, lat = lax.axis_index("member"), lax.axis_index("lat")
    barrier, partners = greet_all(lats, members)
    per = LANES // group
    lane_block = lax.broadcasted_iota(jnp.int32, (lats * width, LANES), 1) // group
    for g in range(members * chunks // per):
        parts = []
        for r in range(rows):
            parts.append(
                jnp.concatenate(
                    [
                        y_ref[(l * rows + r) * width : (l * rows + r + 1) * width, g * LANES : (g + 1) * LANES]
                        for l in range(lats)
                    ],
                    axis=0,
                )
            )
        for j in range(per):
            c = g * per + j
            out = None
            for r in range(rows):
                shift = (group * (r - j)) % LANES
                piece = pltpu.roll(parts[r], shift, 1) if shift else parts[r]
                out = piece if out is None else jnp.where(lane_block == r, piece, out)
            for l in range(lats):
                t_buf[c // chunks, l, c % chunks] = out[l * width : (l + 1) * width]
    pl.semaphore_wait(barrier, partners)
    strip = strip_at(m, lat, lats, members)
    copies = []
    for dl in range(lats):
        for dm in range(members):
            if dm == 0 and dl == 0:
                continue
            to_m, to_l = (m + dm) % members, (lat + dl) % lats
            copy = pltpu.make_async_remote_copy(
                src_ref=t_buf.at[to_m, to_l], dst_ref=z_ref.at[strip],
                send_sem=send.at[dl, dm], recv_sem=recv.at[dl, dm],
                device_id=(to_m, to_l), device_id_type=MESH,
            )
            copy.start()
            copies.append(copy)
    z_ref[strip] = t_buf[m, lat]
    for copy in copies:
        copy.wait()


def backward(analysed, dims):
    lats, members, chunks, rows, width, group = dims
    dma = pltpu.SemaphoreType.DMA
    vmem = pl.BlockSpec(memory_space=pltpu.VMEM)
    f32 = jnp.float32
    return pl.pallas_call(
        functools.partial(backward_kernel, dims),
        out_shape=jax.ShapeDtypeStruct((lats * members, chunks, width, LANES), f32),
        in_specs=[vmem],
        out_specs=vmem,
        scratch_shapes=[
            pltpu.VMEM((members, lats, chunks, width, LANES), f32),
            dma((lats, members)),
            dma((lats, members)),
        ],
        compiler_params=pltpu.CompilerParams(
            collective_id=1, has_side_effects=True, vmem_limit_bytes=48 * 1024 * 1024
        ),
        name="backward",
    )(analysed)


def kernel_device(dims, ensemble, obs_cell, obs_value, obs_var, patch_rows):
    lats, members, chunks, rows, width, group = dims
    nobs = obs_cell.shape[1]
    obs = jnp.concatenate(
        [
            obs_cell.astype(jnp.float32),
            obs_value,
            obs_var,
            jnp.pad(patch_rows.astype(jnp.float32), ((0, 0), (0, nobs - patch_rows.shape[1]))),
            jnp.zeros((4, nobs), jnp.float32),
        ],
        axis=0,
    )
    anomaly, mean, spread, meta = forward(ensemble, obs, dims)
    lengths = meta[1, 4, : patch_rows.shape[1]].astype(jnp.int32)
    shifts = jnp.repeat(jnp.array([-1.0, 0.0, 1.0], jnp.float32), nobs) * width
    flat = meta[:, :4].transpose(1, 0, 2).reshape(4, 3 * nobs)
    near_meta = jnp.concatenate([flat[:3], (flat[3] + shifts)[None, :]], axis=0)
    near_spread = spread.reshape(3 * nobs, spread.shape[2])
    analysed = analyse(anomaly, mean[:, 0], near_spread, near_meta, lengths, width)
    pieces = backward(analysed, dims)
    strips = lats * members
    return (
        pieces.reshape(strips, chunks, width, rows, group)
        .transpose(1, 4, 3, 0, 2)
        .reshape(chunks * group, rows, strips * width)
    )


def kernel_dims(mesh, ensemble, obs_cell, patch_rows):
    lats, members = mesh.shape["lat"], mesh.shape["member"]
    total, lat_all, lon = ensemble.shape
    own, rows = total // members, lat_all // lats
    width = lon // (lats * members)
    if LANES % rows:
        return None
    group = LANES // rows
    fits = (
        own % group == 0
        and (members * (own // group)) % rows == 0
        and width == 8
        and lats % 2 == 0
        and members % 2 == 0
        and obs_cell.shape[1] % LANES == 0
        and patch_rows.shape[1] == 2
    )
    return (lats, members, own // group, rows, width, group) if fits else None


def solution(mesh):
    specs = (P("member", "lat", None),) + (P(("member", "lat"), None),) * 4

    def run(ensemble, obs_cell, obs_value, obs_var, patch_rows):
        dims = kernel_dims(mesh, ensemble, obs_cell, patch_rows)
        body = general_device if dims is None else functools.partial(kernel_device, dims)
        mapped = jax.shard_map(
            body, mesh=mesh, in_specs=specs, out_specs=P("member", "lat", None), check_vma=False
        )
        return mapped(ensemble, obs_cell, obs_value, obs_var, patch_rows)

    return run
```

```python
import functools

import jax
import jax.numpy as jnp
from jax import lax
from jax.experimental import pallas as pl
from jax.experimental.pallas import tpu as pltpu
from jax.sharding import PartitionSpec as P

STEPS = 4

lat_coeff = 0.4
lon_coeff = 0.05
advect_coeff = 0.1

MESH = pl.DeviceIdType.MESH
LANES = 128


def with_halo(value, sides, width, wrap):
    for axis, dim in sides:
        size, length = (lax.axis_size(axis), value.shape[dim])
        up = [(i, (i + 1) % size) for i in range(size if wrap else size - 1)]
        down = [(j, i) for i, j in up]
        last = lax.slice_in_dim(value, length - width, length, axis=dim)
        initial = lax.slice_in_dim(value, 0, width, axis=dim)
        before = lax.ppermute(last, axis, up)
        after = lax.ppermute(initial, axis, down)
        value = jnp.concatenate([before, value, after], axis=dim)
    return value


def advance(padded):
    centre = padded[:, 1:-1]
    northern = padded[:, :-2]
    southern = padded[:, 2:]
    eastern = jnp.roll(centre, -1, axis=2)
    western = jnp.roll(centre, 1, axis=2)
    return (
        centre
        + lat_coeff * (northern + southern - 2.0 * centre)
        + lon_coeff * (eastern + western - 2.0 * centre)
        - advect_coeff * centre * (eastern - western)
    )


def localize(obs_rows, rel_cols, first_row, row_count, lat_scale, width_cols):
    lower = first_row.astype(jnp.float32)
    upper = lower + row_count.astype(jnp.float32) - 1.0
    lat_gap = jnp.maximum(jnp.maximum(lower - obs_rows, obs_rows - upper), 0.0) / lat_scale
    lon_gap = jnp.maximum(jnp.maximum(-rel_cols, rel_cols - (width_cols - 1.0)), 0.0) / width_cols
    return jnp.exp(-lat_gap * lat_gap - lon_gap * lon_gap)


def dot3(left, right):
    return jnp.matmul(left, right, precision=lax.Precision.HIGH, preferred_element_type=jnp.float32)


def analyse(anomaly, state_mean, spread, obs_meta, lengths, width_cols):
    cell_total, members = anomaly.shape
    lat_total = cell_total // width_cols
    near = spread.shape[0]
    starts = jnp.cumsum(lengths) - lengths
    cell_rows = jnp.arange(cell_total, dtype=jnp.int32) // width_cols
    identity = jnp.eye(members, dtype=jnp.float32)
    products = dot3(spread, jnp.concatenate([spread, anomaly], axis=0).T)
    common, crossed = products[:, :near], products[:, near:]
    innov = obs_meta[0]
    shrink = jnp.zeros((cell_total,), jnp.float32)
    shift = state_mean
    weights_all = jnp.zeros((near, cell_total), jnp.float32)
    for patch in range(lengths.shape[0]):
        weights = (
            localize(obs_meta[2], obs_meta[3], starts[patch], lengths[patch], lat_total / 4.0, float(width_cols))
            / obs_meta[1]
        )
        scale = jnp.sqrt(weights)
        gram_matrix = (members - 1.0) * identity + jnp.dot(
            (spread * weights[:, None]).T, spread, preferred_element_type=jnp.float32
        )
        bound = jnp.max(jnp.sum(jnp.abs(gram_matrix), axis=1))
        alpha = (members - 1.0) / bound
        x = common * scale[:, None] * (scale / bound)[None, :]
        c0 = 2.25 + alpha * (-2.4375 + alpha * (1.6875 + alpha * (-0.5625 + alpha * 0.0625)))
        c1 = -2.4375 + alpha * (3.375 + alpha * (-1.6875 + alpha * 0.25))
        c2 = 1.6875 + alpha * (-1.6875 + alpha * 0.375)
        c3 = -0.5625 + alpha * 0.25
        c4 = 0.0625
        x2 = dot3(x, x)
        x34 = dot3(x2, jnp.concatenate([x, x2], axis=1))
        x3, x4 = x34[:, :near], x34[:, near:]
        low = c2 * x + c3 * x2 + c4 * x3
        high = c1 * x + c2 * x2 + c3 * x3 + c4 * x4
        block = jnp.concatenate([crossed * scale[:, None], (scale * innov)[:, None]], axis=1)
        both = dot3(jnp.concatenate([low, high], axis=0), block)
        b1 = c1 * block + both[:near]
        b2 = c0 * block + both[near:]
        b3 = c0 * b2 + dot3(high, b2)
        mixed = alpha * c0 * b1 + b3
        got = 1.5 * b1 - 0.5 * (
            alpha * c0 * c0 * b1
            + c0 * mixed
            + dot3(high, mixed)
            + alpha * (c1 * b3 + dot3(low, b3))
        )
        base = c0 * (1.5 - 0.5 * alpha * c0 * c0)
        driven = base * block[:, -1] + jnp.sum(x * got[:, -1][None, :], axis=1)
        again = jnp.sum(x * driven[None, :], axis=1)
        mean_part = (
            jnp.sum(block[:, :-1] * (base * driven)[:, None] + got[:, :-1] * again[:, None], axis=0)
            / bound
        )
        cell_mask = (cell_rows >= starts[patch]) & (cell_rows < starts[patch] + lengths[patch])
        root_scale = jnp.sqrt((members - 1.0) / bound)
        shift = shift + jnp.where(cell_mask, mean_part, 0.0)
        shrink = jnp.where(cell_mask, root_scale * base, shrink)
        weights_all = jnp.where(
            cell_mask[None, :], got[:, :-1] * (scale * (root_scale / bound))[:, None], weights_all
        )
    return shift[:, None] + shrink[:, None] * anomaly + dot3(weights_all.T, spread)


def general_device(ensemble, obs_cell, obs_value, obs_var, patch_rows):
    members_dev, lat_rows, lon_cells = ensemble.shape
    lat_count = lax.axis_size("lat")
    member_count = lax.axis_size("member")
    servers = lat_count * member_count
    width_cols = lon_cells // servers
    padded = with_halo(ensemble, (("lat", 1),), STEPS, False)
    global_rows = (
        lax.axis_index("lat") * lat_rows + jnp.arange(lat_rows + 2 * STEPS, dtype=jnp.int32) - STEPS
    )
    inside = ((global_rows >= 0) & (global_rows < lat_rows * lat_count)).astype(jnp.float32)
    for step_index in range(STEPS):
        padded = advance(padded)
        keeper = inside[step_index + 1 : inside.shape[0] - step_index - 1]
        padded = padded * keeper[None, :, None]
    blocks = padded.reshape(1, members_dev, lat_rows, lon_cells)
    received = lax.all_to_all(blocks, ("member", "lat"), split_axis=3, concat_axis=0, tiled=True)
    strip = received.reshape(member_count, lat_count, members_dev, lat_rows, width_cols)
    members = member_count * members_dev
    lat_total = lat_count * lat_rows
    states = strip.transpose(1, 3, 4, 0, 2).reshape(lat_total * width_cols, members)
    cell_index = obs_cell[0]
    obs_count = cell_index.shape[0]
    state_mean = jnp.mean(states, axis=1)
    anomaly = states - state_mean[:, None]
    spread = jnp.take(anomaly, cell_index, axis=0)
    innov = obs_value[0] - jnp.take(state_mean, cell_index)
    obs_meta = jnp.stack(
        [
            innov,
            obs_var[0],
            (cell_index // width_cols).astype(jnp.float32),
            (cell_index % width_cols).astype(jnp.float32),
        ]
    )
    near_spread = with_halo(spread, ((("member", "lat"), 0),), obs_count, True)
    near_meta = with_halo(obs_meta, ((("member", "lat"), 1),), obs_count, True)
    shifts = jnp.repeat(jnp.array([-1.0, 0.0, 1.0], jnp.float32), obs_count) * width_cols
    near_meta = jnp.concatenate([near_meta[:3], (near_meta[3] + shifts)[None, :]], axis=0)
    analysed = analyse(anomaly, state_mean, near_spread, near_meta, patch_rows[0], width_cols)
    outgoing = analysed.reshape(lat_count, lat_rows, width_cols, member_count, members_dev)
    outgoing = outgoing.transpose(3, 0, 4, 1, 2).reshape(servers, members_dev, lat_rows, width_cols)
    returned = lax.all_to_all(outgoing, ("member", "lat"), split_axis=0, concat_axis=3, tiled=True)
    return returned.reshape(members_dev, lat_rows, lon_cells)


def place(block, lats):
    half = block // (lats // 2)
    return (1 - half) * (2 * block) + half * (2 * lats - 1 - 2 * block)


def block_at(lat, lats):
    odd = lat % 2
    return (1 - odd) * (lat // 2) + odd * (lats - 1 - lat // 2)


def member_of(block, q, members):
    odd = block % 2
    return (1 - odd) * q + odd * (members - 1 - q)


def strip_at(m, lat, lats, members):
    block = block_at(lat, lats)
    return block * members + member_of(block, m, members)


def home_of(strip, lats, members):
    block = strip // members
    return member_of(block, strip % members, members), place(block, lats)


def greet_all(lats, members):
    m, lat = lax.axis_index("member"), lax.axis_index("lat")
    barrier = pltpu.get_barrier_semaphore()
    for dm in range(members):
        for dl in range(lats):
            if dm == 0 and dl == 0:
                continue
            pl.semaphore_signal(
                barrier, inc=1, device_id=((m + dm) % members, (lat + dl) % lats), device_id_type=MESH
            )
    return barrier, lats * members - 1


def forecast(load, lats, rows, groups):
    fields = [load(l) for l in range(lats)]
    lane = lax.broadcasted_iota(jnp.int32, fields[0].shape, 1)
    first, last = lane < groups, lane >= LANES - groups
    count = fields[0].shape[0]
    zero = jnp.zeros_like(fields[0])
    for _ in range(STEPS):
        new = []
        for l in range(lats):
            c = fields[l]
            above = fields[l - 1] if l > 0 else zero
            below = fields[l + 1] if l + 1 < lats else zero
            north = pltpu.roll(jnp.where(last, above, c), groups, 1)
            south = pltpu.roll(jnp.where(first, below, c), LANES - groups, 1)
            east = pltpu.roll(c, count - 1, 0)
            west = pltpu.roll(c, 1, 0)
            new.append(
                c
                + lat_coeff * (north + south - 2.0 * c)
                + lon_coeff * (east + west - 2.0 * c)
                - advect_coeff * c * (east - west)
            )
        fields = new
    return fields


def forward_kernel(
    dims, x_ref, obs_ref, at_ref, mean_ref, yt_ref, meta_ref,
    s_buf, ra, f_buf, r_buf, obs_buf, a_send, a_recv, b_send, b_recv, o_send, o_recv, y_send, y_recv,
):
    lats, members, chunks, rows, width, group = dims
    cols = width * members
    m, lat = lax.axis_index("member"), lax.axis_index("lat")
    barrier, partners = greet_all(lats, members)
    edge = STEPS

    for kc in range(chunks):
        whole = jnp.concatenate([x_ref[kc * group : (kc + 1) * group, r, :] for r in range(rows)], axis=0)
        turned = whole.T
        lon = turned.shape[0]
        for b in range(lats):
            s_buf[kc, b, 0:cols] = turned[b * cols : (b + 1) * cols]
            east, west = ((b + 1) * cols) % lon, (b * cols - edge) % lon
            s_buf[kc, b, cols : cols + edge] = turned[east : east + edge]
            s_buf[kc, b, cols + edge : cols + 2 * edge] = turned[west : west + edge]

    pl.semaphore_wait(barrier, partners)

    target_m, target_l = home_of(m * lats + lat, lats, members)
    away = jnp.logical_or(target_m != m, target_l != lat)
    obs_copy = pltpu.make_async_remote_copy(
        src_ref=obs_ref, dst_ref=obs_buf, send_sem=o_send, recv_sem=o_recv,
        device_id=(target_m, target_l), device_id_type=MESH,
    )

    @pl.when(away)
    def _():
        obs_copy.start()

    @pl.when(jnp.logical_not(away))
    def _():
        obs_buf[...] = obs_ref[...]

    a_copies = []
    for kc in range(chunks):
        for d in range(1, lats):
            to = (lat + d) % lats
            copy = pltpu.make_async_remote_copy(
                src_ref=s_buf.at[kc, block_at(to, lats)], dst_ref=ra.at[kc, lat],
                send_sem=a_send.at[kc, d], recv_sem=a_recv.at[kc, d],
                device_id=(m, to), device_id_type=MESH,
            )
            copy.start()
            a_copies.append(copy)

    own = block_at(lat, lats)
    own_odd = own % 2
    b_copies = []
    for kc in range(chunks):
        ra[kc, lat] = s_buf[kc, own]
        for copy in a_copies[kc * (lats - 1) : (kc + 1) * (lats - 1)]:
            copy.wait_recv()
        fields = forecast(lambda l, kc=kc: ra[kc, l], lats, rows, group)
        for l in range(lats):
            for q in range(members):
                f_buf[kc, q, l] = fields[l][q * width : (q + 1) * width]
        for d in range(1, members):
            to = (m + d) % members
            copy = pltpu.make_async_remote_copy(
                src_ref=f_buf.at[kc, member_of(own, to, members)], dst_ref=r_buf.at[m, kc],
                send_sem=b_send.at[kc, d], recv_sem=b_recv.at[kc, d],
                device_id=(to, lat), device_id_type=MESH,
            )
            copy.start()
            b_copies.append(copy)
        r_buf[m, kc] = f_buf[kc, member_of(own, m, members)]

    @pl.when(away)
    def _():
        obs_copy.wait_recv()

    for copy in b_copies:
        copy.wait_recv()

    per = LANES // group
    lane_block = lax.broadcasted_iota(jnp.int32, (lats * width, LANES), 1) // group
    total = members * chunks // per
    for g in range(total):
        parts = []
        for j in range(per):
            c = g * per + j
            parts.append(r_buf[c // chunks, c % chunks].reshape(lats * width, LANES))
        for r in range(rows):
            out = None
            for j in range(per):
                shift = (group * (j - r)) % LANES
                piece = pltpu.roll(parts[j], shift, 1) if shift else parts[j]
                out = piece if out is None else jnp.where(lane_block == j, piece, out)
            for l in range(lats):
                at_ref[(l * rows + r) * width : (l * rows + r + 1) * width, g * LANES : (g + 1) * LANES] = out[
                    l * width : (l + 1) * width
                ]
    states = at_ref[...]
    cells, count = states.shape
    mean = jnp.sum(states, axis=1, keepdims=True) * (1.0 / count)
    anomaly = states - mean
    at_ref[...] = anomaly
    mean_ref[...] = jnp.broadcast_to(mean, mean_ref.shape)

    nobs = obs_buf.shape[1]
    eye = (
        lax.broadcasted_iota(jnp.int32, (nobs, nobs), 0) == lax.broadcasted_iota(jnp.int32, (nobs, nobs), 1)
    ).astype(jnp.float32)
    cell_col = jnp.sum(eye * obs_buf[0:1, :], axis=1, keepdims=True)
    onehot = (
        cell_col == lax.broadcasted_iota(jnp.int32, (nobs, cells), 1).astype(jnp.float32)
    ).astype(jnp.float32)
    spread = jnp.dot(onehot, anomaly, precision=lax.Precision.HIGHEST, preferred_element_type=jnp.float32)
    hit = jnp.sum(
        (lax.broadcasted_iota(jnp.int32, (cells, nobs), 0).astype(jnp.float32) == obs_buf[0:1, :]).astype(jnp.float32)
        * mean,
        axis=0,
        keepdims=True,
    )
    cell_row = obs_buf[0:1, :]
    row = jnp.floor(cell_row * (1.0 / width))
    yt_ref[1] = spread
    meta_ref[1, 0:1, :] = obs_buf[1:2, :] - hit
    meta_ref[1, 1:2, :] = obs_buf[2:3, :]
    meta_ref[1, 2:3, :] = row
    meta_ref[1, 3:4, :] = cell_row - width * row
    meta_ref[1, 4:5, :] = obs_buf[3:4, :]
    meta_ref[1, 5:8, :] = jnp.zeros((3, nobs), jnp.float32)

    strip = strip_at(m, lat, lats, members)
    count_strips = lats * members
    y_copies = []
    for side, slot in ((1, 0), (count_strips - 1, 2)):
        to_m, to_l = home_of((strip + side) % count_strips, lats, members)
        for i, ref in enumerate((yt_ref, meta_ref)):
            copy = pltpu.make_async_remote_copy(
                src_ref=ref.at[1], dst_ref=ref.at[slot],
                send_sem=y_send.at[slot, i], recv_sem=y_recv.at[slot, i],
                device_id=(to_m, to_l), device_id_type=MESH,
            )
            copy.start()
            y_copies.append(copy)
    for copy in y_copies:
        copy.wait_recv()

    for copy in a_copies + b_copies + y_copies:
        copy.wait_send()

    @pl.when(away)
    def _():
        obs_copy.wait_send()


def forward(ensemble, obs, dims):
    lats, members, chunks, rows, width, group = dims
    cells, total = lats * rows * width, members * chunks * group
    nobs = obs.shape[1]
    dma = pltpu.SemaphoreType.DMA
    vmem = pl.BlockSpec(memory_space=pltpu.VMEM)
    f32 = jnp.float32
    return pl.pallas_call(
        functools.partial(forward_kernel, dims),
        out_shape=(
            jax.ShapeDtypeStruct((cells, total), f32),
            jax.ShapeDtypeStruct((cells, LANES), f32),
            jax.ShapeDtypeStruct((3, nobs, total), f32),
            jax.ShapeDtypeStruct((3, 8, nobs), f32),
        ),
        in_specs=[vmem, vmem],
        out_specs=[vmem] * 4,
        scratch_shapes=[
            pltpu.VMEM((chunks, lats, members * width + 2 * STEPS, LANES), f32),
            pltpu.VMEM((chunks, lats, members * width + 2 * STEPS, LANES), f32),
            pltpu.VMEM((chunks, members, lats, width, LANES), f32),
            pltpu.VMEM((members, chunks, lats, width, LANES), f32),
            pltpu.VMEM((8, nobs), f32),
            dma((chunks, lats)),
            dma((chunks, lats)),
            dma((chunks, members)),
            dma((chunks, members)),
            dma,
            dma,
            dma((3, 2)),
            dma((3, 2)),
        ],
        compiler_params=pltpu.CompilerParams(
            collective_id=0, has_side_effects=True, vmem_limit_bytes=48 * 1024 * 1024
        ),
        name="forward",
    )(ensemble, obs)


def backward_kernel(dims, y_ref, z_ref, t_buf, send, recv):
    lats, members, chunks, rows, width, group = dims
    m, lat = lax.axis_index("member"), lax.axis_index("lat")
    barrier, partners = greet_all(lats, members)
    per = LANES // group
    lane_block = lax.broadcasted_iota(jnp.int32, (lats * width, LANES), 1) // group
    for g in range(members * chunks // per):
        parts = []
        for r in range(rows):
            parts.append(
                jnp.concatenate(
                    [
                        y_ref[(l * rows + r) * width : (l * rows + r + 1) * width, g * LANES : (g + 1) * LANES]
                        for l in range(lats)
                    ],
                    axis=0,
                )
            )
        for j in range(per):
            c = g * per + j
            out = None
            for r in range(rows):
                shift = (group * (r - j)) % LANES
                piece = pltpu.roll(parts[r], shift, 1) if shift else parts[r]
                out = piece if out is None else jnp.where(lane_block == r, piece, out)
            for l in range(lats):
                t_buf[c // chunks, l, c % chunks] = out[l * width : (l + 1) * width]
    pl.semaphore_wait(barrier, partners)
    strip = strip_at(m, lat, lats, members)
    copies = []
    for dl in range(lats):
        for dm in range(members):
            if dm == 0 and dl == 0:
                continue
            to_m, to_l = (m + dm) % members, (lat + dl) % lats
            copy = pltpu.make_async_remote_copy(
                src_ref=t_buf.at[to_m, to_l], dst_ref=z_ref.at[strip],
                send_sem=send.at[dl, dm], recv_sem=recv.at[dl, dm],
                device_id=(to_m, to_l), device_id_type=MESH,
            )
            copy.start()
            copies.append(copy)
    z_ref[strip] = t_buf[m, lat]
    for copy in copies:
        copy.wait()


def backward(analysed, dims):
    lats, members, chunks, rows, width, group = dims
    dma = pltpu.SemaphoreType.DMA
    vmem = pl.BlockSpec(memory_space=pltpu.VMEM)
    f32 = jnp.float32
    return pl.pallas_call(
        functools.partial(backward_kernel, dims),
        out_shape=jax.ShapeDtypeStruct((lats * members, chunks, width, LANES), f32),
        in_specs=[vmem],
        out_specs=vmem,
        scratch_shapes=[
            pltpu.VMEM((members, lats, chunks, width, LANES), f32),
            dma((lats, members)),
            dma((lats, members)),
        ],
        compiler_params=pltpu.CompilerParams(
            collective_id=1, has_side_effects=True, vmem_limit_bytes=48 * 1024 * 1024
        ),
        name="backward",
    )(analysed)


def split(a):
    high = a.astype(jnp.bfloat16)
    return high, (a - high.astype(jnp.float32)).astype(jnp.bfloat16)


def dot_pairs(a, b, dims=(((1,), (0,)), ((), ()))):
    (ah, al), (bh, bl) = a, b
    one = functools.partial(lax.dot_general, dimension_numbers=dims, preferred_element_type=jnp.float32)
    return one(ah, bh) + (one(ah, bl) + one(al, bh))


def to_column(row):
    eye = lax.broadcasted_iota(jnp.int32, (LANES, LANES), 0) == lax.broadcasted_iota(jnp.int32, (LANES, LANES), 1)
    return jnp.concatenate(
        [
            jnp.sum(jnp.where(eye, row[:, i : i + LANES], 0.0), axis=1, keepdims=True)
            for i in range(0, row.shape[1], LANES)
        ],
        axis=0,
    )


def analysis(dims, at, mean, yt, meta):
    lats, members, chunks, rows, width, group = dims
    cells, count = at.shape
    near = yt.shape[0]
    side = near // 3
    lat_total = cells // width
    y_pair = split(yt)
    a_pair = split(at)
    across = (((1,), (1,)), ((), ()))
    common = dot_pairs(y_pair, y_pair, across)
    crossed = dot_pairs(y_pair, a_pair, across)
    y_turned = yt.T

    strip_of = lax.broadcasted_iota(jnp.int32, (1, near), 1) // side - 1
    innov, var, obs_rows = meta[0:1], meta[1:2], meta[2:3]
    cols = meta[3:4] + (strip_of * width).astype(jnp.float32)
    lengths = [meta[4:5, side + i : side + i + 1] for i in range(2)]
    starts = [jnp.zeros_like(lengths[0]), lengths[0]]
    lon_gap = jnp.maximum(jnp.maximum(-cols, cols - (width - 1.0)), 0.0) / float(width)
    cell_row_lane = (lax.broadcasted_iota(jnp.int32, (1, cells), 1) // width).astype(jnp.float32)
    cell_row_col = (lax.broadcasted_iota(jnp.int32, (cells, 1), 0) // width).astype(jnp.float32)
    lane = lax.broadcasted_iota(jnp.int32, (near, cells), 1)

    shift = jnp.zeros((1, cells), jnp.float32)
    shrink = jnp.zeros((cells, 1), jnp.float32)
    combined = None
    for patch in range(2):
        lower = starts[patch]
        upper = lower + lengths[patch] - 1.0
        lat_gap = jnp.maximum(jnp.maximum(lower - obs_rows, obs_rows - upper), 0.0) / (lat_total / 4.0)
        weights = jnp.exp(-lat_gap * lat_gap - lon_gap * lon_gap) / var
        scale = jnp.sqrt(weights)
        left = (y_turned * weights).astype(jnp.bfloat16)
        sums = None
        for i in range(0, count, LANES):
            tile = jnp.abs(jnp.dot(left[i : i + LANES], y_pair[0], preferred_element_type=jnp.float32))
            part = jnp.sum(tile, axis=0, keepdims=True)
            sums = part if sums is None else sums + part
        bound = (count - 1.0) + jnp.max(sums, axis=1, keepdims=True)
        inverse = 1.0 / bound
        alpha = (count - 1.0) * inverse
        scale_col = to_column(scale)
        x = common * scale_col * (scale * inverse)
        c0 = 2.25 + alpha * (-2.4375 + alpha * (1.6875 + alpha * (-0.5625 + alpha * 0.0625)))
        c1 = -2.4375 + alpha * (3.375 + alpha * (-1.6875 + alpha * 0.25))
        c2 = 1.6875 + alpha * (-1.6875 + alpha * 0.375)
        c3 = -0.5625 + alpha * 0.25
        c4 = 0.0625
        x_pair = split(x)
        x2 = dot_pairs(x_pair, x_pair)
        low = c2 * x + c3 * x2 + c4 * dot_pairs(split(x2), x_pair)
        low_pair = split(low)
        spare = cells - 1 if patch == 0 else 0
        block = jnp.where(lane == spare, to_column(innov), crossed) * scale_col
        b_pair = split(block)
        b1 = c1 * block + dot_pairs(low_pair, b_pair)
        b2 = c0 * block + dot_pairs(x_pair, split(b1))
        w = c1 * b2 + dot_pairs(low_pair, split(b2))
        b3 = c0 * b2 + dot_pairs(x_pair, split(w))
        u = c1 * b3 + dot_pairs(low_pair, split(b3))
        z = c0 * b3 + dot_pairs(x_pair, split(u))
        got = 1.5 * b1 - 0.5 * (z + alpha * (u + c0 * (w + c0 * b1)))
        base = c0 * (1.5 - 0.5 * alpha * c0 * c0)
        full = base * block + dot_pairs(x_pair, split(got))
        drive = full[:, spare : spare + 1]
        mean_part = jnp.sum(full * drive, axis=0, keepdims=True) * inverse
        root_scale = jnp.sqrt(alpha)
        inside = jnp.logical_and(cell_row_lane >= lower, cell_row_lane <= upper)
        inside_col = jnp.logical_and(cell_row_col >= lower, cell_row_col <= upper)
        shift = jnp.where(inside, mean_part, shift)
        shrink = jnp.where(inside_col, root_scale * base, shrink)
        weighted = got * (scale_col * (root_scale * inverse))
        combined = weighted if combined is None else jnp.where(inside, weighted, combined)
    return (mean + to_column(shift)) + shrink * at + dot_pairs(split(combined.T), y_pair)


def analysis_kernel(dims, at_ref, mean_ref, yt_ref, meta_ref, out_ref):
    yt = jnp.concatenate([yt_ref[i] for i in range(3)], axis=0)
    meta = jnp.concatenate([meta_ref[i] for i in range(3)], axis=1)
    out_ref[...] = analysis(dims, at_ref[...], mean_ref[:, 0:1], yt, meta)


def analyse_strip(anomaly, mean, spread, meta, dims):
    vmem = pl.BlockSpec(memory_space=pltpu.VMEM)
    return pl.pallas_call(
        functools.partial(analysis_kernel, dims),
        out_shape=jax.ShapeDtypeStruct(anomaly.shape, jnp.float32),
        in_specs=[vmem] * 4,
        out_specs=vmem,
        compiler_params=pltpu.CompilerParams(vmem_limit_bytes=56 * 1024 * 1024),
        name="analysis",
    )(anomaly, mean, spread, meta)


def settle_kernel(dims, z_ref, out_ref):
    lats, members, chunks, rows, width, group = dims
    for kc in range(chunks):
        lon = jnp.concatenate([z_ref[s, kc] for s in range(lats * members)], axis=0)
        turned = lon.T
        for r in range(rows):
            out_ref[kc * group : (kc + 1) * group, r, :] = turned[r * group : (r + 1) * group]


def settle(pieces, dims):
    lats, members, chunks, rows, width, group = dims
    vmem = pl.BlockSpec(memory_space=pltpu.VMEM)
    return pl.pallas_call(
        functools.partial(settle_kernel, dims),
        out_shape=jax.ShapeDtypeStruct((chunks * group, rows, lats * members * width), jnp.float32),
        in_specs=[vmem],
        out_specs=vmem,
        name="settle",
    )(pieces)


def kernel_device(dims, ensemble, obs_cell, obs_value, obs_var, patch_rows):
    lats, members, chunks, rows, width, group = dims
    nobs = obs_cell.shape[1]
    obs = jnp.concatenate(
        [
            obs_cell.astype(jnp.float32),
            obs_value,
            obs_var,
            jnp.pad(patch_rows.astype(jnp.float32), ((0, 0), (0, nobs - patch_rows.shape[1]))),
            jnp.zeros((4, nobs), jnp.float32),
        ],
        axis=0,
    )
    anomaly, mean, spread, meta = forward(ensemble, obs, dims)
    analysed = analyse_strip(anomaly, mean, spread, meta, dims)
    return settle(backward(analysed, dims), dims)


def kernel_dims(mesh, ensemble, obs_cell, patch_rows):
    lats, members = mesh.shape["lat"], mesh.shape["member"]
    total, lat_all, lon = ensemble.shape
    own, rows = total // members, lat_all // lats
    width = lon // (lats * members)
    if LANES % rows:
        return None
    group = LANES // rows
    fits = (
        own % group == 0
        and (members * (own // group)) % rows == 0
        and width == 8
        and lats % 2 == 0
        and members % 2 == 0
        and obs_cell.shape[1] % LANES == 0
        and patch_rows.shape[1] == 2
    )
    return (lats, members, own // group, rows, width, group) if fits else None


def solution(mesh):
    specs = (P("member", "lat", None),) + (P(("member", "lat"), None),) * 4

    def run(ensemble, obs_cell, obs_value, obs_var, patch_rows):
        dims = kernel_dims(mesh, ensemble, obs_cell, patch_rows)
        body = general_device if dims is None else functools.partial(kernel_device, dims)
        mapped = jax.shard_map(
            body, mesh=mesh, in_specs=specs, out_specs=P("member", "lat", None), check_vma=False
        )
        return mapped(ensemble, obs_cell, obs_value, obs_var, patch_rows)

    return run
```

```python
import functools

import jax
import jax.numpy as jnp
from jax import lax
from jax.experimental import pallas as pl
from jax.experimental.pallas import tpu as pltpu
from jax.sharding import PartitionSpec as P

STEPS = 4

lat_coeff = 0.4
lon_coeff = 0.05
advect_coeff = 0.1

MESH = pl.DeviceIdType.MESH
LANES = 128


def with_halo(value, sides, width, wrap):
    for axis, dim in sides:
        size, length = (lax.axis_size(axis), value.shape[dim])
        up = [(i, (i + 1) % size) for i in range(size if wrap else size - 1)]
        down = [(j, i) for i, j in up]
        last = lax.slice_in_dim(value, length - width, length, axis=dim)
        initial = lax.slice_in_dim(value, 0, width, axis=dim)
        before = lax.ppermute(last, axis, up)
        after = lax.ppermute(initial, axis, down)
        value = jnp.concatenate([before, value, after], axis=dim)
    return value


def advance(padded):
    centre = padded[:, 1:-1]
    northern = padded[:, :-2]
    southern = padded[:, 2:]
    eastern = jnp.roll(centre, -1, axis=2)
    western = jnp.roll(centre, 1, axis=2)
    return (
        centre
        + lat_coeff * (northern + southern - 2.0 * centre)
        + lon_coeff * (eastern + western - 2.0 * centre)
        - advect_coeff * centre * (eastern - western)
    )


def localize(obs_rows, rel_cols, first_row, row_count, lat_scale, width_cols):
    lower = first_row.astype(jnp.float32)
    upper = lower + row_count.astype(jnp.float32) - 1.0
    lat_gap = jnp.maximum(jnp.maximum(lower - obs_rows, obs_rows - upper), 0.0) / lat_scale
    lon_gap = jnp.maximum(jnp.maximum(-rel_cols, rel_cols - (width_cols - 1.0)), 0.0) / width_cols
    return jnp.exp(-lat_gap * lat_gap - lon_gap * lon_gap)


def dot3(left, right):
    return jnp.matmul(left, right, precision=lax.Precision.HIGH, preferred_element_type=jnp.float32)


def analyse(anomaly, state_mean, spread, obs_meta, lengths, width_cols):
    cell_total, members = anomaly.shape
    lat_total = cell_total // width_cols
    near = spread.shape[0]
    starts = jnp.cumsum(lengths) - lengths
    cell_rows = jnp.arange(cell_total, dtype=jnp.int32) // width_cols
    identity = jnp.eye(members, dtype=jnp.float32)
    products = dot3(spread, jnp.concatenate([spread, anomaly], axis=0).T)
    common, crossed = products[:, :near], products[:, near:]
    innov = obs_meta[0]
    shrink = jnp.zeros((cell_total,), jnp.float32)
    shift = state_mean
    weights_all = jnp.zeros((near, cell_total), jnp.float32)
    for patch in range(lengths.shape[0]):
        weights = (
            localize(obs_meta[2], obs_meta[3], starts[patch], lengths[patch], lat_total / 4.0, float(width_cols))
            / obs_meta[1]
        )
        scale = jnp.sqrt(weights)
        gram_matrix = (members - 1.0) * identity + jnp.dot(
            (spread * weights[:, None]).T, spread, preferred_element_type=jnp.float32
        )
        bound = jnp.max(jnp.sum(jnp.abs(gram_matrix), axis=1))
        alpha = (members - 1.0) / bound
        x = common * scale[:, None] * (scale / bound)[None, :]
        c0 = 2.25 + alpha * (-2.4375 + alpha * (1.6875 + alpha * (-0.5625 + alpha * 0.0625)))
        c1 = -2.4375 + alpha * (3.375 + alpha * (-1.6875 + alpha * 0.25))
        c2 = 1.6875 + alpha * (-1.6875 + alpha * 0.375)
        c3 = -0.5625 + alpha * 0.25
        c4 = 0.0625
        x2 = dot3(x, x)
        x34 = dot3(x2, jnp.concatenate([x, x2], axis=1))
        x3, x4 = x34[:, :near], x34[:, near:]
        low = c2 * x + c3 * x2 + c4 * x3
        high = c1 * x + c2 * x2 + c3 * x3 + c4 * x4
        block = jnp.concatenate([crossed * scale[:, None], (scale * innov)[:, None]], axis=1)
        both = dot3(jnp.concatenate([low, high], axis=0), block)
        b1 = c1 * block + both[:near]
        b2 = c0 * block + both[near:]
        b3 = c0 * b2 + dot3(high, b2)
        mixed = alpha * c0 * b1 + b3
        got = 1.5 * b1 - 0.5 * (
            alpha * c0 * c0 * b1
            + c0 * mixed
            + dot3(high, mixed)
            + alpha * (c1 * b3 + dot3(low, b3))
        )
        base = c0 * (1.5 - 0.5 * alpha * c0 * c0)
        driven = base * block[:, -1] + jnp.sum(x * got[:, -1][None, :], axis=1)
        again = jnp.sum(x * driven[None, :], axis=1)
        mean_part = (
            jnp.sum(block[:, :-1] * (base * driven)[:, None] + got[:, :-1] * again[:, None], axis=0)
            / bound
        )
        cell_mask = (cell_rows >= starts[patch]) & (cell_rows < starts[patch] + lengths[patch])
        root_scale = jnp.sqrt((members - 1.0) / bound)
        shift = shift + jnp.where(cell_mask, mean_part, 0.0)
        shrink = jnp.where(cell_mask, root_scale * base, shrink)
        weights_all = jnp.where(
            cell_mask[None, :], got[:, :-1] * (scale * (root_scale / bound))[:, None], weights_all
        )
    return shift[:, None] + shrink[:, None] * anomaly + dot3(weights_all.T, spread)


def general_device(ensemble, obs_cell, obs_value, obs_var, patch_rows):
    members_dev, lat_rows, lon_cells = ensemble.shape
    lat_count = lax.axis_size("lat")
    member_count = lax.axis_size("member")
    servers = lat_count * member_count
    width_cols = lon_cells // servers
    padded = with_halo(ensemble, (("lat", 1),), STEPS, False)
    global_rows = (
        lax.axis_index("lat") * lat_rows + jnp.arange(lat_rows + 2 * STEPS, dtype=jnp.int32) - STEPS
    )
    inside = ((global_rows >= 0) & (global_rows < lat_rows * lat_count)).astype(jnp.float32)
    for step_index in range(STEPS):
        padded = advance(padded)
        keeper = inside[step_index + 1 : inside.shape[0] - step_index - 1]
        padded = padded * keeper[None, :, None]
    blocks = padded.reshape(1, members_dev, lat_rows, lon_cells)
    received = lax.all_to_all(blocks, ("member", "lat"), split_axis=3, concat_axis=0, tiled=True)
    strip = received.reshape(member_count, lat_count, members_dev, lat_rows, width_cols)
    members = member_count * members_dev
    lat_total = lat_count * lat_rows
    states = strip.transpose(1, 3, 4, 0, 2).reshape(lat_total * width_cols, members)
    cell_index = obs_cell[0]
    obs_count = cell_index.shape[0]
    state_mean = jnp.mean(states, axis=1)
    anomaly = states - state_mean[:, None]
    spread = jnp.take(anomaly, cell_index, axis=0)
    innov = obs_value[0] - jnp.take(state_mean, cell_index)
    obs_meta = jnp.stack(
        [
            innov,
            obs_var[0],
            (cell_index // width_cols).astype(jnp.float32),
            (cell_index % width_cols).astype(jnp.float32),
        ]
    )
    near_spread = with_halo(spread, ((("member", "lat"), 0),), obs_count, True)
    near_meta = with_halo(obs_meta, ((("member", "lat"), 1),), obs_count, True)
    shifts = jnp.repeat(jnp.array([-1.0, 0.0, 1.0], jnp.float32), obs_count) * width_cols
    near_meta = jnp.concatenate([near_meta[:3], (near_meta[3] + shifts)[None, :]], axis=0)
    analysed = analyse(anomaly, state_mean, near_spread, near_meta, patch_rows[0], width_cols)
    outgoing = analysed.reshape(lat_count, lat_rows, width_cols, member_count, members_dev)
    outgoing = outgoing.transpose(3, 0, 4, 1, 2).reshape(servers, members_dev, lat_rows, width_cols)
    returned = lax.all_to_all(outgoing, ("member", "lat"), split_axis=0, concat_axis=3, tiled=True)
    return returned.reshape(members_dev, lat_rows, lon_cells)


def place(block, lats):
    half = block // (lats // 2)
    return (1 - half) * (2 * block) + half * (2 * lats - 1 - 2 * block)


def block_at(lat, lats):
    odd = lat % 2
    return (1 - odd) * (lat // 2) + odd * (lats - 1 - lat // 2)


def member_of(block, q, members):
    odd = block % 2
    return (1 - odd) * q + odd * (members - 1 - q)


def strip_at(m, lat, lats, members):
    block = block_at(lat, lats)
    return block * members + member_of(block, m, members)


def home_of(strip, lats, members):
    block = strip // members
    return member_of(block, strip % members, members), place(block, lats)


def greet_all(lats, members):
    m, lat = lax.axis_index("member"), lax.axis_index("lat")
    barrier = pltpu.get_barrier_semaphore()
    for dm in range(members):
        for dl in range(lats):
            if dm == 0 and dl == 0:
                continue
            pl.semaphore_signal(
                barrier, inc=1, device_id=((m + dm) % members, (lat + dl) % lats), device_id_type=MESH
            )
    return barrier, lats * members - 1


def split(a):
    high = a.astype(jnp.bfloat16)
    return high, (a - high.astype(jnp.float32)).astype(jnp.bfloat16)


def dot_pairs(a, b, dims=(((1,), (0,)), ((), ()))):
    (ah, al), (bh, bl) = a, b
    one = functools.partial(lax.dot_general, dimension_numbers=dims, preferred_element_type=jnp.float32)
    return one(ah, bh) + (one(ah, bl) + one(al, bh))


def to_column(row):
    eye = lax.broadcasted_iota(jnp.int32, (LANES, LANES), 0) == lax.broadcasted_iota(jnp.int32, (LANES, LANES), 1)
    return jnp.concatenate(
        [
            jnp.sum(jnp.where(eye, row[:, i : i + LANES], 0.0), axis=1, keepdims=True)
            for i in range(0, row.shape[1], LANES)
        ],
        axis=0,
    )


def analysis(dims, at, mean, yt, y_mean, meta):
    lats, members, chunks, rows, width, group = dims
    cells, count = at.shape
    near = yt.shape[0]
    side = near // 3
    lat_total = cells // width
    y_pair = split(yt)
    a_pair = split(at)
    across = (((1,), (1,)), ((), ()))
    common = dot_pairs(y_pair, y_pair, across)
    crossed = dot_pairs(y_pair, a_pair, across)
    y_turned = yt.T

    strip_of = lax.broadcasted_iota(jnp.int32, (1, near), 1) // side - 1
    innov = to_column(meta[0:1]) - y_mean
    var, obs_rows = meta[1:2], meta[2:3]
    cols = meta[3:4] + (strip_of * width).astype(jnp.float32)
    lengths = [meta[4:5, side + i : side + i + 1] for i in range(2)]
    starts = [jnp.zeros_like(lengths[0]), lengths[0]]
    lon_gap = jnp.maximum(jnp.maximum(-cols, cols - (width - 1.0)), 0.0) / float(width)
    cell_row_lane = (lax.broadcasted_iota(jnp.int32, (1, cells), 1) // width).astype(jnp.float32)
    cell_row_col = (lax.broadcasted_iota(jnp.int32, (cells, 1), 0) // width).astype(jnp.float32)
    lane = lax.broadcasted_iota(jnp.int32, (near, cells), 1)

    shift = jnp.zeros((1, cells), jnp.float32)
    shrink = jnp.zeros((cells, 1), jnp.float32)
    combined = None
    for patch in range(2):
        lower = starts[patch]
        upper = lower + lengths[patch] - 1.0
        lat_gap = jnp.maximum(jnp.maximum(lower - obs_rows, obs_rows - upper), 0.0) / (lat_total / 4.0)
        weights = jnp.exp(-lat_gap * lat_gap - lon_gap * lon_gap) / var
        scale = jnp.sqrt(weights)
        left = (y_turned * weights).astype(jnp.bfloat16)
        sums = None
        for i in range(0, count, LANES):
            tile = jnp.abs(jnp.dot(left[i : i + LANES], y_pair[0], preferred_element_type=jnp.float32))
            part = jnp.sum(tile, axis=0, keepdims=True)
            sums = part if sums is None else sums + part
        bound = (count - 1.0) + jnp.max(sums, axis=1, keepdims=True)
        inverse = 1.0 / bound
        alpha = (count - 1.0) * inverse
        scale_col = to_column(scale)
        x = common * scale_col * (scale * inverse)
        c0 = 2.25 + alpha * (-2.4375 + alpha * (1.6875 + alpha * (-0.5625 + alpha * 0.0625)))
        c1 = -2.4375 + alpha * (3.375 + alpha * (-1.6875 + alpha * 0.25))
        c2 = 1.6875 + alpha * (-1.6875 + alpha * 0.375)
        c3 = -0.5625 + alpha * 0.25
        c4 = 0.0625
        x_pair = split(x)
        x2 = dot_pairs(x_pair, x_pair)
        low = c2 * x + c3 * x2 + c4 * dot_pairs(split(x2), x_pair)
        low_pair = split(low)
        spare = cells - 1 if patch == 0 else 0
        block = jnp.where(lane == spare, innov, crossed) * scale_col
        b_pair = split(block)
        b1 = c1 * block + dot_pairs(low_pair, b_pair)
        b2 = c0 * block + dot_pairs(x_pair, split(b1))
        w = c1 * b2 + dot_pairs(low_pair, split(b2))
        b3 = c0 * b2 + dot_pairs(x_pair, split(w))
        u = c1 * b3 + dot_pairs(low_pair, split(b3))
        z = c0 * b3 + dot_pairs(x_pair, split(u))
        got = 1.5 * b1 - 0.5 * (z + alpha * (u + c0 * (w + c0 * b1)))
        base = c0 * (1.5 - 0.5 * alpha * c0 * c0)
        full = base * block + dot_pairs(x_pair, split(got))
        drive = full[:, spare : spare + 1]
        mean_part = jnp.sum(full * drive, axis=0, keepdims=True) * inverse
        root_scale = jnp.sqrt(alpha)
        inside = jnp.logical_and(cell_row_lane >= lower, cell_row_lane <= upper)
        inside_col = jnp.logical_and(cell_row_col >= lower, cell_row_col <= upper)
        shift = jnp.where(inside, mean_part, shift)
        shrink = jnp.where(inside_col, root_scale * base, shrink)
        weighted = got * (scale_col * (root_scale * inverse))
        combined = weighted if combined is None else jnp.where(inside, weighted, combined)
    return (mean + to_column(shift)) + shrink * at + dot_pairs(split(combined.T), y_pair)


def forecast(load, lats, group):
    fields = [load(l) for l in range(lats)]
    lane = lax.broadcasted_iota(jnp.int32, fields[0].shape, 1)
    first, last = lane < group, lane >= LANES - group
    count = fields[0].shape[0]
    zero = jnp.zeros_like(fields[0])
    for _ in range(STEPS):
        new = []
        for l in range(lats):
            c = fields[l]
            above = fields[l - 1] if l > 0 else zero
            below = fields[l + 1] if l + 1 < lats else zero
            north = pltpu.roll(jnp.where(last, above, c), group, 1)
            south = pltpu.roll(jnp.where(first, below, c), LANES - group, 1)
            east = pltpu.roll(c, count - 1, 0)
            west = pltpu.roll(c, 1, 0)
            new.append(
                c
                + lat_coeff * (north + south - 2.0 * c)
                + lon_coeff * (east + west - 2.0 * c)
                - advect_coeff * c * (east - west)
            )
        fields = new
    return fields


def swap_blocks(parts, group):
    per = len(parts)
    lane_block = lax.broadcasted_iota(jnp.int32, parts[0].shape, 1) // group
    outs = []
    for i in range(per):
        out = None
        for j in range(per):
            shift = (group * (j - i)) % LANES
            piece = pltpu.roll(parts[j], shift, 1) if shift else parts[j]
            out = piece if out is None else jnp.where(lane_block == j, piece, out)
        outs.append(out)
    return outs


def pick(onehot, values):
    total, rest = None, values
    for _ in range(3):
        term = rest.astype(jnp.bfloat16)
        part = jnp.dot(onehot, term, preferred_element_type=jnp.float32)
        total = part if total is None else total + part
        rest = rest - term.astype(jnp.float32)
    return total


def engine_kernel(
    dims, x_hbm, cell_ref, value_ref, var_ref, rows_ref, z_hbm,
    x_buf, s_buf, ra, f_buf, r_buf, xt, yt, meta, obs_out, obs_in, t_buf,
    x_sem, a_send, a_recv, b_send, b_recv, o_send, o_recv, m_send, m_recv, y_send, y_recv, z_send, z_recv, own_sem,
):
    lats, members, chunks, rows, width, group = dims
    cols = width * members
    cells = lats * rows * width
    strips = lats * members
    edge = STEPS
    m, lat = lax.axis_index("member"), lax.axis_index("lat")
    own = block_at(lat, lats)
    strip = strip_at(m, lat, lats, members)
    neighbours = [(slot, home_of((strip + side) % strips, lats, members)) for side, slot in ((1, 0), (strips - 1, 2))]

    def remote(src, dst, send, recv, to):
        return pltpu.make_async_remote_copy(
            src_ref=src, dst_ref=dst, send_sem=send, recv_sem=recv, device_id=to, device_id_type=MESH
        )

    reads = [
        pltpu.make_async_copy(x_hbm.at[pl.ds(kc * group, group)], x_buf.at[kc], x_sem.at[kc]) for kc in range(chunks)
    ]
    for read in reads:
        read.start()
    barrier, partners = greet_all(lats, members)

    obs_out[...] = jnp.zeros_like(obs_out)
    obs_out[0:1, :] = cell_ref[...].astype(jnp.float32)
    obs_out[1:2, :] = value_ref[...]
    obs_out[2:3, :] = var_ref[...]
    obs_out[3:4, 0 : rows_ref.shape[1]] = rows_ref[...].astype(jnp.float32)

    target_m, target_l = home_of(m * lats + lat, lats, members)
    away = jnp.logical_or(target_m != m, target_l != lat)
    obs_copy = remote(obs_out, obs_in, o_send, o_recv, (target_m, target_l))

    a_copies = []
    for kc in range(chunks):
        reads[kc].wait()
        whole = jnp.concatenate([x_buf[kc, :, r, :] for r in range(rows)], axis=0)
        turned = whole.T
        lon = turned.shape[0]
        for b in range(lats):
            s_buf[kc, b, 0:cols] = turned[b * cols : (b + 1) * cols]
            east, west = ((b + 1) * cols) % lon, (b * cols - edge) % lon
            s_buf[kc, b, cols : cols + edge] = turned[east : east + edge]
            s_buf[kc, b, cols + edge : cols + 2 * edge] = turned[west : west + edge]
        if kc == 0:
            pl.semaphore_wait(barrier, partners)

            @pl.when(away)
            def _():
                obs_copy.start()

            @pl.when(jnp.logical_not(away))
            def _():
                obs_in[...] = obs_out[...]

        run = []
        for d in range(1, lats):
            to = (lat + d) % lats
            copy = remote(
                s_buf.at[kc, block_at(to, lats)], ra.at[kc, lat], a_send.at[kc, d], a_recv.at[kc, d], (m, to)
            )
            copy.start()
            run.append(copy)
        a_copies.append(run)

    @pl.when(away)
    def _():
        obs_copy.wait_recv()

    cell_lane = obs_in[0:1, :]
    obs_row = jnp.floor(cell_lane * (1.0 / width))
    meta[1, 0:1, :] = obs_in[1:2, :]
    meta[1, 1:2, :] = obs_in[2:3, :]
    meta[1, 2:3, :] = obs_row
    meta[1, 3:4, :] = cell_lane - width * obs_row
    meta[1, 4:5, :] = obs_in[3:4, :]
    meta[1, 5:8, :] = jnp.zeros((3, cell_lane.shape[1]), jnp.float32)
    late = []
    for slot, to in neighbours:
        copy = remote(meta.at[1], meta.at[slot], m_send.at[slot], m_recv.at[slot], to)
        copy.start()
        late.append(copy)
    onehot = (
        to_column(cell_lane)
        == lax.broadcasted_iota(jnp.int32, (cell_lane.shape[1], cells), 1).astype(jnp.float32)
    ).astype(jnp.bfloat16)

    b_copies = []

    def arrive(kc):
        for copy in b_copies[kc]:
            copy.wait_recv()
        parts = [r_buf[j, kc].reshape(lats * width, LANES) for j in range(members)]
        for r, out in enumerate(swap_blocks(parts, group)):
            for l in range(lats):
                xt[kc, (l * rows + r) * width : (l * rows + r + 1) * width] = out[l * width : (l + 1) * width]
        yt[1, kc] = pick(onehot, xt[kc])
        for slot, to in neighbours:
            copy = remote(yt.at[1, kc], yt.at[slot, kc], y_send.at[slot, kc], y_recv.at[slot, kc], to)
            copy.start()
            late.append(copy)

    for kc in range(chunks):
        ra[kc, lat] = s_buf[kc, own]
        for copy in a_copies[kc]:
            copy.wait_recv()
        fields = forecast(lambda l, kc=kc: ra[kc, l], lats, group)
        for l in range(lats):
            for q in range(members):
                f_buf[kc, q, l] = fields[l][q * width : (q + 1) * width]
        run = []
        for d in range(1, members):
            to = (m + d) % members
            copy = remote(
                f_buf.at[kc, member_of(own, to, members)], r_buf.at[m, kc], b_send.at[kc, d], b_recv.at[kc, d], (to, lat)
            )
            copy.start()
            run.append(copy)
        b_copies.append(run)
        r_buf[m, kc] = f_buf[kc, member_of(own, m, members)]
        if kc:
            arrive(kc - 1)
    arrive(chunks - 1)

    states = jnp.concatenate([xt[kc] for kc in range(chunks)], axis=1)
    mean = jnp.sum(states, axis=1, keepdims=True) * (1.0 / states.shape[1])
    at = states - mean
    for copy in late:
        copy.wait_recv()
    y_raw = jnp.concatenate(
        [jnp.concatenate([yt[slot, kc] for kc in range(chunks)], axis=1) for slot in range(3)], axis=0
    )
    y_mean = jnp.sum(y_raw, axis=1, keepdims=True) * (1.0 / y_raw.shape[1])
    all_meta = jnp.concatenate([meta[slot] for slot in range(3)], axis=1)
    analysed = analysis(dims, at, mean, y_raw - y_mean, y_mean, all_meta)

    for kc in range(chunks):
        lanes = analysed[:, kc * LANES : (kc + 1) * LANES]
        parts = [
            jnp.concatenate(
                [lanes[(l * rows + r) * width : (l * rows + r + 1) * width] for l in range(lats)], axis=0
            )
            for r in range(rows)
        ]
        for j, out in enumerate(swap_blocks(parts, group)):
            for l in range(lats):
                t_buf[j, l, kc] = out[l * width : (l + 1) * width]
    z_copies = []
    for dl in range(lats):
        for dm in range(members):
            if dm == 0 and dl == 0:
                continue
            to = ((m + dm) % members, (lat + dl) % lats)
            copy = remote(t_buf.at[to[0], to[1]], z_hbm.at[strip], z_send.at[dl, dm], z_recv.at[dl, dm], to)
            copy.start()
            z_copies.append(copy)
    kept = pltpu.make_async_copy(t_buf.at[m, lat], z_hbm.at[strip], own_sem)
    kept.start()

    for run in a_copies + b_copies + [late]:
        for copy in run:
            copy.wait_send()

    @pl.when(away)
    def _():
        obs_copy.wait_send()

    kept.wait()
    for copy in z_copies:
        copy.wait()


def engine(ensemble, obs_cell, obs_value, obs_var, patch_rows, dims):
    lats, members, chunks, rows, width, group = dims
    cells = lats * rows * width
    nobs = obs_cell.shape[1]
    strips = lats * members
    dma, f32 = pltpu.SemaphoreType.DMA, jnp.float32
    vmem, anywhere = pl.BlockSpec(memory_space=pltpu.VMEM), pl.BlockSpec(memory_space=pl.ANY)
    block = (chunks, lats, members * width + 2 * STEPS, LANES)
    return pl.pallas_call(
        functools.partial(engine_kernel, dims),
        out_shape=jax.ShapeDtypeStruct((strips, chunks, width, LANES), f32),
        in_specs=[anywhere, vmem, vmem, vmem, vmem],
        out_specs=anywhere,
        scratch_shapes=[
            pltpu.VMEM((chunks, group, rows, strips * width), f32),
            pltpu.VMEM(block, f32),
            pltpu.VMEM(block, f32),
            pltpu.VMEM((chunks, members, lats, width, LANES), f32),
            pltpu.VMEM((members, chunks, lats, width, LANES), f32),
            pltpu.VMEM((chunks, cells, LANES), f32),
            pltpu.VMEM((3, chunks, nobs, LANES), f32),
            pltpu.VMEM((3, 8, nobs), f32),
            pltpu.VMEM((8, nobs), f32),
            pltpu.VMEM((8, nobs), f32),
            pltpu.VMEM((members, lats, chunks, width, LANES), f32),
            dma((chunks,)),
            dma((chunks, lats)),
            dma((chunks, lats)),
            dma((chunks, members)),
            dma((chunks, members)),
            dma,
            dma,
            dma((3,)),
            dma((3,)),
            dma((3, chunks)),
            dma((3, chunks)),
            dma((lats, members)),
            dma((lats, members)),
            dma,
        ],
        compiler_params=pltpu.CompilerParams(
            collective_id=0, has_side_effects=True, vmem_limit_bytes=56 * 1024 * 1024
        ),
        name="engine",
    )(ensemble, obs_cell, obs_value, obs_var, patch_rows)


def settle_kernel(dims, z_ref, out_ref):
    lats, members, chunks, rows, width, group = dims
    turned = z_ref[...].reshape(lats * members * width, LANES).T
    for r in range(rows):
        out_ref[:, r, :] = turned[r * group : (r + 1) * group]


def settle(pieces, dims):
    lats, members, chunks, rows, width, group = dims
    strips = lats * members
    return pl.pallas_call(
        functools.partial(settle_kernel, dims),
        grid=(chunks,),
        out_shape=jax.ShapeDtypeStruct((chunks * group, rows, strips * width), jnp.float32),
        in_specs=[pl.BlockSpec((strips, None, width, LANES), lambda kc: (0, kc, 0, 0))],
        out_specs=pl.BlockSpec((group, rows, strips * width), lambda kc: (kc, 0, 0)),
        name="settle",
    )(pieces)


def kernel_device(dims, ensemble, obs_cell, obs_value, obs_var, patch_rows):
    return settle(engine(ensemble, obs_cell, obs_value, obs_var, patch_rows, dims), dims)


def kernel_dims(mesh, ensemble, obs_cell, patch_rows):
    lats, members = mesh.shape["lat"], mesh.shape["member"]
    total, lat_all, lon = ensemble.shape
    own, rows = total // members, lat_all // lats
    width = lon // (lats * members)
    if LANES % rows:
        return None
    group = LANES // rows
    fits = (
        own % group == 0
        and (members * (own // group)) % rows == 0
        and width == 8
        and lats % 2 == 0
        and members % 2 == 0
        and obs_cell.shape[1] % LANES == 0
        and patch_rows.shape[1] == 2
    )
    return (lats, members, own // group, rows, width, group) if fits else None


def solution(mesh):
    specs = (P("member", "lat", None),) + (P(("member", "lat"), None),) * 4

    def run(ensemble, obs_cell, obs_value, obs_var, patch_rows):
        dims = kernel_dims(mesh, ensemble, obs_cell, patch_rows)
        body = general_device if dims is None else functools.partial(kernel_device, dims)
        mapped = jax.shard_map(
            body, mesh=mesh, in_specs=specs, out_specs=P("member", "lat", None), check_vma=False
        )
        return mapped(ensemble, obs_cell, obs_value, obs_var, patch_rows)

    return run
```

```python
import functools

import jax
import jax.numpy as jnp
from jax import lax
from jax.experimental import pallas as pl
from jax.experimental.pallas import tpu as pltpu
from jax.sharding import PartitionSpec as P

STEPS = 4

lat_coeff = 0.4
lon_coeff = 0.05
advect_coeff = 0.1

MESH = pl.DeviceIdType.MESH
LANES = 128


def with_halo(value, sides, width, wrap):
    for axis, dim in sides:
        size, length = (lax.axis_size(axis), value.shape[dim])
        up = [(i, (i + 1) % size) for i in range(size if wrap else size - 1)]
        down = [(j, i) for i, j in up]
        last = lax.slice_in_dim(value, length - width, length, axis=dim)
        initial = lax.slice_in_dim(value, 0, width, axis=dim)
        before = lax.ppermute(last, axis, up)
        after = lax.ppermute(initial, axis, down)
        value = jnp.concatenate([before, value, after], axis=dim)
    return value


def advance(padded):
    centre = padded[:, 1:-1]
    northern = padded[:, :-2]
    southern = padded[:, 2:]
    eastern = jnp.roll(centre, -1, axis=2)
    western = jnp.roll(centre, 1, axis=2)
    return (
        centre
        + lat_coeff * (northern + southern - 2.0 * centre)
        + lon_coeff * (eastern + western - 2.0 * centre)
        - advect_coeff * centre * (eastern - western)
    )


def localize(obs_rows, rel_cols, first_row, row_count, lat_scale, width_cols):
    lower = first_row.astype(jnp.float32)
    upper = lower + row_count.astype(jnp.float32) - 1.0
    lat_gap = jnp.maximum(jnp.maximum(lower - obs_rows, obs_rows - upper), 0.0) / lat_scale
    lon_gap = jnp.maximum(jnp.maximum(-rel_cols, rel_cols - (width_cols - 1.0)), 0.0) / width_cols
    return jnp.exp(-lat_gap * lat_gap - lon_gap * lon_gap)


def dot3(left, right):
    return jnp.matmul(left, right, precision=lax.Precision.HIGH, preferred_element_type=jnp.float32)


def analyse(anomaly, state_mean, spread, obs_meta, lengths, width_cols):
    cell_total, members = anomaly.shape
    lat_total = cell_total // width_cols
    near = spread.shape[0]
    starts = jnp.cumsum(lengths) - lengths
    cell_rows = jnp.arange(cell_total, dtype=jnp.int32) // width_cols
    identity = jnp.eye(members, dtype=jnp.float32)
    products = dot3(spread, jnp.concatenate([spread, anomaly], axis=0).T)
    common, crossed = products[:, :near], products[:, near:]
    innov = obs_meta[0]
    shrink = jnp.zeros((cell_total,), jnp.float32)
    shift = state_mean
    weights_all = jnp.zeros((near, cell_total), jnp.float32)
    for patch in range(lengths.shape[0]):
        weights = (
            localize(obs_meta[2], obs_meta[3], starts[patch], lengths[patch], lat_total / 4.0, float(width_cols))
            / obs_meta[1]
        )
        scale = jnp.sqrt(weights)
        gram_matrix = (members - 1.0) * identity + jnp.dot(
            (spread * weights[:, None]).T, spread, preferred_element_type=jnp.float32
        )
        bound = jnp.max(jnp.sum(jnp.abs(gram_matrix), axis=1))
        alpha = (members - 1.0) / bound
        x = common * scale[:, None] * (scale / bound)[None, :]
        c0 = 2.25 + alpha * (-2.4375 + alpha * (1.6875 + alpha * (-0.5625 + alpha * 0.0625)))
        c1 = -2.4375 + alpha * (3.375 + alpha * (-1.6875 + alpha * 0.25))
        c2 = 1.6875 + alpha * (-1.6875 + alpha * 0.375)
        c3 = -0.5625 + alpha * 0.25
        c4 = 0.0625
        x2 = dot3(x, x)
        x34 = dot3(x2, jnp.concatenate([x, x2], axis=1))
        x3, x4 = x34[:, :near], x34[:, near:]
        low = c2 * x + c3 * x2 + c4 * x3
        high = c1 * x + c2 * x2 + c3 * x3 + c4 * x4
        block = jnp.concatenate([crossed * scale[:, None], (scale * innov)[:, None]], axis=1)
        both = dot3(jnp.concatenate([low, high], axis=0), block)
        b1 = c1 * block + both[:near]
        b2 = c0 * block + both[near:]
        b3 = c0 * b2 + dot3(high, b2)
        mixed = alpha * c0 * b1 + b3
        got = 1.5 * b1 - 0.5 * (
            alpha * c0 * c0 * b1
            + c0 * mixed
            + dot3(high, mixed)
            + alpha * (c1 * b3 + dot3(low, b3))
        )
        base = c0 * (1.5 - 0.5 * alpha * c0 * c0)
        driven = base * block[:, -1] + jnp.sum(x * got[:, -1][None, :], axis=1)
        again = jnp.sum(x * driven[None, :], axis=1)
        mean_part = (
            jnp.sum(block[:, :-1] * (base * driven)[:, None] + got[:, :-1] * again[:, None], axis=0)
            / bound
        )
        cell_mask = (cell_rows >= starts[patch]) & (cell_rows < starts[patch] + lengths[patch])
        root_scale = jnp.sqrt((members - 1.0) / bound)
        shift = shift + jnp.where(cell_mask, mean_part, 0.0)
        shrink = jnp.where(cell_mask, root_scale * base, shrink)
        weights_all = jnp.where(
            cell_mask[None, :], got[:, :-1] * (scale * (root_scale / bound))[:, None], weights_all
        )
    return shift[:, None] + shrink[:, None] * anomaly + dot3(weights_all.T, spread)


def general_device(ensemble, obs_cell, obs_value, obs_var, patch_rows):
    members_dev, lat_rows, lon_cells = ensemble.shape
    lat_count = lax.axis_size("lat")
    member_count = lax.axis_size("member")
    servers = lat_count * member_count
    width_cols = lon_cells // servers
    padded = with_halo(ensemble, (("lat", 1),), STEPS, False)
    global_rows = (
        lax.axis_index("lat") * lat_rows + jnp.arange(lat_rows + 2 * STEPS, dtype=jnp.int32) - STEPS
    )
    inside = ((global_rows >= 0) & (global_rows < lat_rows * lat_count)).astype(jnp.float32)
    for step_index in range(STEPS):
        padded = advance(padded)
        keeper = inside[step_index + 1 : inside.shape[0] - step_index - 1]
        padded = padded * keeper[None, :, None]
    blocks = padded.reshape(1, members_dev, lat_rows, lon_cells)
    received = lax.all_to_all(blocks, ("member", "lat"), split_axis=3, concat_axis=0, tiled=True)
    strip = received.reshape(member_count, lat_count, members_dev, lat_rows, width_cols)
    members = member_count * members_dev
    lat_total = lat_count * lat_rows
    states = strip.transpose(1, 3, 4, 0, 2).reshape(lat_total * width_cols, members)
    cell_index = obs_cell[0]
    obs_count = cell_index.shape[0]
    state_mean = jnp.mean(states, axis=1)
    anomaly = states - state_mean[:, None]
    spread = jnp.take(anomaly, cell_index, axis=0)
    innov = obs_value[0] - jnp.take(state_mean, cell_index)
    obs_meta = jnp.stack(
        [
            innov,
            obs_var[0],
            (cell_index // width_cols).astype(jnp.float32),
            (cell_index % width_cols).astype(jnp.float32),
        ]
    )
    near_spread = with_halo(spread, ((("member", "lat"), 0),), obs_count, True)
    near_meta = with_halo(obs_meta, ((("member", "lat"), 1),), obs_count, True)
    shifts = jnp.repeat(jnp.array([-1.0, 0.0, 1.0], jnp.float32), obs_count) * width_cols
    near_meta = jnp.concatenate([near_meta[:3], (near_meta[3] + shifts)[None, :]], axis=0)
    analysed = analyse(anomaly, state_mean, near_spread, near_meta, patch_rows[0], width_cols)
    outgoing = analysed.reshape(lat_count, lat_rows, width_cols, member_count, members_dev)
    outgoing = outgoing.transpose(3, 0, 4, 1, 2).reshape(servers, members_dev, lat_rows, width_cols)
    returned = lax.all_to_all(outgoing, ("member", "lat"), split_axis=0, concat_axis=3, tiled=True)
    return returned.reshape(members_dev, lat_rows, lon_cells)


def place(block, lats):
    half = block // (lats // 2)
    return (1 - half) * (2 * block) + half * (2 * lats - 1 - 2 * block)


def block_at(lat, lats):
    odd = lat % 2
    return (1 - odd) * (lat // 2) + odd * (lats - 1 - lat // 2)


def member_of(block, q, members):
    odd = block % 2
    return (1 - odd) * q + odd * (members - 1 - q)


def strip_at(m, lat, lats, members):
    block = block_at(lat, lats)
    return block * members + member_of(block, m, members)


def home_of(strip, lats, members):
    block = strip // members
    return member_of(block, strip % members, members), place(block, lats)


def greet_all(lats, members):
    m, lat = lax.axis_index("member"), lax.axis_index("lat")
    barrier = pltpu.get_barrier_semaphore()
    for dm in range(members):
        for dl in range(lats):
            if dm == 0 and dl == 0:
                continue
            pl.semaphore_signal(
                barrier, inc=1, device_id=((m + dm) % members, (lat + dl) % lats), device_id_type=MESH
            )
    return barrier, lats * members - 1


def split(a):
    high = a.astype(jnp.bfloat16)
    return high, (a - high.astype(jnp.float32)).astype(jnp.bfloat16)


def left_form(a):
    high, low = split(a)
    return jnp.concatenate([high, high, low], axis=1)


def put_right(ref, at, a):
    high, low = split(a)
    depth = ref.shape[0] // 3
    rows = a.shape[0]
    ref[at : at + rows] = high
    ref[depth + at : depth + at + rows] = low
    ref[2 * depth + at : 2 * depth + at + rows] = high


def dot(a, b):
    return jnp.dot(a, b, preferred_element_type=jnp.float32)


def dot_across(a, b):
    return lax.dot_general(a, b, (((1,), (1,)), ((), ())), preferred_element_type=jnp.float32)


def to_column(row):
    eye = lax.broadcasted_iota(jnp.int32, (LANES, LANES), 0) == lax.broadcasted_iota(jnp.int32, (LANES, LANES), 1)
    return jnp.concatenate(
        [
            jnp.sum(jnp.where(eye, row[:, i : i + LANES], 0.0), axis=1, keepdims=True)
            for i in range(0, row.shape[1], LANES)
        ],
        axis=0,
    )


def analysis_scratch(cells, count, near):
    f32, bf16 = jnp.float32, jnp.bfloat16
    return [
        pltpu.VMEM((near, near), f32),
        pltpu.VMEM((near, cells), f32),
        pltpu.VMEM((3 * near, count), bf16),
        pltpu.VMEM((count, near), bf16),
        pltpu.VMEM((near, 3 * near), bf16),
        pltpu.VMEM((3 * near, near), bf16),
        pltpu.VMEM((near, 3 * near), bf16),
        pltpu.VMEM((8, 3 * near, cells), bf16),
        pltpu.VMEM((7, near, cells), f32),
        pltpu.VMEM((2, cells, near), f32),
    ]


def products(work, y, at):
    common, crossed, y_right, y_turned = work[:4]
    near = y.shape[0]
    put_right(y_right, 0, y)
    yh, yl = y_right[0:near], y_right[near : 2 * near]
    ah, al = split(at)
    y_turned[...] = yh.T
    right = jnp.concatenate([yh, ah], axis=0)
    right = jnp.concatenate([right, jnp.concatenate([yl, al], axis=0), right], axis=1)
    both = dot_across(jnp.concatenate([yh, yh, yl], axis=1), right)
    common[...] = both[:, :near]
    crossed[...] = both[:, near:]


def solve_patch(dims, work, slot, spare_first, lower, upper, innov, meta):
    lats, members, chunks, rows, width, group = dims
    common, crossed, y_right, y_turned, x_left, x_right, low_left, b_right, blocks, turned = work
    count, near = y_turned.shape
    cells = crossed.shape[1]
    tile = near // 2
    tiles = range(0, near, tile)
    var, obs_rows = meta[1:2], meta[2:3]
    strip_of = lax.broadcasted_iota(jnp.int32, (1, near), 1) // (near // 3) - 1
    cols = meta[3:4] + (strip_of * width).astype(jnp.float32)
    lon_gap = jnp.maximum(jnp.maximum(-cols, cols - (width - 1.0)), 0.0) / float(width)
    lat_gap = jnp.maximum(jnp.maximum(lower - obs_rows, obs_rows - upper), 0.0) / (cells // width / 4.0)
    weights = jnp.exp(-lat_gap * lat_gap - lon_gap * lon_gap) / var
    scale = jnp.sqrt(weights)
    scale_col = to_column(scale)

    left = (y_turned[...].astype(jnp.float32) * weights).astype(jnp.bfloat16)
    gram = jnp.abs(dot(left, y_right[0:near]))
    sums = jnp.sum(gram.reshape(count // 8, 8, count), axis=0)
    bound = (count - 1.0) + jnp.max(jnp.sum(sums, axis=0, keepdims=True), axis=1, keepdims=True)
    inverse = 1.0 / bound
    alpha = (count - 1.0) * inverse
    c0 = 2.25 + alpha * (-2.4375 + alpha * (1.6875 + alpha * (-0.5625 + alpha * 0.0625)))
    c1 = -2.4375 + alpha * (3.375 + alpha * (-1.6875 + alpha * 0.25))
    c2 = 1.6875 + alpha * (-1.6875 + alpha * 0.375)
    c3 = -0.5625 + alpha * 0.25
    c4 = 0.0625

    lane = lax.broadcasted_iota(jnp.int32, (tile, cells), 1)
    spare = (1 - spare_first) * (cells - 1)
    scale_row = scale * inverse

    def x_tile(i):
        return common[i : i + tile] * scale_col[i : i + tile] * scale_row

    block, b1, b2, w, b3, u, got = range(7)

    def keep(i, which, value):
        blocks[which, i : i + tile] = value
        put_right(b_right.at[which], i, value)

    for i in tiles:
        x = x_tile(i)
        x_left[i : i + tile] = left_form(x)
        put_right(x_right, i, x)
        keep(i, block, jnp.where(lane == spare, innov[i : i + tile], crossed[i : i + tile]) * scale_col[i : i + tile])
    for i in tiles:
        x2 = dot(x_left[i : i + tile], x_right[...])
        x3 = dot(left_form(x2), x_right[...])
        low_left[i : i + tile] = left_form(c2 * x_tile(i) + c3 * x2 + c4 * x3)

    def low_on(i, which):
        return dot(low_left[i : i + tile], b_right[which])

    def x_on(i, which):
        return dot(x_left[i : i + tile], b_right[which])

    for i in tiles:
        keep(i, b1, c1 * blocks[block, i : i + tile] + low_on(i, block))
    for i in tiles:
        keep(i, b2, c0 * blocks[block, i : i + tile] + x_on(i, b1))
    for i in tiles:
        keep(i, w, c1 * blocks[b2, i : i + tile] + low_on(i, b2))
    for i in tiles:
        keep(i, b3, c0 * blocks[b2, i : i + tile] + x_on(i, w))
    for i in tiles:
        keep(i, u, c1 * blocks[b3, i : i + tile] + low_on(i, b3))
    root_scale = jnp.sqrt(alpha)
    for i in tiles:
        z = c0 * blocks[b3, i : i + tile] + x_on(i, u)
        first = blocks[b1, i : i + tile]
        value = 1.5 * first - 0.5 * (
            z + alpha * (blocks[u, i : i + tile] + c0 * (blocks[w, i : i + tile] + c0 * first))
        )
        put_right(b_right.at[got], i, value)
        turned[slot, :, i : i + tile] = (value * (scale_col[i : i + tile] * (root_scale * inverse))).T
    base = c0 * (1.5 - 0.5 * alpha * c0 * c0)
    change = None
    for i in tiles:
        full = base * blocks[block, i : i + tile] + x_on(i, got)
        drive = jnp.where(spare_first == 1, full[:, 0:1], full[:, cells - 1 : cells])
        part = jnp.sum((full * drive).reshape(tile // 8, 8, cells), axis=0)
        change = part if change is None else change + part
    return jnp.sum(change, axis=0, keepdims=True) * inverse, root_scale * base


def forecast(load, lats, group):
    fields = [load(l) for l in range(lats)]
    lane = lax.broadcasted_iota(jnp.int32, fields[0].shape, 1)
    first, last = lane < group, lane >= LANES - group
    count = fields[0].shape[0]
    zero = jnp.zeros_like(fields[0])
    for _ in range(STEPS):
        new = []
        for l in range(lats):
            c = fields[l]
            above = fields[l - 1] if l > 0 else zero
            below = fields[l + 1] if l + 1 < lats else zero
            north = pltpu.roll(jnp.where(last, above, c), group, 1)
            south = pltpu.roll(jnp.where(first, below, c), LANES - group, 1)
            east = pltpu.roll(c, count - 1, 0)
            west = pltpu.roll(c, 1, 0)
            new.append(
                c
                + lat_coeff * (north + south - 2.0 * c)
                + lon_coeff * (east + west - 2.0 * c)
                - advect_coeff * c * (east - west)
            )
        fields = new
    return fields


def swap_blocks(parts, group):
    per = len(parts)
    lane_block = lax.broadcasted_iota(jnp.int32, parts[0].shape, 1) // group
    outs = []
    for i in range(per):
        out = None
        for j in range(per):
            shift = (group * (j - i)) % LANES
            piece = pltpu.roll(parts[j], shift, 1) if shift else parts[j]
            out = piece if out is None else jnp.where(lane_block == j, piece, out)
        outs.append(out)
    return outs


def pick(onehot, values):
    total, rest = None, values
    for _ in range(3):
        term = rest.astype(jnp.bfloat16)
        part = jnp.dot(onehot, term, preferred_element_type=jnp.float32)
        total = part if total is None else total + part
        rest = rest - term.astype(jnp.float32)
    return total


def engine_kernel(
    dims, x_hbm, cell_ref, value_ref, var_ref, rows_ref, z_hbm,
    x_buf, s_buf, ra, f_buf, r_buf, xt, yt, meta, obs_out, obs_in, t_buf, at_buf,
    x_sem, a_send, a_recv, b_send, b_recv, o_send, o_recv, m_send, m_recv, y_send, y_recv, z_send, z_recv, own_sem, *work,
):
    lats, members, chunks, rows, width, group = dims
    cols = width * members
    cells = lats * rows * width
    strips = lats * members
    edge = STEPS
    m, lat = lax.axis_index("member"), lax.axis_index("lat")
    own = block_at(lat, lats)
    strip = strip_at(m, lat, lats, members)
    neighbours = [(slot, home_of((strip + side) % strips, lats, members)) for side, slot in ((1, 0), (strips - 1, 2))]

    def remote(src, dst, send, recv, to):
        return pltpu.make_async_remote_copy(
            src_ref=src, dst_ref=dst, send_sem=send, recv_sem=recv, device_id=to, device_id_type=MESH
        )

    reads = [
        pltpu.make_async_copy(x_hbm.at[pl.ds(kc * group, group)], x_buf.at[kc], x_sem.at[kc]) for kc in range(chunks)
    ]
    for read in reads:
        read.start()
    barrier, partners = greet_all(lats, members)

    obs_out[...] = jnp.zeros_like(obs_out)
    obs_out[0:1, :] = cell_ref[...].astype(jnp.float32)
    obs_out[1:2, :] = value_ref[...]
    obs_out[2:3, :] = var_ref[...]
    obs_out[3:4, 0 : rows_ref.shape[1]] = rows_ref[...].astype(jnp.float32)

    target_m, target_l = home_of(m * lats + lat, lats, members)
    away = jnp.logical_or(target_m != m, target_l != lat)
    obs_copy = remote(obs_out, obs_in, o_send, o_recv, (target_m, target_l))

    a_copies = []
    for kc in range(chunks):
        reads[kc].wait()
        whole = jnp.concatenate([x_buf[kc, :, r, :] for r in range(rows)], axis=0)
        turned = whole.T
        lon = turned.shape[0]
        for b in range(lats):
            s_buf[kc, b, 0:cols] = turned[b * cols : (b + 1) * cols]
            east, west = ((b + 1) * cols) % lon, (b * cols - edge) % lon
            s_buf[kc, b, cols : cols + edge] = turned[east : east + edge]
            s_buf[kc, b, cols + edge : cols + 2 * edge] = turned[west : west + edge]
        if kc == 0:
            pl.semaphore_wait(barrier, partners)

            @pl.when(away)
            def _():
                obs_copy.start()

            @pl.when(jnp.logical_not(away))
            def _():
                obs_in[...] = obs_out[...]

        run = []
        for d in range(1, lats):
            to = (lat + d) % lats
            copy = remote(
                s_buf.at[kc, block_at(to, lats)], ra.at[kc, lat], a_send.at[kc, d], a_recv.at[kc, d], (m, to)
            )
            copy.start()
            run.append(copy)
        a_copies.append(run)

    @pl.when(away)
    def _():
        obs_copy.wait_recv()

    cell_lane = obs_in[0:1, :]
    obs_row = jnp.floor(cell_lane * (1.0 / width))
    meta[1, 0:1, :] = obs_in[1:2, :]
    meta[1, 1:2, :] = obs_in[2:3, :]
    meta[1, 2:3, :] = obs_row
    meta[1, 3:4, :] = cell_lane - width * obs_row
    meta[1, 4:5, :] = obs_in[3:4, :]
    meta[1, 5:8, :] = jnp.zeros((3, cell_lane.shape[1]), jnp.float32)
    late = []
    for slot, to in neighbours:
        copy = remote(meta.at[1], meta.at[slot], m_send.at[slot], m_recv.at[slot], to)
        copy.start()
        late.append(copy)
    onehot = (
        to_column(cell_lane)
        == lax.broadcasted_iota(jnp.int32, (cell_lane.shape[1], cells), 1).astype(jnp.float32)
    ).astype(jnp.bfloat16)

    b_copies = []

    def arrive(kc):
        for copy in b_copies[kc]:
            copy.wait_recv()
        parts = [r_buf[j, kc].reshape(lats * width, LANES) for j in range(members)]
        for r, out in enumerate(swap_blocks(parts, group)):
            for l in range(lats):
                xt[kc, (l * rows + r) * width : (l * rows + r + 1) * width] = out[l * width : (l + 1) * width]
        yt[1, kc] = pick(onehot, xt[kc])
        for slot, to in neighbours:
            copy = remote(yt.at[1, kc], yt.at[slot, kc], y_send.at[slot, kc], y_recv.at[slot, kc], to)
            copy.start()
            late.append(copy)

    for kc in range(chunks):
        ra[kc, lat] = s_buf[kc, own]
        for copy in a_copies[kc]:
            copy.wait_recv()
        fields = forecast(lambda l, kc=kc: ra[kc, l], lats, group)
        for l in range(lats):
            for q in range(members):
                f_buf[kc, q, l] = fields[l][q * width : (q + 1) * width]
        run = []
        for d in range(1, members):
            to = (m + d) % members
            copy = remote(
                f_buf.at[kc, member_of(own, to, members)], r_buf.at[m, kc], b_send.at[kc, d], b_recv.at[kc, d], (to, lat)
            )
            copy.start()
            run.append(copy)
        b_copies.append(run)
        r_buf[m, kc] = f_buf[kc, member_of(own, m, members)]
        if kc:
            arrive(kc - 1)
    arrive(chunks - 1)

    states = jnp.concatenate([xt[kc] for kc in range(chunks)], axis=1)
    mean = jnp.sum(states, axis=1, keepdims=True) * (1.0 / states.shape[1])
    at = states - mean
    at_buf[...] = at
    for copy in late:
        copy.wait_recv()
    y_raw = jnp.concatenate(
        [jnp.concatenate([yt[slot, kc] for kc in range(chunks)], axis=1) for slot in range(3)], axis=0
    )
    y_mean = jnp.sum(y_raw, axis=1, keepdims=True) * (1.0 / y_raw.shape[1])
    all_meta = jnp.concatenate([meta[slot] for slot in range(3)], axis=1)
    innov = to_column(all_meta[0:1]) - y_mean
    products(work, y_raw - y_mean, at)
    y_right, turned = work[2], work[9]

    nobs = cell_lane.shape[1]
    sure = lats // 4
    rest = lats - sure
    last = 1 - lat // (lats // 2)
    lasts = last.astype(jnp.float32)
    first_len = all_meta[4:5, nobs : nobs + 1]
    second_len = all_meta[4:5, nobs + 1 : nobs + 2]
    spans = []
    for which in (lasts, 1.0 - lasts):
        lower = which * first_len
        spans.append((lower, lower + (first_len + which * (second_len - first_len)) - 1.0))

    def finish(tile, tiles, pick_cells, weights, change, factor):
        begin = tile * (rows * width)
        span = pl.ds(pl.multiple_of(begin, rows * width), tiles * rows * width)
        out = pick_cells(mean) + change + factor * at_buf[span, :] + dot(left_form(weights), y_right[...])
        for kc in range(chunks):
            lanes = out[:, kc * LANES : (kc + 1) * LANES]
            parts = [
                jnp.concatenate(
                    [lanes[(l * rows + r) * width : (l * rows + r + 1) * width] for l in range(tiles)], axis=0
                )
                for r in range(rows)
            ]
            for j, piece in enumerate(swap_blocks(parts, group)):
                for l in range(tiles):
                    t_buf[j, tile + l, kc] = piece[l * width : (l + 1) * width]

    def give(to):
        copy = remote(t_buf.at[to[0], to[1]], z_hbm.at[strip], z_send.at[len(z_copies)], z_recv.at[strip], to)
        copy.start()
        z_copies.append(copy)

    z_copies = []
    cut, tail = sure * rows * width, rest * rows * width
    early = last * rest
    change, factor = solve_patch(dims, work, 0, last, *spans[0], innov, all_meta)
    change_col = to_column(change)

    def far(column):
        return jnp.where(last == 1, column[tail:], column[:cut])

    def near(column):
        return jnp.where(last == 1, column[:tail], column[cut:])

    finish(early, sure, far, far(turned[0]), far(change_col), factor)
    for l in range(sure):
        for dm in range(members):
            give(((m + dm) % members, early + l))

    change2, factor2 = solve_patch(dims, work, 1, 1 - last, *spans[1], innov, all_meta)
    cell_row = (lax.broadcasted_iota(jnp.int32, (cells, 1), 0) // width).astype(jnp.float32)
    inside = near(jnp.logical_and(cell_row >= spans[0][0], cell_row <= spans[0][1]).astype(jnp.float32)) > 0.5
    base = (1 - last) * sure
    finish(
        base,
        rest,
        near,
        jnp.where(inside, near(turned[0]), near(turned[1])),
        jnp.where(inside, near(change_col), near(to_column(change2))),
        jnp.where(inside, factor, factor2),
    )
    for j in range(rest - 1):
        for dm in range(members):
            give(((m + dm) % members, base + (lat - base + 1 + j) % rest))
    for dm in range(1, members):
        give(((m + dm) % members, lat))
    kept = pltpu.make_async_copy(t_buf.at[m, lat], z_hbm.at[strip], own_sem)
    kept.start()

    for run in a_copies + b_copies + [late]:
        for copy in run:
            copy.wait_send()

    @pl.when(away)
    def _():
        obs_copy.wait_send()

    kept.wait()
    for copy in z_copies:
        copy.wait_send()
    for d in range(1, strips):
        other = (strip + d) % strips
        remote(
            t_buf.at[0, 0], z_hbm.at[other], z_send.at[0], z_recv.at[other], ((m + 1) % members, lat)
        ).wait_recv()


def engine(ensemble, obs_cell, obs_value, obs_var, patch_rows, dims):
    lats, members, chunks, rows, width, group = dims
    cells = lats * rows * width
    nobs = obs_cell.shape[1]
    strips = lats * members
    dma, f32 = pltpu.SemaphoreType.DMA, jnp.float32
    vmem, anywhere = pl.BlockSpec(memory_space=pltpu.VMEM), pl.BlockSpec(memory_space=pl.ANY)
    block = (chunks, lats, members * width + 2 * STEPS, LANES)
    return pl.pallas_call(
        functools.partial(engine_kernel, dims),
        out_shape=jax.ShapeDtypeStruct((strips, chunks, width, LANES), f32),
        in_specs=[anywhere, vmem, vmem, vmem, vmem],
        out_specs=anywhere,
        scratch_shapes=[
            pltpu.VMEM((chunks, group, rows, strips * width), f32),
            pltpu.VMEM(block, f32),
            pltpu.VMEM(block, f32),
            pltpu.VMEM((chunks, members, lats, width, LANES), f32),
            pltpu.VMEM((members, chunks, lats, width, LANES), f32),
            pltpu.VMEM((chunks, cells, LANES), f32),
            pltpu.VMEM((3, chunks, nobs, LANES), f32),
            pltpu.VMEM((3, 8, nobs), f32),
            pltpu.VMEM((8, nobs), f32),
            pltpu.VMEM((8, nobs), f32),
            pltpu.VMEM((members, lats, chunks, width, LANES), f32),
            pltpu.VMEM((cells, members * chunks * group), f32),
            dma((chunks,)),
            dma((chunks, lats)),
            dma((chunks, lats)),
            dma((chunks, members)),
            dma((chunks, members)),
            dma,
            dma,
            dma((3,)),
            dma((3,)),
            dma((3, chunks)),
            dma((3, chunks)),
            dma((strips,)),
            dma((strips,)),
            dma,
        ]
        + analysis_scratch(cells, members * chunks * group, 3 * nobs),
        compiler_params=pltpu.CompilerParams(
            collective_id=0, has_side_effects=True, vmem_limit_bytes=56 * 1024 * 1024
        ),
        name="engine",
    )(ensemble, obs_cell, obs_value, obs_var, patch_rows)


def settle_kernel(dims, z_ref, out_ref):
    lats, members, chunks, rows, width, group = dims
    turned = z_ref[...].reshape(lats * members * width, LANES).T
    for r in range(rows):
        out_ref[:, r, :] = turned[r * group : (r + 1) * group]


def settle(pieces, dims):
    lats, members, chunks, rows, width, group = dims
    strips = lats * members
    return pl.pallas_call(
        functools.partial(settle_kernel, dims),
        grid=(chunks,),
        out_shape=jax.ShapeDtypeStruct((chunks * group, rows, strips * width), jnp.float32),
        in_specs=[pl.BlockSpec((strips, None, width, LANES), lambda kc: (0, kc, 0, 0))],
        out_specs=pl.BlockSpec((group, rows, strips * width), lambda kc: (kc, 0, 0)),
        name="settle",
    )(pieces)


def kernel_device(dims, ensemble, obs_cell, obs_value, obs_var, patch_rows):
    return settle(engine(ensemble, obs_cell, obs_value, obs_var, patch_rows, dims), dims)


def kernel_dims(mesh, ensemble, obs_cell, patch_rows):
    lats, members = mesh.shape["lat"], mesh.shape["member"]
    total, lat_all, lon = ensemble.shape
    own, rows = total // members, lat_all // lats
    width = lon // (lats * members)
    if LANES % rows:
        return None
    group = LANES // rows
    fits = (
        own % group == 0
        and (members * (own // group)) % rows == 0
        and width == 8
        and lats % 4 == 0
        and members % 2 == 0
        and obs_cell.shape[1] % LANES == 0
        and patch_rows.shape[1] == 2
    )
    return (lats, members, own // group, rows, width, group) if fits else None


def solution(mesh):
    specs = (P("member", "lat", None),) + (P(("member", "lat"), None),) * 4

    def run(ensemble, obs_cell, obs_value, obs_var, patch_rows):
        dims = kernel_dims(mesh, ensemble, obs_cell, patch_rows)
        body = general_device if dims is None else functools.partial(kernel_device, dims)
        mapped = jax.shard_map(
            body, mesh=mesh, in_specs=specs, out_specs=P("member", "lat", None), check_vma=False
        )
        return mapped(ensemble, obs_cell, obs_value, obs_var, patch_rows)

    return run
```

```python
import functools

import jax
import jax.numpy as jnp
from jax import lax
from jax.experimental import pallas as pl
from jax.experimental.pallas import tpu as pltpu
from jax.sharding import PartitionSpec as P

STEPS = 4

lat_coeff = 0.4
lon_coeff = 0.05
advect_coeff = 0.1

MESH = pl.DeviceIdType.MESH
LANES = 128


def with_halo(value, sides, width, wrap):
    for axis, dim in sides:
        size, length = (lax.axis_size(axis), value.shape[dim])
        up = [(i, (i + 1) % size) for i in range(size if wrap else size - 1)]
        down = [(j, i) for i, j in up]
        last = lax.slice_in_dim(value, length - width, length, axis=dim)
        initial = lax.slice_in_dim(value, 0, width, axis=dim)
        before = lax.ppermute(last, axis, up)
        after = lax.ppermute(initial, axis, down)
        value = jnp.concatenate([before, value, after], axis=dim)
    return value


def advance(padded):
    centre = padded[:, 1:-1]
    northern = padded[:, :-2]
    southern = padded[:, 2:]
    eastern = jnp.roll(centre, -1, axis=2)
    western = jnp.roll(centre, 1, axis=2)
    return (
        centre
        + lat_coeff * (northern + southern - 2.0 * centre)
        + lon_coeff * (eastern + western - 2.0 * centre)
        - advect_coeff * centre * (eastern - western)
    )


def localize(obs_rows, rel_cols, first_row, row_count, lat_scale, width_cols):
    lower = first_row.astype(jnp.float32)
    upper = lower + row_count.astype(jnp.float32) - 1.0
    lat_gap = jnp.maximum(jnp.maximum(lower - obs_rows, obs_rows - upper), 0.0) / lat_scale
    lon_gap = jnp.maximum(jnp.maximum(-rel_cols, rel_cols - (width_cols - 1.0)), 0.0) / width_cols
    return jnp.exp(-lat_gap * lat_gap - lon_gap * lon_gap)


def dot3(left, right):
    return jnp.matmul(left, right, precision=lax.Precision.HIGH, preferred_element_type=jnp.float32)


def analyse(anomaly, state_mean, spread, obs_meta, lengths, width_cols):
    cell_total, members = anomaly.shape
    lat_total = cell_total // width_cols
    near = spread.shape[0]
    starts = jnp.cumsum(lengths) - lengths
    cell_rows = jnp.arange(cell_total, dtype=jnp.int32) // width_cols
    identity = jnp.eye(members, dtype=jnp.float32)
    products = dot3(spread, jnp.concatenate([spread, anomaly], axis=0).T)
    common, crossed = products[:, :near], products[:, near:]
    innov = obs_meta[0]
    shrink = jnp.zeros((cell_total,), jnp.float32)
    shift = state_mean
    weights_all = jnp.zeros((near, cell_total), jnp.float32)
    for patch in range(lengths.shape[0]):
        weights = (
            localize(obs_meta[2], obs_meta[3], starts[patch], lengths[patch], lat_total / 4.0, float(width_cols))
            / obs_meta[1]
        )
        scale = jnp.sqrt(weights)
        gram_matrix = (members - 1.0) * identity + jnp.dot(
            (spread * weights[:, None]).T, spread, preferred_element_type=jnp.float32
        )
        bound = jnp.max(jnp.sum(jnp.abs(gram_matrix), axis=1))
        alpha = (members - 1.0) / bound
        x = common * scale[:, None] * (scale / bound)[None, :]
        c0 = 2.25 + alpha * (-2.4375 + alpha * (1.6875 + alpha * (-0.5625 + alpha * 0.0625)))
        c1 = -2.4375 + alpha * (3.375 + alpha * (-1.6875 + alpha * 0.25))
        c2 = 1.6875 + alpha * (-1.6875 + alpha * 0.375)
        c3 = -0.5625 + alpha * 0.25
        c4 = 0.0625
        x2 = dot3(x, x)
        x34 = dot3(x2, jnp.concatenate([x, x2], axis=1))
        x3, x4 = x34[:, :near], x34[:, near:]
        low = c2 * x + c3 * x2 + c4 * x3
        high = c1 * x + c2 * x2 + c3 * x3 + c4 * x4
        block = jnp.concatenate([crossed * scale[:, None], (scale * innov)[:, None]], axis=1)
        both = dot3(jnp.concatenate([low, high], axis=0), block)
        b1 = c1 * block + both[:near]
        b2 = c0 * block + both[near:]
        b3 = c0 * b2 + dot3(high, b2)
        mixed = alpha * c0 * b1 + b3
        got = 1.5 * b1 - 0.5 * (
            alpha * c0 * c0 * b1
            + c0 * mixed
            + dot3(high, mixed)
            + alpha * (c1 * b3 + dot3(low, b3))
        )
        base = c0 * (1.5 - 0.5 * alpha * c0 * c0)
        driven = base * block[:, -1] + jnp.sum(x * got[:, -1][None, :], axis=1)
        again = jnp.sum(x * driven[None, :], axis=1)
        mean_part = (
            jnp.sum(block[:, :-1] * (base * driven)[:, None] + got[:, :-1] * again[:, None], axis=0)
            / bound
        )
        cell_mask = (cell_rows >= starts[patch]) & (cell_rows < starts[patch] + lengths[patch])
        root_scale = jnp.sqrt((members - 1.0) / bound)
        shift = shift + jnp.where(cell_mask, mean_part, 0.0)
        shrink = jnp.where(cell_mask, root_scale * base, shrink)
        weights_all = jnp.where(
            cell_mask[None, :], got[:, :-1] * (scale * (root_scale / bound))[:, None], weights_all
        )
    return shift[:, None] + shrink[:, None] * anomaly + dot3(weights_all.T, spread)


def general_device(ensemble, obs_cell, obs_value, obs_var, patch_rows):
    members_dev, lat_rows, lon_cells = ensemble.shape
    lat_count = lax.axis_size("lat")
    member_count = lax.axis_size("member")
    servers = lat_count * member_count
    width_cols = lon_cells // servers
    padded = with_halo(ensemble, (("lat", 1),), STEPS, False)
    global_rows = (
        lax.axis_index("lat") * lat_rows + jnp.arange(lat_rows + 2 * STEPS, dtype=jnp.int32) - STEPS
    )
    inside = ((global_rows >= 0) & (global_rows < lat_rows * lat_count)).astype(jnp.float32)
    for step_index in range(STEPS):
        padded = advance(padded)
        keeper = inside[step_index + 1 : inside.shape[0] - step_index - 1]
        padded = padded * keeper[None, :, None]
    blocks = padded.reshape(1, members_dev, lat_rows, lon_cells)
    received = lax.all_to_all(blocks, ("member", "lat"), split_axis=3, concat_axis=0, tiled=True)
    strip = received.reshape(member_count, lat_count, members_dev, lat_rows, width_cols)
    members = member_count * members_dev
    lat_total = lat_count * lat_rows
    states = strip.transpose(1, 3, 4, 0, 2).reshape(lat_total * width_cols, members)
    cell_index = obs_cell[0]
    obs_count = cell_index.shape[0]
    state_mean = jnp.mean(states, axis=1)
    anomaly = states - state_mean[:, None]
    spread = jnp.take(anomaly, cell_index, axis=0)
    innov = obs_value[0] - jnp.take(state_mean, cell_index)
    obs_meta = jnp.stack(
        [
            innov,
            obs_var[0],
            (cell_index // width_cols).astype(jnp.float32),
            (cell_index % width_cols).astype(jnp.float32),
        ]
    )
    near_spread = with_halo(spread, ((("member", "lat"), 0),), obs_count, True)
    near_meta = with_halo(obs_meta, ((("member", "lat"), 1),), obs_count, True)
    shifts = jnp.repeat(jnp.array([-1.0, 0.0, 1.0], jnp.float32), obs_count) * width_cols
    near_meta = jnp.concatenate([near_meta[:3], (near_meta[3] + shifts)[None, :]], axis=0)
    analysed = analyse(anomaly, state_mean, near_spread, near_meta, patch_rows[0], width_cols)
    outgoing = analysed.reshape(lat_count, lat_rows, width_cols, member_count, members_dev)
    outgoing = outgoing.transpose(3, 0, 4, 1, 2).reshape(servers, members_dev, lat_rows, width_cols)
    returned = lax.all_to_all(outgoing, ("member", "lat"), split_axis=0, concat_axis=3, tiled=True)
    return returned.reshape(members_dev, lat_rows, lon_cells)


def place(block, lats):
    half = block // (lats // 2)
    return (1 - half) * (2 * block) + half * (2 * lats - 1 - 2 * block)


def block_at(lat, lats):
    odd = lat % 2
    return (1 - odd) * (lat // 2) + odd * (lats - 1 - lat // 2)


def member_of(block, q, members):
    odd = block % 2
    return (1 - odd) * q + odd * (members - 1 - q)


def strip_at(m, lat, lats, members):
    block = block_at(lat, lats)
    return block * members + member_of(block, m, members)


def home_of(strip, lats, members):
    block = strip // members
    return member_of(block, strip % members, members), place(block, lats)


def greet_all(lats, members):
    m, lat = lax.axis_index("member"), lax.axis_index("lat")
    barrier = pltpu.get_barrier_semaphore()
    for dm in range(members):
        for dl in range(lats):
            if dm == 0 and dl == 0:
                continue
            pl.semaphore_signal(
                barrier, inc=1, device_id=((m + dm) % members, (lat + dl) % lats), device_id_type=MESH
            )
    return barrier, lats * members - 1


def split(a):
    high = a.astype(jnp.bfloat16)
    return high, (a - high.astype(jnp.float32)).astype(jnp.bfloat16)


def left_form(a):
    high, low = split(a)
    return jnp.concatenate([high, high, low], axis=1)


def put_right(ref, at, a):
    high, low = split(a)
    depth = ref.shape[0] // 3
    rows = a.shape[0]
    ref[at : at + rows] = high
    ref[depth + at : depth + at + rows] = low
    ref[2 * depth + at : 2 * depth + at + rows] = high


def dot(a, b):
    return jnp.dot(a, b, preferred_element_type=jnp.float32)


def dot_across(a, b):
    return lax.dot_general(a, b, (((1,), (1,)), ((), ())), preferred_element_type=jnp.float32)


def to_column(row):
    eye = lax.broadcasted_iota(jnp.int32, (LANES, LANES), 0) == lax.broadcasted_iota(jnp.int32, (LANES, LANES), 1)
    return jnp.concatenate(
        [
            jnp.sum(jnp.where(eye, row[:, i : i + LANES], 0.0), axis=1, keepdims=True)
            for i in range(0, row.shape[1], LANES)
        ],
        axis=0,
    )


def analysis_scratch(cells, count, near):
    f32, bf16 = jnp.float32, jnp.bfloat16
    return [
        pltpu.VMEM((near, near), f32),
        pltpu.VMEM((near, cells), f32),
        pltpu.VMEM((3 * near, count), bf16),
        pltpu.VMEM((count, near), bf16),
        pltpu.VMEM((near, 3 * near), bf16),
        pltpu.VMEM((3 * near, near), bf16),
        pltpu.VMEM((near, 3 * near), bf16),
        pltpu.VMEM((8, 3 * near, cells), bf16),
        pltpu.VMEM((7, near, cells), f32),
        pltpu.VMEM((2, cells, near), f32),
    ]


def products(work, y, at):
    common, crossed, y_right, y_turned = work[:4]
    near = y.shape[0]
    put_right(y_right, 0, y)
    yh, yl = y_right[0:near], y_right[near : 2 * near]
    ah, al = split(at)
    y_turned[...] = yh.T
    right = jnp.concatenate([yh, ah], axis=0)
    right = jnp.concatenate([right, jnp.concatenate([yl, al], axis=0), right], axis=1)
    both = dot_across(jnp.concatenate([yh, yh, yl], axis=1), right)
    common[...] = both[:, :near]
    crossed[...] = both[:, near:]


def solve_patch(dims, work, slot, spare_first, lower, upper, innov, meta):
    lats, members, chunks, rows, width, group = dims
    common, crossed, y_right, y_turned, x_left, x_right, low_left, b_right, blocks, turned = work
    count, near = y_turned.shape
    cells = crossed.shape[1]
    tile = near // 2
    tiles = range(0, near, tile)
    var, obs_rows = meta[1:2], meta[2:3]
    strip_of = lax.broadcasted_iota(jnp.int32, (1, near), 1) // (near // 3) - 1
    cols = meta[3:4] + (strip_of * width).astype(jnp.float32)
    lon_gap = jnp.maximum(jnp.maximum(-cols, cols - (width - 1.0)), 0.0) / float(width)
    lat_gap = jnp.maximum(jnp.maximum(lower - obs_rows, obs_rows - upper), 0.0) / (cells // width / 4.0)
    weights = jnp.exp(-lat_gap * lat_gap - lon_gap * lon_gap) / var
    scale = jnp.sqrt(weights)
    scale_col = to_column(scale)

    left = (y_turned[...].astype(jnp.float32) * weights).astype(jnp.bfloat16)
    gram = jnp.abs(dot(left, y_right[0:near]))
    sums = jnp.sum(gram.reshape(count // 8, 8, count), axis=0)
    bound = (count - 1.0) + jnp.max(jnp.sum(sums, axis=0, keepdims=True), axis=1, keepdims=True)
    inverse = 1.0 / bound
    alpha = (count - 1.0) * inverse
    c0 = 2.25 + alpha * (-2.4375 + alpha * (1.6875 + alpha * (-0.5625 + alpha * 0.0625)))
    c1 = -2.4375 + alpha * (3.375 + alpha * (-1.6875 + alpha * 0.25))
    c2 = 1.6875 + alpha * (-1.6875 + alpha * 0.375)
    c3 = -0.5625 + alpha * 0.25
    c4 = 0.0625

    lane = lax.broadcasted_iota(jnp.int32, (tile, cells), 1)
    spare = (1 - spare_first) * (cells - 1)
    scale_row = scale * inverse

    def x_tile(i):
        return common[i : i + tile] * scale_col[i : i + tile] * scale_row

    block, b1, b2, w, b3, u, got = range(7)

    def keep(i, which, value):
        blocks[which, i : i + tile] = value
        put_right(b_right.at[which], i, value)

    for i in tiles:
        x = x_tile(i)
        x_left[i : i + tile] = left_form(x)
        put_right(x_right, i, x)
        keep(i, block, jnp.where(lane == spare, innov[i : i + tile], crossed[i : i + tile]) * scale_col[i : i + tile])
    for i in tiles:
        x2 = dot(x_left[i : i + tile], x_right[...])
        x3 = dot(left_form(x2), x_right[...])
        low_left[i : i + tile] = left_form(c2 * x_tile(i) + c3 * x2 + c4 * x3)

    def low_on(i, which):
        return dot(low_left[i : i + tile], b_right[which])

    def x_on(i, which):
        return dot(x_left[i : i + tile], b_right[which])

    for i in tiles:
        keep(i, b1, c1 * blocks[block, i : i + tile] + low_on(i, block))
    for i in tiles:
        keep(i, b2, c0 * blocks[block, i : i + tile] + x_on(i, b1))
    for i in tiles:
        keep(i, w, c1 * blocks[b2, i : i + tile] + low_on(i, b2))
    for i in tiles:
        keep(i, b3, c0 * blocks[b2, i : i + tile] + x_on(i, w))
    for i in tiles:
        keep(i, u, c1 * blocks[b3, i : i + tile] + low_on(i, b3))
    root_scale = jnp.sqrt(alpha)
    for i in tiles:
        z = c0 * blocks[b3, i : i + tile] + x_on(i, u)
        first = blocks[b1, i : i + tile]
        value = 1.5 * first - 0.5 * (
            z + alpha * (blocks[u, i : i + tile] + c0 * (blocks[w, i : i + tile] + c0 * first))
        )
        put_right(b_right.at[got], i, value)
        turned[slot, :, i : i + tile] = (value * (scale_col[i : i + tile] * (root_scale * inverse))).T
    base = c0 * (1.5 - 0.5 * alpha * c0 * c0)
    change = None
    for i in tiles:
        full = base * blocks[block, i : i + tile] + x_on(i, got)
        drive = jnp.where(spare_first == 1, full[:, 0:1], full[:, cells - 1 : cells])
        part = jnp.sum((full * drive).reshape(tile // 8, 8, cells), axis=0)
        change = part if change is None else change + part
    return jnp.sum(change, axis=0, keepdims=True) * inverse, root_scale * base


def forecast(load, lats, group):
    fields = [load(l) for l in range(lats)]
    lane = lax.broadcasted_iota(jnp.int32, fields[0].shape, 1)
    first, last = lane < group, lane >= LANES - group
    count = fields[0].shape[0]
    zero = jnp.zeros_like(fields[0])
    for _ in range(STEPS):
        new = []
        for l in range(lats):
            c = fields[l]
            above = fields[l - 1] if l > 0 else zero
            below = fields[l + 1] if l + 1 < lats else zero
            north = pltpu.roll(jnp.where(last, above, c), group, 1)
            south = pltpu.roll(jnp.where(first, below, c), LANES - group, 1)
            east = pltpu.roll(c, count - 1, 0)
            west = pltpu.roll(c, 1, 0)
            new.append(
                c
                + lat_coeff * (north + south - 2.0 * c)
                + lon_coeff * (east + west - 2.0 * c)
                - advect_coeff * c * (east - west)
            )
        fields = new
    return fields


def swap_blocks(parts, group):
    per = len(parts)
    lane_block = lax.broadcasted_iota(jnp.int32, parts[0].shape, 1) // group
    outs = []
    for i in range(per):
        out = None
        for j in range(per):
            shift = (group * (j - i)) % LANES
            piece = pltpu.roll(parts[j], shift, 1) if shift else parts[j]
            out = piece if out is None else jnp.where(lane_block == j, piece, out)
        outs.append(out)
    return outs


def pick(onehot, values):
    total, rest = None, values
    for _ in range(3):
        term = rest.astype(jnp.bfloat16)
        part = jnp.dot(onehot, term, preferred_element_type=jnp.float32)
        total = part if total is None else total + part
        rest = rest - term.astype(jnp.float32)
    return total


def engine_kernel(
    dims, x_hbm, cell_ref, value_ref, var_ref, rows_ref, z_hbm,
    x_buf, s_buf, ra, f_buf, r_buf, xt, yt, meta, obs_out, obs_in, t_buf, at_buf,
    x_sem, a_send, a_recv, b_send, b_recv, o_send, o_recv, m_send, m_recv, y_send, y_recv, z_send, z_recv, own_sem, *work,
):
    lats, members, chunks, rows, width, group = dims
    cols = width * members
    cells = lats * rows * width
    strips = lats * members
    edge = STEPS
    m, lat = lax.axis_index("member"), lax.axis_index("lat")
    own = block_at(lat, lats)
    strip = strip_at(m, lat, lats, members)
    neighbours = [(slot, home_of((strip + side) % strips, lats, members)) for side, slot in ((1, 0), (strips - 1, 2))]

    def remote(src, dst, send, recv, to):
        return pltpu.make_async_remote_copy(
            src_ref=src, dst_ref=dst, send_sem=send, recv_sem=recv, device_id=to, device_id_type=MESH
        )

    reads = [
        pltpu.make_async_copy(x_hbm.at[pl.ds(kc * group, group)], x_buf.at[kc], x_sem.at[kc]) for kc in range(chunks)
    ]
    for read in reads:
        read.start()
    barrier, partners = greet_all(lats, members)

    obs_out[...] = jnp.zeros_like(obs_out)
    obs_out[0:1, :] = cell_ref[...].astype(jnp.float32)
    obs_out[1:2, :] = value_ref[...]
    obs_out[2:3, :] = var_ref[...]
    obs_out[3:4, 0 : rows_ref.shape[1]] = rows_ref[...].astype(jnp.float32)

    target_m, target_l = home_of(m * lats + lat, lats, members)
    away = jnp.logical_or(target_m != m, target_l != lat)
    obs_copy = remote(obs_out, obs_in, o_send, o_recv, (target_m, target_l))

    a_copies = []
    for kc in range(chunks):
        reads[kc].wait()
        whole = jnp.concatenate([x_buf[kc, :, r, :] for r in range(rows)], axis=0)
        turned = whole.T
        lon = turned.shape[0]
        for b in range(lats):
            s_buf[kc, b, 0:cols] = turned[b * cols : (b + 1) * cols]
            east, west = ((b + 1) * cols) % lon, (b * cols - edge) % lon
            s_buf[kc, b, cols : cols + edge] = turned[east : east + edge]
            s_buf[kc, b, cols + edge : cols + 2 * edge] = turned[west : west + edge]
        if kc == 0:
            pl.semaphore_wait(barrier, partners)

            @pl.when(away)
            def _():
                obs_copy.start()

            @pl.when(jnp.logical_not(away))
            def _():
                obs_in[...] = obs_out[...]

        run = []
        for d in range(1, lats):
            to = (lat + d) % lats
            copy = remote(
                s_buf.at[kc, block_at(to, lats)], ra.at[kc, lat], a_send.at[kc, d], a_recv.at[kc, d], (m, to)
            )
            copy.start()
            run.append(copy)
        a_copies.append(run)

    @pl.when(away)
    def _():
        obs_copy.wait_recv()

    cell_lane = obs_in[0:1, :]
    obs_row = jnp.floor(cell_lane * (1.0 / width))
    meta[1, 0:1, :] = obs_in[1:2, :]
    meta[1, 1:2, :] = obs_in[2:3, :]
    meta[1, 2:3, :] = obs_row
    meta[1, 3:4, :] = cell_lane - width * obs_row
    meta[1, 4:5, :] = obs_in[3:4, :]
    meta[1, 5:8, :] = jnp.zeros((3, cell_lane.shape[1]), jnp.float32)
    late = []
    for slot, to in neighbours:
        copy = remote(meta.at[1], meta.at[slot], m_send.at[slot], m_recv.at[slot], to)
        copy.start()
        late.append(copy)
    onehot = (
        to_column(cell_lane)
        == lax.broadcasted_iota(jnp.int32, (cell_lane.shape[1], cells), 1).astype(jnp.float32)
    ).astype(jnp.bfloat16)

    b_copies = []

    def arrive(kc):
        for copy in b_copies[kc]:
            copy.wait_recv()
        parts = [r_buf[j, kc].reshape(lats * width, LANES) for j in range(members)]
        for r, out in enumerate(swap_blocks(parts, group)):
            for l in range(lats):
                xt[kc, (l * rows + r) * width : (l * rows + r + 1) * width] = out[l * width : (l + 1) * width]
        yt[1, kc] = pick(onehot, xt[kc])
        for slot, to in neighbours:
            copy = remote(yt.at[1, kc], yt.at[slot, kc], y_send.at[slot, kc], y_recv.at[slot, kc], to)
            copy.start()
            late.append(copy)

    for kc in range(chunks):
        ra[kc, lat] = s_buf[kc, own]
        for copy in a_copies[kc]:
            copy.wait_recv()
        fields = forecast(lambda l, kc=kc: ra[kc, l], lats, group)
        for l in range(lats):
            for q in range(members):
                f_buf[kc, q, l] = fields[l][q * width : (q + 1) * width]
        run = []
        for d in range(1, members):
            to = (m + d) % members
            copy = remote(
                f_buf.at[kc, member_of(own, to, members)], r_buf.at[m, kc], b_send.at[kc, d], b_recv.at[kc, d], (to, lat)
            )
            copy.start()
            run.append(copy)
        b_copies.append(run)
        r_buf[m, kc] = f_buf[kc, member_of(own, m, members)]
        if kc:
            arrive(kc - 1)
    arrive(chunks - 1)

    states = jnp.concatenate([xt[kc] for kc in range(chunks)], axis=1)
    mean = jnp.sum(states, axis=1, keepdims=True) * (1.0 / states.shape[1])
    at = states - mean
    at_buf[...] = at
    for copy in late:
        copy.wait_recv()
    y_raw = jnp.concatenate(
        [jnp.concatenate([yt[slot, kc] for kc in range(chunks)], axis=1) for slot in range(3)], axis=0
    )
    y_mean = jnp.sum(y_raw, axis=1, keepdims=True) * (1.0 / y_raw.shape[1])
    all_meta = jnp.concatenate([meta[slot] for slot in range(3)], axis=1)
    innov = to_column(all_meta[0:1]) - y_mean
    products(work, y_raw - y_mean, at)
    y_right, turned = work[2], work[9]

    nobs = cell_lane.shape[1]
    sure = lats // 4
    rest = lats - sure
    last = 1 - lat // (lats // 2)
    lasts = last.astype(jnp.float32)
    first_len = all_meta[4:5, nobs : nobs + 1]
    second_len = all_meta[4:5, nobs + 1 : nobs + 2]
    spans = []
    for which in (lasts, 1.0 - lasts):
        lower = which * first_len
        spans.append((lower, lower + (first_len + which * (second_len - first_len)) - 1.0))

    def finish(tile, tiles, pick_cells, weights, change, factor):
        begin = tile * (rows * width)
        span = pl.ds(pl.multiple_of(begin, rows * width), tiles * rows * width)
        out = pick_cells(mean) + change + factor * at_buf[span, :] + dot(left_form(weights), y_right[...])
        for kc in range(chunks):
            lanes = out[:, kc * LANES : (kc + 1) * LANES]
            parts = [
                jnp.concatenate(
                    [lanes[(l * rows + r) * width : (l * rows + r + 1) * width] for l in range(tiles)], axis=0
                )
                for r in range(rows)
            ]
            for j, piece in enumerate(swap_blocks(parts, group)):
                for l in range(tiles):
                    t_buf[j, tile + l, kc] = piece[l * width : (l + 1) * width]

    def give(to):
        copy = remote(t_buf.at[to[0], to[1]], z_hbm.at[strip], z_send.at[len(z_copies)], z_recv.at[strip], to)
        copy.start()
        z_copies.append(copy)

    z_copies = []
    cut, tail = sure * rows * width, rest * rows * width
    early = last * rest
    change, factor = solve_patch(dims, work, 0, last, *spans[0], innov, all_meta)
    change_col = to_column(change)

    def far(column):
        return jnp.where(last == 1, column[tail:], column[:cut])

    def near(column):
        return jnp.where(last == 1, column[:tail], column[cut:])

    finish(early, sure, far, far(turned[0]), far(change_col), factor)
    for l in range(sure):
        for dm in range(members):
            give(((m + dm) % members, early + l))

    change2, factor2 = solve_patch(dims, work, 1, 1 - last, *spans[1], innov, all_meta)
    cell_row = (lax.broadcasted_iota(jnp.int32, (cells, 1), 0) // width).astype(jnp.float32)
    inside = near(jnp.logical_and(cell_row >= spans[0][0], cell_row <= spans[0][1]).astype(jnp.float32)) > 0.5
    base = (1 - last) * sure
    finish(
        base,
        rest,
        near,
        jnp.where(inside, near(turned[0]), near(turned[1])),
        jnp.where(inside, near(change_col), near(to_column(change2))),
        jnp.where(inside, factor, factor2),
    )
    for j in range(rest - 1):
        for dm in range(members):
            give(((m + dm) % members, base + (lat - base + 1 + j) % rest))
    for dm in range(1, members):
        give(((m + dm) % members, lat))
    kept = pltpu.make_async_copy(t_buf.at[m, lat], z_hbm.at[strip], own_sem)
    kept.start()

    for run in a_copies + b_copies + [late]:
        for copy in run:
            copy.wait_send()

    @pl.when(away)
    def _():
        obs_copy.wait_send()

    kept.wait()
    for copy in z_copies:
        copy.wait_send()
    for d in range(1, strips):
        other = (strip + d) % strips
        remote(
            t_buf.at[0, 0], z_hbm.at[other], z_send.at[0], z_recv.at[other], ((m + 1) % members, lat)
        ).wait_recv()


def engine(ensemble, obs_cell, obs_value, obs_var, patch_rows, dims):
    lats, members, chunks, rows, width, group = dims
    cells = lats * rows * width
    nobs = obs_cell.shape[1]
    strips = lats * members
    dma, f32 = pltpu.SemaphoreType.DMA, jnp.float32
    vmem, anywhere = pl.BlockSpec(memory_space=pltpu.VMEM), pl.BlockSpec(memory_space=pl.ANY)
    block = (chunks, lats, members * width + 2 * STEPS, LANES)
    return pl.pallas_call(
        functools.partial(engine_kernel, dims),
        out_shape=jax.ShapeDtypeStruct((strips, chunks, width, LANES), f32),
        in_specs=[anywhere, vmem, vmem, vmem, vmem],
        out_specs=anywhere,
        scratch_shapes=[
            pltpu.VMEM((chunks, group, rows, strips * width), f32),
            pltpu.VMEM(block, f32),
            pltpu.VMEM(block, f32),
            pltpu.VMEM((chunks, members, lats, width, LANES), f32),
            pltpu.VMEM((members, chunks, lats, width, LANES), f32),
            pltpu.VMEM((chunks, cells, LANES), f32),
            pltpu.VMEM((3, chunks, nobs, LANES), f32),
            pltpu.VMEM((3, 8, nobs), f32),
            pltpu.VMEM((8, nobs), f32),
            pltpu.VMEM((8, nobs), f32),
            pltpu.VMEM((members, lats, chunks, width, LANES), f32),
            pltpu.VMEM((cells, members * chunks * group), f32),
            dma((chunks,)),
            dma((chunks, lats)),
            dma((chunks, lats)),
            dma((chunks, members)),
            dma((chunks, members)),
            dma,
            dma,
            dma((3,)),
            dma((3,)),
            dma((3, chunks)),
            dma((3, chunks)),
            dma((strips,)),
            dma((strips,)),
            dma,
        ]
        + analysis_scratch(cells, members * chunks * group, 3 * nobs),
        compiler_params=pltpu.CompilerParams(
            collective_id=0, has_side_effects=True, vmem_limit_bytes=56 * 1024 * 1024
        ),
        name="engine",
    )(ensemble, obs_cell, obs_value, obs_var, patch_rows)


def settle_kernel(dims, z_hbm, out_hbm, z_buf, out_buf, in_sem, out_sem):
    lats, members, chunks, rows, width, group = dims
    reads = [pltpu.make_async_copy(z_hbm.at[:, kc], z_buf.at[kc], in_sem.at[kc]) for kc in range(chunks)]
    for read in reads:
        read.start()
    writes = []
    for kc in range(chunks):
        reads[kc].wait()
        turned = z_buf[kc].reshape(lats * members * width, LANES).T
        for r in range(rows):
            out_buf[kc, :, r, :] = turned[r * group : (r + 1) * group]
        write = pltpu.make_async_copy(out_buf.at[kc], out_hbm.at[pl.ds(kc * group, group)], out_sem.at[kc])
        write.start()
        writes.append(write)
    for write in writes:
        write.wait()


def settle(pieces, dims):
    lats, members, chunks, rows, width, group = dims
    strips = lats * members
    f32, anywhere = jnp.float32, pl.BlockSpec(memory_space=pl.ANY)
    return pl.pallas_call(
        functools.partial(settle_kernel, dims),
        out_shape=jax.ShapeDtypeStruct((chunks * group, rows, strips * width), f32),
        in_specs=[anywhere],
        out_specs=anywhere,
        scratch_shapes=[
            pltpu.VMEM((chunks, strips, width, LANES), f32),
            pltpu.VMEM((chunks, group, rows, strips * width), f32),
            pltpu.SemaphoreType.DMA((chunks,)),
            pltpu.SemaphoreType.DMA((chunks,)),
        ],
        name="settle",
    )(pieces)


def kernel_device(dims, ensemble, obs_cell, obs_value, obs_var, patch_rows):
    return settle(engine(ensemble, obs_cell, obs_value, obs_var, patch_rows, dims), dims)


def kernel_dims(mesh, ensemble, obs_cell, patch_rows):
    lats, members = mesh.shape["lat"], mesh.shape["member"]
    total, lat_all, lon = ensemble.shape
    own, rows = total // members, lat_all // lats
    width = lon // (lats * members)
    if LANES % rows:
        return None
    group = LANES // rows
    fits = (
        own % group == 0
        and (members * (own // group)) % rows == 0
        and width == 8
        and lats % 4 == 0
        and members % 2 == 0
        and obs_cell.shape[1] % LANES == 0
        and patch_rows.shape[1] == 2
    )
    return (lats, members, own // group, rows, width, group) if fits else None


def solution(mesh):
    specs = (P("member", "lat", None),) + (P(("member", "lat"), None),) * 4

    def run(ensemble, obs_cell, obs_value, obs_var, patch_rows):
        dims = kernel_dims(mesh, ensemble, obs_cell, patch_rows)
        body = general_device if dims is None else functools.partial(kernel_device, dims)
        mapped = jax.shard_map(
            body, mesh=mesh, in_specs=specs, out_specs=P("member", "lat", None), check_vma=False
        )
        return mapped(ensemble, obs_cell, obs_value, obs_var, patch_rows)

    return run
```

```python
import functools

import jax
import jax.numpy as jnp
from jax import lax
from jax.experimental import pallas as pl
from jax.experimental.pallas import tpu as pltpu
from jax.sharding import PartitionSpec as P

STEPS = 4

lat_coeff = 0.4
lon_coeff = 0.05
advect_coeff = 0.1

MESH = pl.DeviceIdType.MESH
LANES = 128


def with_halo(value, sides, width, wrap):
    for axis, dim in sides:
        size, length = (lax.axis_size(axis), value.shape[dim])
        up = [(i, (i + 1) % size) for i in range(size if wrap else size - 1)]
        down = [(j, i) for i, j in up]
        last = lax.slice_in_dim(value, length - width, length, axis=dim)
        initial = lax.slice_in_dim(value, 0, width, axis=dim)
        before = lax.ppermute(last, axis, up)
        after = lax.ppermute(initial, axis, down)
        value = jnp.concatenate([before, value, after], axis=dim)
    return value


def advance(padded):
    centre = padded[:, 1:-1]
    northern = padded[:, :-2]
    southern = padded[:, 2:]
    eastern = jnp.roll(centre, -1, axis=2)
    western = jnp.roll(centre, 1, axis=2)
    return (
        centre
        + lat_coeff * (northern + southern - 2.0 * centre)
        + lon_coeff * (eastern + western - 2.0 * centre)
        - advect_coeff * centre * (eastern - western)
    )


def localize(obs_rows, rel_cols, first_row, row_count, lat_scale, width_cols):
    lower = first_row.astype(jnp.float32)
    upper = lower + row_count.astype(jnp.float32) - 1.0
    lat_gap = jnp.maximum(jnp.maximum(lower - obs_rows, obs_rows - upper), 0.0) / lat_scale
    lon_gap = jnp.maximum(jnp.maximum(-rel_cols, rel_cols - (width_cols - 1.0)), 0.0) / width_cols
    return jnp.exp(-lat_gap * lat_gap - lon_gap * lon_gap)


def dot3(left, right):
    return jnp.matmul(left, right, precision=lax.Precision.HIGH, preferred_element_type=jnp.float32)


def analyse(anomaly, state_mean, spread, obs_meta, lengths, width_cols):
    cell_total, members = anomaly.shape
    lat_total = cell_total // width_cols
    near = spread.shape[0]
    starts = jnp.cumsum(lengths) - lengths
    cell_rows = jnp.arange(cell_total, dtype=jnp.int32) // width_cols
    identity = jnp.eye(members, dtype=jnp.float32)
    products = dot3(spread, jnp.concatenate([spread, anomaly], axis=0).T)
    common, crossed = products[:, :near], products[:, near:]
    innov = obs_meta[0]
    shrink = jnp.zeros((cell_total,), jnp.float32)
    shift = state_mean
    weights_all = jnp.zeros((near, cell_total), jnp.float32)
    for patch in range(lengths.shape[0]):
        weights = (
            localize(obs_meta[2], obs_meta[3], starts[patch], lengths[patch], lat_total / 4.0, float(width_cols))
            / obs_meta[1]
        )
        scale = jnp.sqrt(weights)
        gram_matrix = (members - 1.0) * identity + jnp.dot(
            (spread * weights[:, None]).T, spread, preferred_element_type=jnp.float32
        )
        bound = jnp.max(jnp.sum(jnp.abs(gram_matrix), axis=1))
        alpha = (members - 1.0) / bound
        x = common * scale[:, None] * (scale / bound)[None, :]
        c0 = 2.25 + alpha * (-2.4375 + alpha * (1.6875 + alpha * (-0.5625 + alpha * 0.0625)))
        c1 = -2.4375 + alpha * (3.375 + alpha * (-1.6875 + alpha * 0.25))
        c2 = 1.6875 + alpha * (-1.6875 + alpha * 0.375)
        c3 = -0.5625 + alpha * 0.25
        c4 = 0.0625
        x2 = dot3(x, x)
        x34 = dot3(x2, jnp.concatenate([x, x2], axis=1))
        x3, x4 = x34[:, :near], x34[:, near:]
        low = c2 * x + c3 * x2 + c4 * x3
        high = c1 * x + c2 * x2 + c3 * x3 + c4 * x4
        block = jnp.concatenate([crossed * scale[:, None], (scale * innov)[:, None]], axis=1)
        both = dot3(jnp.concatenate([low, high], axis=0), block)
        b1 = c1 * block + both[:near]
        b2 = c0 * block + both[near:]
        b3 = c0 * b2 + dot3(high, b2)
        mixed = alpha * c0 * b1 + b3
        got = 1.5 * b1 - 0.5 * (
            alpha * c0 * c0 * b1
            + c0 * mixed
            + dot3(high, mixed)
            + alpha * (c1 * b3 + dot3(low, b3))
        )
        base = c0 * (1.5 - 0.5 * alpha * c0 * c0)
        driven = base * block[:, -1] + jnp.sum(x * got[:, -1][None, :], axis=1)
        again = jnp.sum(x * driven[None, :], axis=1)
        mean_part = (
            jnp.sum(block[:, :-1] * (base * driven)[:, None] + got[:, :-1] * again[:, None], axis=0)
            / bound
        )
        cell_mask = (cell_rows >= starts[patch]) & (cell_rows < starts[patch] + lengths[patch])
        root_scale = jnp.sqrt((members - 1.0) / bound)
        shift = shift + jnp.where(cell_mask, mean_part, 0.0)
        shrink = jnp.where(cell_mask, root_scale * base, shrink)
        weights_all = jnp.where(
            cell_mask[None, :], got[:, :-1] * (scale * (root_scale / bound))[:, None], weights_all
        )
    return shift[:, None] + shrink[:, None] * anomaly + dot3(weights_all.T, spread)


def general_device(ensemble, obs_cell, obs_value, obs_var, patch_rows):
    members_dev, lat_rows, lon_cells = ensemble.shape
    lat_count = lax.axis_size("lat")
    member_count = lax.axis_size("member")
    servers = lat_count * member_count
    width_cols = lon_cells // servers
    padded = with_halo(ensemble, (("lat", 1),), STEPS, False)
    global_rows = (
        lax.axis_index("lat") * lat_rows + jnp.arange(lat_rows + 2 * STEPS, dtype=jnp.int32) - STEPS
    )
    inside = ((global_rows >= 0) & (global_rows < lat_rows * lat_count)).astype(jnp.float32)
    for step_index in range(STEPS):
        padded = advance(padded)
        keeper = inside[step_index + 1 : inside.shape[0] - step_index - 1]
        padded = padded * keeper[None, :, None]
    blocks = padded.reshape(1, members_dev, lat_rows, lon_cells)
    received = lax.all_to_all(blocks, ("member", "lat"), split_axis=3, concat_axis=0, tiled=True)
    strip = received.reshape(member_count, lat_count, members_dev, lat_rows, width_cols)
    members = member_count * members_dev
    lat_total = lat_count * lat_rows
    states = strip.transpose(1, 3, 4, 0, 2).reshape(lat_total * width_cols, members)
    cell_index = obs_cell[0]
    obs_count = cell_index.shape[0]
    state_mean = jnp.mean(states, axis=1)
    anomaly = states - state_mean[:, None]
    spread = jnp.take(anomaly, cell_index, axis=0)
    innov = obs_value[0] - jnp.take(state_mean, cell_index)
    obs_meta = jnp.stack(
        [
            innov,
            obs_var[0],
            (cell_index // width_cols).astype(jnp.float32),
            (cell_index % width_cols).astype(jnp.float32),
        ]
    )
    near_spread = with_halo(spread, ((("member", "lat"), 0),), obs_count, True)
    near_meta = with_halo(obs_meta, ((("member", "lat"), 1),), obs_count, True)
    shifts = jnp.repeat(jnp.array([-1.0, 0.0, 1.0], jnp.float32), obs_count) * width_cols
    near_meta = jnp.concatenate([near_meta[:3], (near_meta[3] + shifts)[None, :]], axis=0)
    analysed = analyse(anomaly, state_mean, near_spread, near_meta, patch_rows[0], width_cols)
    outgoing = analysed.reshape(lat_count, lat_rows, width_cols, member_count, members_dev)
    outgoing = outgoing.transpose(3, 0, 4, 1, 2).reshape(servers, members_dev, lat_rows, width_cols)
    returned = lax.all_to_all(outgoing, ("member", "lat"), split_axis=0, concat_axis=3, tiled=True)
    return returned.reshape(members_dev, lat_rows, lon_cells)


def place(block, lats):
    half = block // (lats // 2)
    return (1 - half) * (2 * block) + half * (2 * lats - 1 - 2 * block)


def block_at(lat, lats):
    odd = lat % 2
    return (1 - odd) * (lat // 2) + odd * (lats - 1 - lat // 2)


def member_of(block, q, members):
    odd = block % 2
    return (1 - odd) * q + odd * (members - 1 - q)


def strip_at(m, lat, lats, members):
    block = block_at(lat, lats)
    return block * members + member_of(block, m, members)


def home_of(strip, lats, members):
    block = strip // members
    return member_of(block, strip % members, members), place(block, lats)


def greet_all(lats, members):
    m, lat = lax.axis_index("member"), lax.axis_index("lat")
    barrier = pltpu.get_barrier_semaphore()
    for dm in range(members):
        for dl in range(lats):
            if dm == 0 and dl == 0:
                continue
            pl.semaphore_signal(
                barrier, inc=1, device_id=((m + dm) % members, (lat + dl) % lats), device_id_type=MESH
            )
    return barrier, lats * members - 1


def split(a):
    high = a.astype(jnp.bfloat16)
    return high, (a - high.astype(jnp.float32)).astype(jnp.bfloat16)


def left_form(a):
    high, low = split(a)
    return jnp.concatenate([high, high, low], axis=1)


def put_right(ref, at, a):
    high, low = split(a)
    depth = ref.shape[0] // 3
    rows = a.shape[0]
    ref[at : at + rows] = high
    ref[depth + at : depth + at + rows] = low
    ref[2 * depth + at : 2 * depth + at + rows] = high


def dot(a, b):
    return jnp.dot(a, b, preferred_element_type=jnp.float32)


def dot_across(a, b):
    return lax.dot_general(a, b, (((1,), (1,)), ((), ())), preferred_element_type=jnp.float32)


def to_column(row):
    eye = lax.broadcasted_iota(jnp.int32, (LANES, LANES), 0) == lax.broadcasted_iota(jnp.int32, (LANES, LANES), 1)
    return jnp.concatenate(
        [
            jnp.sum(jnp.where(eye, row[:, i : i + LANES], 0.0), axis=1, keepdims=True)
            for i in range(0, row.shape[1], LANES)
        ],
        axis=0,
    )


def analysis_scratch(cells, count, near):
    f32, bf16 = jnp.float32, jnp.bfloat16
    return [
        pltpu.VMEM((near, near), f32),
        pltpu.VMEM((near, cells), f32),
        pltpu.VMEM((3 * near, count), bf16),
        pltpu.VMEM((count, near), bf16),
        pltpu.VMEM((near, 3 * near), bf16),
        pltpu.VMEM((3 * near, near), bf16),
        pltpu.VMEM((near, 3 * near), bf16),
        pltpu.VMEM((8, 3 * near, cells), bf16),
        pltpu.VMEM((7, near, cells), f32),
        pltpu.VMEM((2, cells, near), f32),
    ]


def own_products(work, y, right):
    common, crossed, y_right, y_turned = work[:4]
    side = y.shape[0]
    put_right(y_right, side, y)
    high, low = y_right[side : 2 * side], y_right[4 * side : 5 * side]
    left = jnp.concatenate([high, high, low], axis=1)
    crossed[side : 2 * side] = dot_across(left, right)
    common[side : 2 * side, side : 2 * side] = dot_across(left, jnp.concatenate([high, low, high], axis=1))


def other_products(work, sides, right):
    common, crossed, y_right, y_turned = work[:4]
    side = sides[0].shape[0]
    for slot, y in zip((0, 2), sides):
        put_right(y_right, slot * side, y)
    near = 3 * side
    high, low = y_right[0:near], y_right[near : 2 * near]
    y_turned[...] = high.T
    terms = [jnp.concatenate([v[0:side], v[2 * side :]], axis=0) for v in (high, low)]
    left = jnp.concatenate([terms[0], terms[0], terms[1]], axis=1)
    mine = dot_across(left, jnp.concatenate([high, low, high], axis=1))
    apart = dot_across(left, right)
    for i, slot in enumerate((0, 2)):
        span = slice(slot * side, (slot + 1) * side)
        common[span] = mine[i * side : (i + 1) * side]
        crossed[span] = apart[i * side : (i + 1) * side]
        common[side : 2 * side, span] = mine[i * side : (i + 1) * side, side : 2 * side].T


def solve_patch(dims, work, slot, spare_first, lower, upper, innov, meta):
    lats, members, chunks, rows, width, group = dims
    common, crossed, y_right, y_turned, x_left, x_right, low_left, b_right, blocks, turned = work
    count, near = y_turned.shape
    cells = crossed.shape[1]
    tile = near // 2
    tiles = range(0, near, tile)
    var, obs_rows = meta[1:2], meta[2:3]
    strip_of = lax.broadcasted_iota(jnp.int32, (1, near), 1) // (near // 3) - 1
    cols = meta[3:4] + (strip_of * width).astype(jnp.float32)
    lon_gap = jnp.maximum(jnp.maximum(-cols, cols - (width - 1.0)), 0.0) / float(width)
    lat_gap = jnp.maximum(jnp.maximum(lower - obs_rows, obs_rows - upper), 0.0) / (cells // width / 4.0)
    weights = jnp.exp(-lat_gap * lat_gap - lon_gap * lon_gap) / var
    scale = jnp.sqrt(weights)
    scale_col = to_column(scale)

    left = (y_turned[...].astype(jnp.float32) * weights).astype(jnp.bfloat16)
    gram = jnp.abs(dot(left, y_right[0:near]))
    sums = jnp.sum(gram.reshape(count // 8, 8, count), axis=0)
    bound = (count - 1.0) + jnp.max(jnp.sum(sums, axis=0, keepdims=True), axis=1, keepdims=True)
    inverse = 1.0 / bound
    alpha = (count - 1.0) * inverse
    c0 = 2.25 + alpha * (-2.4375 + alpha * (1.6875 + alpha * (-0.5625 + alpha * 0.0625)))
    c1 = -2.4375 + alpha * (3.375 + alpha * (-1.6875 + alpha * 0.25))
    c2 = 1.6875 + alpha * (-1.6875 + alpha * 0.375)
    c3 = -0.5625 + alpha * 0.25
    c4 = 0.0625

    lane = lax.broadcasted_iota(jnp.int32, (tile, cells), 1)
    spare = (1 - spare_first) * (cells - 1)
    scale_row = scale * inverse

    def x_tile(i):
        return common[i : i + tile] * scale_col[i : i + tile] * scale_row

    block, b1, b2, w, b3, u, got = range(7)

    def keep(i, which, value):
        blocks[which, i : i + tile] = value
        put_right(b_right.at[which], i, value)

    for i in tiles:
        x = x_tile(i)
        x_left[i : i + tile] = left_form(x)
        put_right(x_right, i, x)
        keep(i, block, jnp.where(lane == spare, innov[i : i + tile], crossed[i : i + tile]) * scale_col[i : i + tile])
    x2 = dot(x_left[...], x_right[...])
    x3 = dot(left_form(x2), x_right[...])
    low_left[...] = left_form(c2 * (common[...] * scale_col * scale_row) + c3 * x2 + c4 * x3)

    def low_on(i, which):
        return dot(low_left[i : i + tile], b_right[which])

    def x_on(i, which):
        return dot(x_left[i : i + tile], b_right[which])

    for i in tiles:
        keep(i, b1, c1 * blocks[block, i : i + tile] + low_on(i, block))
    for i in tiles:
        keep(i, b2, c0 * blocks[block, i : i + tile] + x_on(i, b1))
    for i in tiles:
        keep(i, w, c1 * blocks[b2, i : i + tile] + low_on(i, b2))
    for i in tiles:
        keep(i, b3, c0 * blocks[b2, i : i + tile] + x_on(i, w))
    for i in tiles:
        keep(i, u, c1 * blocks[b3, i : i + tile] + low_on(i, b3))
    root_scale = jnp.sqrt(alpha)
    for i in tiles:
        z = c0 * blocks[b3, i : i + tile] + x_on(i, u)
        first = blocks[b1, i : i + tile]
        value = 1.5 * first - 0.5 * (
            z + alpha * (blocks[u, i : i + tile] + c0 * (blocks[w, i : i + tile] + c0 * first))
        )
        put_right(b_right.at[got], i, value)
        turned[slot, :, i : i + tile] = (value * (scale_col[i : i + tile] * (root_scale * inverse))).T
    base = c0 * (1.5 - 0.5 * alpha * c0 * c0)
    change = None
    for i in tiles:
        full = base * blocks[block, i : i + tile] + x_on(i, got)
        drive = jnp.where(spare_first == 1, full[:, 0:1], full[:, cells - 1 : cells])
        part = jnp.sum((full * drive).reshape(tile // 8, 8, cells), axis=0)
        change = part if change is None else change + part
    return jnp.sum(change, axis=0, keepdims=True) * inverse, root_scale * base


def forecast(load, lats, group):
    fields = [load(l) for l in range(lats)]
    lane = lax.broadcasted_iota(jnp.int32, fields[0].shape, 1)
    first, last = lane < group, lane >= LANES - group
    count = fields[0].shape[0]
    zero = jnp.zeros_like(fields[0])
    for _ in range(STEPS):
        new = []
        for l in range(lats):
            c = fields[l]
            above = fields[l - 1] if l > 0 else zero
            below = fields[l + 1] if l + 1 < lats else zero
            north = pltpu.roll(jnp.where(last, above, c), group, 1)
            south = pltpu.roll(jnp.where(first, below, c), LANES - group, 1)
            east = pltpu.roll(c, count - 1, 0)
            west = pltpu.roll(c, 1, 0)
            new.append(
                c
                + lat_coeff * (north + south - 2.0 * c)
                + lon_coeff * (east + west - 2.0 * c)
                - advect_coeff * c * (east - west)
            )
        fields = new
    return fields


def swap_blocks(parts, group):
    per = len(parts)
    lane_block = lax.broadcasted_iota(jnp.int32, parts[0].shape, 1) // group
    outs = []
    for i in range(per):
        out = None
        for j in range(per):
            shift = (group * (j - i)) % LANES
            piece = pltpu.roll(parts[j], shift, 1) if shift else parts[j]
            out = piece if out is None else jnp.where(lane_block == j, piece, out)
        outs.append(out)
    return outs


def pick(onehot, values):
    total, rest = None, values
    for _ in range(3):
        term = rest.astype(jnp.bfloat16)
        part = jnp.dot(onehot, term, preferred_element_type=jnp.float32)
        total = part if total is None else total + part
        rest = rest - term.astype(jnp.float32)
    return total


def engine_kernel(
    dims, x_hbm, cell_ref, value_ref, var_ref, rows_ref, z_hbm,
    x_buf, s_buf, ra, f_buf, r_buf, xt, yt, meta, obs_out, obs_in, t_buf, at_buf,
    x_sem, a_send, a_recv, b_send, b_recv, o_send, o_recv, m_send, m_recv, y_send, y_recv, z_send, z_recv, own_sem, *work,
):
    lats, members, chunks, rows, width, group = dims
    cols = width * members
    cells = lats * rows * width
    strips = lats * members
    edge = STEPS
    m, lat = lax.axis_index("member"), lax.axis_index("lat")
    own = block_at(lat, lats)
    strip = strip_at(m, lat, lats, members)
    neighbours = [(slot, home_of((strip + side) % strips, lats, members)) for side, slot in ((1, 0), (strips - 1, 2))]

    def remote(src, dst, send, recv, to):
        return pltpu.make_async_remote_copy(
            src_ref=src, dst_ref=dst, send_sem=send, recv_sem=recv, device_id=to, device_id_type=MESH
        )

    reads = [
        pltpu.make_async_copy(x_hbm.at[pl.ds(kc * group, group)], x_buf.at[kc], x_sem.at[kc]) for kc in range(chunks)
    ]
    barrier, partners = greet_all(lats, members)
    for read in reads:
        read.start()

    obs_out[...] = jnp.zeros_like(obs_out)
    obs_out[0:1, :] = cell_ref[...].astype(jnp.float32)
    obs_out[1:2, :] = value_ref[...]
    obs_out[2:3, :] = var_ref[...]
    obs_out[3:4, 0 : rows_ref.shape[1]] = rows_ref[...].astype(jnp.float32)

    target_m, target_l = home_of(m * lats + lat, lats, members)
    away = jnp.logical_or(target_m != m, target_l != lat)
    obs_copy = remote(obs_out, obs_in, o_send, o_recv, (target_m, target_l))

    a_copies = []
    for kc in range(chunks):
        reads[kc].wait()
        whole = jnp.concatenate([x_buf[kc, :, r, :] for r in range(rows)], axis=0)
        turned = whole.T
        lon = turned.shape[0]
        for b in range(lats):
            s_buf[kc, b, 0:cols] = turned[b * cols : (b + 1) * cols]
            east, west = ((b + 1) * cols) % lon, (b * cols - edge) % lon
            s_buf[kc, b, cols : cols + edge] = turned[east : east + edge]
            s_buf[kc, b, cols + edge : cols + 2 * edge] = turned[west : west + edge]
        if kc == 0:
            pl.semaphore_wait(barrier, partners)

            @pl.when(away)
            def _():
                obs_copy.start()

            @pl.when(jnp.logical_not(away))
            def _():
                obs_in[...] = obs_out[...]

        run = []
        for d in range(1, lats):
            to = (lat + d) % lats
            copy = remote(
                s_buf.at[kc, block_at(to, lats)], ra.at[kc, lat], a_send.at[kc, d], a_recv.at[kc, d], (m, to)
            )
            copy.start()
            run.append(copy)
        a_copies.append(run)

    @pl.when(away)
    def _():
        obs_copy.wait_recv()

    cell_lane = obs_in[0:1, :]
    obs_row = jnp.floor(cell_lane * (1.0 / width))
    meta[1, 0:1, :] = obs_in[1:2, :]
    meta[1, 1:2, :] = obs_in[2:3, :]
    meta[1, 2:3, :] = obs_row
    meta[1, 3:4, :] = cell_lane - width * obs_row
    meta[1, 4:5, :] = obs_in[3:4, :]
    meta[1, 5:8, :] = jnp.zeros((3, cell_lane.shape[1]), jnp.float32)
    late = []
    for slot, to in neighbours:
        copy = remote(meta.at[1], meta.at[slot], m_send.at[slot], m_recv.at[slot], to)
        copy.start()
        late.append(copy)
    onehot = (
        to_column(cell_lane)
        == lax.broadcasted_iota(jnp.int32, (cell_lane.shape[1], cells), 1).astype(jnp.float32)
    ).astype(jnp.bfloat16)

    b_copies = []

    def arrive(kc):
        for copy in b_copies[kc]:
            copy.wait_recv()
        parts = [r_buf[j, kc].reshape(lats * width, LANES) for j in range(members)]
        for r, out in enumerate(swap_blocks(parts, group)):
            for l in range(lats):
                xt[kc, (l * rows + r) * width : (l * rows + r + 1) * width] = out[l * width : (l + 1) * width]
        yt[1, kc] = pick(onehot, xt[kc])
        for slot, to in neighbours:
            copy = remote(yt.at[1, kc], yt.at[slot, kc], y_send.at[slot, kc], y_recv.at[slot, kc], to)
            copy.start()
            late.append(copy)

    for kc in range(chunks):
        ra[kc, lat] = s_buf[kc, own]
        for copy in a_copies[kc]:
            copy.wait_recv()
        fields = forecast(lambda l, kc=kc: ra[kc, l], lats, group)
        for l in range(lats):
            for q in range(members):
                f_buf[kc, q, l] = fields[l][q * width : (q + 1) * width]
        run = []
        for d in range(1, members):
            to = (m + d) % members
            copy = remote(
                f_buf.at[kc, member_of(own, to, members)], r_buf.at[m, kc], b_send.at[kc, d], b_recv.at[kc, d], (to, lat)
            )
            copy.start()
            run.append(copy)
        b_copies.append(run)
        r_buf[m, kc] = f_buf[kc, member_of(own, m, members)]
        if kc:
            arrive(kc - 1)
    arrive(chunks - 1)

    states = jnp.concatenate([xt[kc] for kc in range(chunks)], axis=1)
    mean = jnp.sum(states, axis=1, keepdims=True) * (1.0 / states.shape[1])
    at = states - mean
    at_buf[...] = at
    ah, al = split(at)
    right = jnp.concatenate([ah, al, ah], axis=1)

    def observed(slot):
        raw = jnp.concatenate([yt[slot, kc] for kc in range(chunks)], axis=1)
        centre = jnp.sum(raw, axis=1, keepdims=True) * (1.0 / raw.shape[1])
        return raw - centre, centre

    own_spread, own_mean = observed(1)
    own_products(work, own_spread, right)
    for copy in late:
        copy.wait_recv()
    before, before_mean = observed(0)
    after, after_mean = observed(2)
    other_products(work, (before, after), right)
    all_meta = jnp.concatenate([meta[slot] for slot in range(3)], axis=1)
    innov = to_column(all_meta[0:1]) - jnp.concatenate([before_mean, own_mean, after_mean], axis=0)
    y_right, turned = work[2], work[9]

    nobs = cell_lane.shape[1]
    sure = lats // 4
    rest = lats - sure
    last = 1 - lat // (lats // 2)
    lasts = last.astype(jnp.float32)
    first_len = all_meta[4:5, nobs : nobs + 1]
    second_len = all_meta[4:5, nobs + 1 : nobs + 2]
    spans = []
    for which in (lasts, 1.0 - lasts):
        lower = which * first_len
        spans.append((lower, lower + (first_len + which * (second_len - first_len)) - 1.0))

    def finish(tile, tiles, pick_cells, weights, change, factor):
        begin = tile * (rows * width)
        span = pl.ds(pl.multiple_of(begin, rows * width), tiles * rows * width)
        out = pick_cells(mean) + change + factor * at_buf[span, :] + dot(left_form(weights), y_right[...])
        for kc in range(chunks):
            lanes = out[:, kc * LANES : (kc + 1) * LANES]
            parts = [
                jnp.concatenate(
                    [lanes[(l * rows + r) * width : (l * rows + r + 1) * width] for l in range(tiles)], axis=0
                )
                for r in range(rows)
            ]
            for j, piece in enumerate(swap_blocks(parts, group)):
                for l in range(tiles):
                    t_buf[j, tile + l, kc] = piece[l * width : (l + 1) * width]

    def give(to):
        copy = remote(t_buf.at[to[0], to[1]], z_hbm.at[strip], z_send.at[len(z_copies)], z_recv.at[strip], to)
        copy.start()
        z_copies.append(copy)

    z_copies = []
    cut, tail = sure * rows * width, rest * rows * width
    early = last * rest
    change, factor = solve_patch(dims, work, 0, last, *spans[0], innov, all_meta)
    change_col = to_column(change)

    def far(column):
        return jnp.where(last == 1, column[tail:], column[:cut])

    def near(column):
        return jnp.where(last == 1, column[:tail], column[cut:])

    finish(early, sure, far, far(turned[0]), far(change_col), factor)
    for l in range(sure):
        for dm in range(members):
            give(((m + dm) % members, early + l))

    change2, factor2 = solve_patch(dims, work, 1, 1 - last, *spans[1], innov, all_meta)
    cell_row = (lax.broadcasted_iota(jnp.int32, (cells, 1), 0) // width).astype(jnp.float32)
    inside = near(jnp.logical_and(cell_row >= spans[0][0], cell_row <= spans[0][1]).astype(jnp.float32)) > 0.5
    base = (1 - last) * sure
    finish(
        base,
        rest,
        near,
        jnp.where(inside, near(turned[0]), near(turned[1])),
        jnp.where(inside, near(change_col), near(to_column(change2))),
        jnp.where(inside, factor, factor2),
    )
    for j in range(rest - 1):
        for dm in range(members):
            give(((m + dm) % members, base + (lat - base + 1 + j) % rest))
    for dm in range(1, members):
        give(((m + dm) % members, lat))
    kept = pltpu.make_async_copy(t_buf.at[m, lat], z_hbm.at[strip], own_sem)
    kept.start()

    for run in a_copies + b_copies + [late]:
        for copy in run:
            copy.wait_send()

    @pl.when(away)
    def _():
        obs_copy.wait_send()

    kept.wait()
    for copy in z_copies:
        copy.wait_send()
    for d in range(1, strips):
        other = (strip + d) % strips
        remote(
            t_buf.at[0, 0], z_hbm.at[other], z_send.at[0], z_recv.at[other], ((m + 1) % members, lat)
        ).wait_recv()


def engine(ensemble, obs_cell, obs_value, obs_var, patch_rows, dims):
    lats, members, chunks, rows, width, group = dims
    cells = lats * rows * width
    nobs = obs_cell.shape[1]
    strips = lats * members
    dma, f32 = pltpu.SemaphoreType.DMA, jnp.float32
    vmem, anywhere = pl.BlockSpec(memory_space=pltpu.VMEM), pl.BlockSpec(memory_space=pl.ANY)
    block = (chunks, lats, members * width + 2 * STEPS, LANES)
    return pl.pallas_call(
        functools.partial(engine_kernel, dims),
        out_shape=jax.ShapeDtypeStruct((strips, chunks, width, LANES), f32),
        in_specs=[anywhere, vmem, vmem, vmem, vmem],
        out_specs=anywhere,
        scratch_shapes=[
            pltpu.VMEM((chunks, group, rows, strips * width), f32),
            pltpu.VMEM(block, f32),
            pltpu.VMEM(block, f32),
            pltpu.VMEM((chunks, members, lats, width, LANES), f32),
            pltpu.VMEM((members, chunks, lats, width, LANES), f32),
            pltpu.VMEM((chunks, cells, LANES), f32),
            pltpu.VMEM((3, chunks, nobs, LANES), f32),
            pltpu.VMEM((3, 8, nobs), f32),
            pltpu.VMEM((8, nobs), f32),
            pltpu.VMEM((8, nobs), f32),
            pltpu.VMEM((members, lats, chunks, width, LANES), f32),
            pltpu.VMEM((cells, members * chunks * group), f32),
            dma((chunks,)),
            dma((chunks, lats)),
            dma((chunks, lats)),
            dma((chunks, members)),
            dma((chunks, members)),
            dma,
            dma,
            dma((3,)),
            dma((3,)),
            dma((3, chunks)),
            dma((3, chunks)),
            dma((strips,)),
            dma((strips,)),
            dma,
        ]
        + analysis_scratch(cells, members * chunks * group, 3 * nobs),
        compiler_params=pltpu.CompilerParams(
            collective_id=0, has_side_effects=True, vmem_limit_bytes=56 * 1024 * 1024
        ),
        name="engine",
    )(ensemble, obs_cell, obs_value, obs_var, patch_rows)


def settle_kernel(dims, z_hbm, out_hbm, z_buf, out_buf, in_sem, out_sem):
    lats, members, chunks, rows, width, group = dims
    reads = [pltpu.make_async_copy(z_hbm.at[:, kc], z_buf.at[kc], in_sem.at[kc]) for kc in range(chunks)]
    for read in reads:
        read.start()
    writes = []
    for kc in range(chunks):
        reads[kc].wait()
        turned = z_buf[kc].reshape(lats * members * width, LANES).T
        for r in range(rows):
            out_buf[kc, :, r, :] = turned[r * group : (r + 1) * group]
        write = pltpu.make_async_copy(out_buf.at[kc], out_hbm.at[pl.ds(kc * group, group)], out_sem.at[kc])
        write.start()
        writes.append(write)
    for write in writes:
        write.wait()


def settle(pieces, dims):
    lats, members, chunks, rows, width, group = dims
    strips = lats * members
    f32, anywhere = jnp.float32, pl.BlockSpec(memory_space=pl.ANY)
    return pl.pallas_call(
        functools.partial(settle_kernel, dims),
        out_shape=jax.ShapeDtypeStruct((chunks * group, rows, strips * width), f32),
        in_specs=[anywhere],
        out_specs=anywhere,
        scratch_shapes=[
            pltpu.VMEM((chunks, strips, width, LANES), f32),
            pltpu.VMEM((chunks, group, rows, strips * width), f32),
            pltpu.SemaphoreType.DMA((chunks,)),
            pltpu.SemaphoreType.DMA((chunks,)),
        ],
        name="settle",
    )(pieces)


def kernel_device(dims, ensemble, obs_cell, obs_value, obs_var, patch_rows):
    return settle(engine(ensemble, obs_cell, obs_value, obs_var, patch_rows, dims), dims)


def kernel_dims(mesh, ensemble, obs_cell, patch_rows):
    lats, members = mesh.shape["lat"], mesh.shape["member"]
    total, lat_all, lon = ensemble.shape
    own, rows = total // members, lat_all // lats
    width = lon // (lats * members)
    if LANES % rows:
        return None
    group = LANES // rows
    fits = (
        own % group == 0
        and (members * (own // group)) % rows == 0
        and width == 8
        and lats % 4 == 0
        and members % 2 == 0
        and obs_cell.shape[1] % LANES == 0
        and patch_rows.shape[1] == 2
    )
    return (lats, members, own // group, rows, width, group) if fits else None


def solution(mesh):
    specs = (P("member", "lat", None),) + (P(("member", "lat"), None),) * 4

    def run(ensemble, obs_cell, obs_value, obs_var, patch_rows):
        dims = kernel_dims(mesh, ensemble, obs_cell, patch_rows)
        body = general_device if dims is None else functools.partial(kernel_device, dims)
        mapped = jax.shard_map(
            body, mesh=mesh, in_specs=specs, out_specs=P("member", "lat", None), check_vma=False
        )
        return mapped(ensemble, obs_cell, obs_value, obs_var, patch_rows)

    return run
```

```python
import functools

import jax
import jax.numpy as jnp
from jax import lax
from jax.experimental import pallas as pl
from jax.experimental.pallas import tpu as pltpu
from jax.sharding import PartitionSpec as P

STEPS = 4

lat_coeff = 0.4
lon_coeff = 0.05
advect_coeff = 0.1

MESH = pl.DeviceIdType.MESH
LANES = 128


def with_halo(value, sides, width, wrap):
    for axis, dim in sides:
        size, length = (lax.axis_size(axis), value.shape[dim])
        up = [(i, (i + 1) % size) for i in range(size if wrap else size - 1)]
        down = [(j, i) for i, j in up]
        last = lax.slice_in_dim(value, length - width, length, axis=dim)
        initial = lax.slice_in_dim(value, 0, width, axis=dim)
        before = lax.ppermute(last, axis, up)
        after = lax.ppermute(initial, axis, down)
        value = jnp.concatenate([before, value, after], axis=dim)
    return value


def advance(padded):
    centre = padded[:, 1:-1]
    northern = padded[:, :-2]
    southern = padded[:, 2:]
    eastern = jnp.roll(centre, -1, axis=2)
    western = jnp.roll(centre, 1, axis=2)
    return (
        centre
        + lat_coeff * (northern + southern - 2.0 * centre)
        + lon_coeff * (eastern + western - 2.0 * centre)
        - advect_coeff * centre * (eastern - western)
    )


def localize(obs_rows, rel_cols, first_row, row_count, lat_scale, width_cols):
    lower = first_row.astype(jnp.float32)
    upper = lower + row_count.astype(jnp.float32) - 1.0
    lat_gap = jnp.maximum(jnp.maximum(lower - obs_rows, obs_rows - upper), 0.0) / lat_scale
    lon_gap = jnp.maximum(jnp.maximum(-rel_cols, rel_cols - (width_cols - 1.0)), 0.0) / width_cols
    return jnp.exp(-lat_gap * lat_gap - lon_gap * lon_gap)


def dot3(left, right):
    return jnp.matmul(left, right, precision=lax.Precision.HIGH, preferred_element_type=jnp.float32)


def analyse(anomaly, state_mean, spread, obs_meta, lengths, width_cols):
    cell_total, members = anomaly.shape
    lat_total = cell_total // width_cols
    near = spread.shape[0]
    starts = jnp.cumsum(lengths) - lengths
    cell_rows = jnp.arange(cell_total, dtype=jnp.int32) // width_cols
    identity = jnp.eye(members, dtype=jnp.float32)
    products = dot3(spread, jnp.concatenate([spread, anomaly], axis=0).T)
    common, crossed = products[:, :near], products[:, near:]
    innov = obs_meta[0]
    shrink = jnp.zeros((cell_total,), jnp.float32)
    shift = state_mean
    weights_all = jnp.zeros((near, cell_total), jnp.float32)
    for patch in range(lengths.shape[0]):
        weights = (
            localize(obs_meta[2], obs_meta[3], starts[patch], lengths[patch], lat_total / 4.0, float(width_cols))
            / obs_meta[1]
        )
        scale = jnp.sqrt(weights)
        gram_matrix = (members - 1.0) * identity + jnp.dot(
            (spread * weights[:, None]).T, spread, preferred_element_type=jnp.float32
        )
        bound = jnp.max(jnp.sum(jnp.abs(gram_matrix), axis=1))
        alpha = (members - 1.0) / bound
        x = common * scale[:, None] * (scale / bound)[None, :]
        c0 = 2.25 + alpha * (-2.4375 + alpha * (1.6875 + alpha * (-0.5625 + alpha * 0.0625)))
        c1 = -2.4375 + alpha * (3.375 + alpha * (-1.6875 + alpha * 0.25))
        c2 = 1.6875 + alpha * (-1.6875 + alpha * 0.375)
        c3 = -0.5625 + alpha * 0.25
        c4 = 0.0625
        x2 = dot3(x, x)
        x34 = dot3(x2, jnp.concatenate([x, x2], axis=1))
        x3, x4 = x34[:, :near], x34[:, near:]
        low = c2 * x + c3 * x2 + c4 * x3
        high = c1 * x + c2 * x2 + c3 * x3 + c4 * x4
        block = jnp.concatenate([crossed * scale[:, None], (scale * innov)[:, None]], axis=1)
        both = dot3(jnp.concatenate([low, high], axis=0), block)
        b1 = c1 * block + both[:near]
        b2 = c0 * block + both[near:]
        b3 = c0 * b2 + dot3(high, b2)
        mixed = alpha * c0 * b1 + b3
        got = 1.5 * b1 - 0.5 * (
            alpha * c0 * c0 * b1
            + c0 * mixed
            + dot3(high, mixed)
            + alpha * (c1 * b3 + dot3(low, b3))
        )
        base = c0 * (1.5 - 0.5 * alpha * c0 * c0)
        driven = base * block[:, -1] + jnp.sum(x * got[:, -1][None, :], axis=1)
        again = jnp.sum(x * driven[None, :], axis=1)
        mean_part = (
            jnp.sum(block[:, :-1] * (base * driven)[:, None] + got[:, :-1] * again[:, None], axis=0)
            / bound
        )
        cell_mask = (cell_rows >= starts[patch]) & (cell_rows < starts[patch] + lengths[patch])
        root_scale = jnp.sqrt((members - 1.0) / bound)
        shift = shift + jnp.where(cell_mask, mean_part, 0.0)
        shrink = jnp.where(cell_mask, root_scale * base, shrink)
        weights_all = jnp.where(
            cell_mask[None, :], got[:, :-1] * (scale * (root_scale / bound))[:, None], weights_all
        )
    return shift[:, None] + shrink[:, None] * anomaly + dot3(weights_all.T, spread)


def general_device(ensemble, obs_cell, obs_value, obs_var, patch_rows):
    members_dev, lat_rows, lon_cells = ensemble.shape
    lat_count = lax.axis_size("lat")
    member_count = lax.axis_size("member")
    servers = lat_count * member_count
    width_cols = lon_cells // servers
    padded = with_halo(ensemble, (("lat", 1),), STEPS, False)
    global_rows = (
        lax.axis_index("lat") * lat_rows + jnp.arange(lat_rows + 2 * STEPS, dtype=jnp.int32) - STEPS
    )
    inside = ((global_rows >= 0) & (global_rows < lat_rows * lat_count)).astype(jnp.float32)
    for step_index in range(STEPS):
        padded = advance(padded)
        keeper = inside[step_index + 1 : inside.shape[0] - step_index - 1]
        padded = padded * keeper[None, :, None]
    blocks = padded.reshape(1, members_dev, lat_rows, lon_cells)
    received = lax.all_to_all(blocks, ("member", "lat"), split_axis=3, concat_axis=0, tiled=True)
    strip = received.reshape(member_count, lat_count, members_dev, lat_rows, width_cols)
    members = member_count * members_dev
    lat_total = lat_count * lat_rows
    states = strip.transpose(1, 3, 4, 0, 2).reshape(lat_total * width_cols, members)
    cell_index = obs_cell[0]
    obs_count = cell_index.shape[0]
    state_mean = jnp.mean(states, axis=1)
    anomaly = states - state_mean[:, None]
    spread = jnp.take(anomaly, cell_index, axis=0)
    innov = obs_value[0] - jnp.take(state_mean, cell_index)
    obs_meta = jnp.stack(
        [
            innov,
            obs_var[0],
            (cell_index // width_cols).astype(jnp.float32),
            (cell_index % width_cols).astype(jnp.float32),
        ]
    )
    near_spread = with_halo(spread, ((("member", "lat"), 0),), obs_count, True)
    near_meta = with_halo(obs_meta, ((("member", "lat"), 1),), obs_count, True)
    shifts = jnp.repeat(jnp.array([-1.0, 0.0, 1.0], jnp.float32), obs_count) * width_cols
    near_meta = jnp.concatenate([near_meta[:3], (near_meta[3] + shifts)[None, :]], axis=0)
    analysed = analyse(anomaly, state_mean, near_spread, near_meta, patch_rows[0], width_cols)
    outgoing = analysed.reshape(lat_count, lat_rows, width_cols, member_count, members_dev)
    outgoing = outgoing.transpose(3, 0, 4, 1, 2).reshape(servers, members_dev, lat_rows, width_cols)
    returned = lax.all_to_all(outgoing, ("member", "lat"), split_axis=0, concat_axis=3, tiled=True)
    return returned.reshape(members_dev, lat_rows, lon_cells)


def place(block, lats):
    half = block // (lats // 2)
    return (1 - half) * (2 * block) + half * (2 * lats - 1 - 2 * block)


def block_at(lat, lats):
    odd = lat % 2
    return (1 - odd) * (lat // 2) + odd * (lats - 1 - lat // 2)


def member_of(block, q, members):
    odd = block % 2
    return (1 - odd) * q + odd * (members - 1 - q)


def strip_at(m, lat, lats, members):
    block = block_at(lat, lats)
    return block * members + member_of(block, m, members)


def home_of(strip, lats, members):
    block = strip // members
    return member_of(block, strip % members, members), place(block, lats)


def greet_all(lats, members):
    m, lat = lax.axis_index("member"), lax.axis_index("lat")
    barrier = pltpu.get_barrier_semaphore()
    for dm in range(members):
        for dl in range(lats):
            if dm == 0 and dl == 0:
                continue
            pl.semaphore_signal(
                barrier, inc=1, device_id=((m + dm) % members, (lat + dl) % lats), device_id_type=MESH
            )
    return barrier, lats * members - 1


def split(a):
    high = a.astype(jnp.bfloat16)
    return high, (a - high.astype(jnp.float32)).astype(jnp.bfloat16)


def left_form(a):
    high, low = split(a)
    return jnp.concatenate([high, high, low], axis=1)


def put_right(ref, at, a):
    high, low = split(a)
    depth = ref.shape[0] // 3
    rows = a.shape[0]
    ref[at : at + rows] = high
    ref[depth + at : depth + at + rows] = low
    ref[2 * depth + at : 2 * depth + at + rows] = high


def dot(a, b):
    return jnp.dot(a, b, preferred_element_type=jnp.float32)


def dot_across(a, b):
    return lax.dot_general(a, b, (((1,), (1,)), ((), ())), preferred_element_type=jnp.float32)


def to_column(row):
    eye = lax.broadcasted_iota(jnp.int32, (LANES, LANES), 0) == lax.broadcasted_iota(jnp.int32, (LANES, LANES), 1)
    return jnp.concatenate(
        [
            jnp.sum(jnp.where(eye, row[:, i : i + LANES], 0.0), axis=1, keepdims=True)
            for i in range(0, row.shape[1], LANES)
        ],
        axis=0,
    )


def analysis_scratch(cells, count, near):
    f32, bf16 = jnp.float32, jnp.bfloat16
    return [
        pltpu.VMEM((near, near), f32),
        pltpu.VMEM((near, cells), f32),
        pltpu.VMEM((3 * near, count), bf16),
        pltpu.VMEM((count, near), bf16),
        pltpu.VMEM((near, 3 * near), bf16),
        pltpu.VMEM((3 * near, near), bf16),
        pltpu.VMEM((near, 3 * near), bf16),
        pltpu.VMEM((8, 3 * near, cells), bf16),
        pltpu.VMEM((7, near, cells), f32),
        pltpu.VMEM((2, cells, near), f32),
    ]


def own_products(work, y, right):
    common, crossed, y_right, y_turned = work[:4]
    side = y.shape[0]
    put_right(y_right, side, y)
    high, low = y_right[side : 2 * side], y_right[4 * side : 5 * side]
    left = jnp.concatenate([high, high, low], axis=1)
    crossed[side : 2 * side] = dot_across(left, right)
    common[side : 2 * side, side : 2 * side] = dot_across(left, jnp.concatenate([high, low, high], axis=1))


def other_products(work, sides, right):
    common, crossed, y_right, y_turned = work[:4]
    side = sides[0].shape[0]
    for slot, y in zip((0, 2), sides):
        put_right(y_right, slot * side, y)
    near = 3 * side
    high, low = y_right[0:near], y_right[near : 2 * near]
    y_turned[...] = high.T
    terms = [jnp.concatenate([v[0:side], v[2 * side :]], axis=0) for v in (high, low)]
    left = jnp.concatenate([terms[0], terms[0], terms[1]], axis=1)
    mine = dot_across(left, jnp.concatenate([high, low, high], axis=1))
    apart = dot_across(left, right)
    for i, slot in enumerate((0, 2)):
        span = slice(slot * side, (slot + 1) * side)
        common[span] = mine[i * side : (i + 1) * side]
        crossed[span] = apart[i * side : (i + 1) * side]
        common[side : 2 * side, span] = mine[i * side : (i + 1) * side, side : 2 * side].T


def weigh(width, cells, near, lower, upper, meta):
    var, obs_rows = meta[1:2], meta[2:3]
    strip_of = lax.broadcasted_iota(jnp.int32, (1, near), 1) // (near // 3) - 1
    cols = meta[3:4] + (strip_of * width).astype(jnp.float32)
    lon_gap = jnp.maximum(jnp.maximum(-cols, cols - (width - 1.0)), 0.0) / float(width)
    lat_gap = jnp.maximum(jnp.maximum(lower - obs_rows, obs_rows - upper), 0.0) / (cells // width / 4.0)
    weights = jnp.exp(-lat_gap * lat_gap - lon_gap * lon_gap) / var
    scale = jnp.sqrt(weights)
    return weights, scale, to_column(scale)


def solve_patch(dims, work, slot, spare_first, near_weights, innov):
    lats, members, chunks, rows, width, group = dims
    common, crossed, y_right, y_turned, x_left, x_right, low_left, b_right, blocks, turned = work
    count, near = y_turned.shape
    cells = crossed.shape[1]
    tile = near // 2
    tiles = range(0, near, tile)
    weights, scale, scale_col = near_weights

    left = (y_turned[...].astype(jnp.float32) * weights).astype(jnp.bfloat16)
    gram = jnp.abs(dot(left, y_right[0:near]))
    sums = jnp.sum(gram.reshape(count // 8, 8, count), axis=0)
    bound = (count - 1.0) + jnp.max(jnp.sum(sums, axis=0, keepdims=True), axis=1, keepdims=True)
    inverse = 1.0 / bound
    alpha = (count - 1.0) * inverse
    c0 = 2.25 + alpha * (-2.4375 + alpha * (1.6875 + alpha * (-0.5625 + alpha * 0.0625)))
    c1 = -2.4375 + alpha * (3.375 + alpha * (-1.6875 + alpha * 0.25))
    c2 = 1.6875 + alpha * (-1.6875 + alpha * 0.375)
    c3 = -0.5625 + alpha * 0.25
    c4 = 0.0625

    lane = lax.broadcasted_iota(jnp.int32, (tile, cells), 1)
    spare = (1 - spare_first) * (cells - 1)
    scale_row = scale * inverse

    def x_tile(i):
        return common[i : i + tile] * scale_col[i : i + tile] * scale_row

    block, b1, b2, w, b3, u, got = range(7)

    def keep(i, which, value):
        blocks[which, i : i + tile] = value
        put_right(b_right.at[which], i, value)

    for i in tiles:
        x = x_tile(i)
        x_left[i : i + tile] = left_form(x)
        put_right(x_right, i, x)
        keep(i, block, jnp.where(lane == spare, innov[i : i + tile], crossed[i : i + tile]) * scale_col[i : i + tile])
    x2 = dot(x_left[...], x_right[...])
    x3 = dot(left_form(x2), x_right[...])
    low_left[...] = left_form(c2 * (common[...] * scale_col * scale_row) + c3 * x2 + c4 * x3)

    def low_on(i, which):
        return dot(low_left[i : i + tile], b_right[which])

    def x_on(i, which):
        return dot(x_left[i : i + tile], b_right[which])

    for i in tiles:
        keep(i, b1, c1 * blocks[block, i : i + tile] + low_on(i, block))
    for i in tiles:
        keep(i, b2, c0 * blocks[block, i : i + tile] + x_on(i, b1))
    for i in tiles:
        keep(i, w, c1 * blocks[b2, i : i + tile] + low_on(i, b2))
    for i in tiles:
        keep(i, b3, c0 * blocks[b2, i : i + tile] + x_on(i, w))
    for i in tiles:
        keep(i, u, c1 * blocks[b3, i : i + tile] + low_on(i, b3))
    root_scale = jnp.sqrt(alpha)
    for i in tiles:
        z = c0 * blocks[b3, i : i + tile] + x_on(i, u)
        first = blocks[b1, i : i + tile]
        value = 1.5 * first - 0.5 * (
            z + alpha * (blocks[u, i : i + tile] + c0 * (blocks[w, i : i + tile] + c0 * first))
        )
        put_right(b_right.at[got], i, value)
        turned[slot, :, i : i + tile] = (value * (scale_col[i : i + tile] * (root_scale * inverse))).T
    base = c0 * (1.5 - 0.5 * alpha * c0 * c0)
    change = None
    for i in tiles:
        full = base * blocks[block, i : i + tile] + x_on(i, got)
        drive = jnp.where(spare_first == 1, full[:, 0:1], full[:, cells - 1 : cells])
        part = jnp.sum((full * drive).reshape(tile // 8, 8, cells), axis=0)
        change = part if change is None else change + part
    return jnp.sum(change, axis=0, keepdims=True) * inverse, root_scale * base


def forecast(load, lats, group):
    fields = [load(l) for l in range(lats)]
    lane = lax.broadcasted_iota(jnp.int32, fields[0].shape, 1)
    first, last = lane < group, lane >= LANES - group
    count = fields[0].shape[0]
    zero = jnp.zeros_like(fields[0])
    for _ in range(STEPS):
        new = []
        for l in range(lats):
            c = fields[l]
            above = fields[l - 1] if l > 0 else zero
            below = fields[l + 1] if l + 1 < lats else zero
            north = pltpu.roll(jnp.where(last, above, c), group, 1)
            south = pltpu.roll(jnp.where(first, below, c), LANES - group, 1)
            east = pltpu.roll(c, count - 1, 0)
            west = pltpu.roll(c, 1, 0)
            new.append(
                c
                + lat_coeff * (north + south - 2.0 * c)
                + lon_coeff * (east + west - 2.0 * c)
                - advect_coeff * c * (east - west)
            )
        fields = new
    return fields


def swap_blocks(parts, group):
    per = len(parts)
    lane_block = lax.broadcasted_iota(jnp.int32, parts[0].shape, 1) // group
    outs = []
    for i in range(per):
        out = None
        for j in range(per):
            shift = (group * (j - i)) % LANES
            piece = pltpu.roll(parts[j], shift, 1) if shift else parts[j]
            out = piece if out is None else jnp.where(lane_block == j, piece, out)
        outs.append(out)
    return outs


def pick(onehot, values):
    total, rest = None, values
    for _ in range(3):
        term = rest.astype(jnp.bfloat16)
        part = jnp.dot(onehot, term, preferred_element_type=jnp.float32)
        total = part if total is None else total + part
        rest = rest - term.astype(jnp.float32)
    return total


def engine_kernel(
    dims, x_hbm, cell_ref, value_ref, var_ref, rows_ref, z_hbm,
    x_buf, s_buf, ra, f_buf, r_buf, xt, yt, meta, obs_out, obs_in, t_buf, at_buf,
    x_sem, a_send, a_recv, b_send, b_recv, o_send, o_recv, m_send, m_recv, y_send, y_recv, z_send, z_recv, own_sem, *work,
):
    lats, members, chunks, rows, width, group = dims
    cols = width * members
    cells = lats * rows * width
    strips = lats * members
    edge = STEPS
    m, lat = lax.axis_index("member"), lax.axis_index("lat")
    own = block_at(lat, lats)
    strip = strip_at(m, lat, lats, members)
    neighbours = [(slot, home_of((strip + side) % strips, lats, members)) for side, slot in ((1, 0), (strips - 1, 2))]

    def remote(src, dst, send, recv, to):
        return pltpu.make_async_remote_copy(
            src_ref=src, dst_ref=dst, send_sem=send, recv_sem=recv, device_id=to, device_id_type=MESH
        )

    reads = [
        pltpu.make_async_copy(x_hbm.at[pl.ds(kc * group, group)], x_buf.at[kc], x_sem.at[kc]) for kc in range(chunks)
    ]
    barrier, partners = greet_all(lats, members)
    for read in reads:
        read.start()

    obs_out[...] = jnp.zeros_like(obs_out)
    obs_out[0:1, :] = cell_ref[...].astype(jnp.float32)
    obs_out[1:2, :] = value_ref[...]
    obs_out[2:3, :] = var_ref[...]
    obs_out[3:4, 0 : rows_ref.shape[1]] = rows_ref[...].astype(jnp.float32)

    target_m, target_l = home_of(m * lats + lat, lats, members)
    away = jnp.logical_or(target_m != m, target_l != lat)
    obs_copy = remote(obs_out, obs_in, o_send, o_recv, (target_m, target_l))

    a_copies = []
    for kc in range(chunks):
        reads[kc].wait()
        whole = jnp.concatenate([x_buf[kc, :, r, :] for r in range(rows)], axis=0)
        turned = whole.T
        lon = turned.shape[0]
        for b in range(lats):
            s_buf[kc, b, 0:cols] = turned[b * cols : (b + 1) * cols]
            east, west = ((b + 1) * cols) % lon, (b * cols - edge) % lon
            s_buf[kc, b, cols : cols + edge] = turned[east : east + edge]
            s_buf[kc, b, cols + edge : cols + 2 * edge] = turned[west : west + edge]
        if kc == 0:
            pl.semaphore_wait(barrier, partners)

            @pl.when(away)
            def _():
                obs_copy.start()

            @pl.when(jnp.logical_not(away))
            def _():
                obs_in[...] = obs_out[...]

        run = []
        for d in range(1, lats):
            to = (lat + d) % lats
            copy = remote(
                s_buf.at[kc, block_at(to, lats)], ra.at[kc, lat], a_send.at[kc, d], a_recv.at[kc, d], (m, to)
            )
            copy.start()
            run.append(copy)
        a_copies.append(run)

    @pl.when(away)
    def _():
        obs_copy.wait_recv()

    cell_lane = obs_in[0:1, :]
    obs_row = jnp.floor(cell_lane * (1.0 / width))
    meta[1, 0:1, :] = obs_in[1:2, :]
    meta[1, 1:2, :] = obs_in[2:3, :]
    meta[1, 2:3, :] = obs_row
    meta[1, 3:4, :] = cell_lane - width * obs_row
    meta[1, 4:5, :] = obs_in[3:4, :]
    meta[1, 5:8, :] = jnp.zeros((3, cell_lane.shape[1]), jnp.float32)
    late = []
    for slot, to in neighbours:
        copy = remote(meta.at[1], meta.at[slot], m_send.at[slot], m_recv.at[slot], to)
        copy.start()
        late.append(copy)
    onehot = (
        to_column(cell_lane)
        == lax.broadcasted_iota(jnp.int32, (cell_lane.shape[1], cells), 1).astype(jnp.float32)
    ).astype(jnp.bfloat16)

    b_copies = []

    def arrive(kc):
        for copy in b_copies[kc]:
            copy.wait_recv()
        parts = [r_buf[j, kc].reshape(lats * width, LANES) for j in range(members)]
        for r, out in enumerate(swap_blocks(parts, group)):
            for l in range(lats):
                xt[kc, (l * rows + r) * width : (l * rows + r + 1) * width] = out[l * width : (l + 1) * width]
        yt[1, kc] = pick(onehot, xt[kc])
        for slot, to in neighbours:
            copy = remote(yt.at[1, kc], yt.at[slot, kc], y_send.at[slot, kc], y_recv.at[slot, kc], to)
            copy.start()
            late.append(copy)

    for kc in range(chunks):
        ra[kc, lat] = s_buf[kc, own]
        for copy in a_copies[kc]:
            copy.wait_recv()
        fields = forecast(lambda l, kc=kc: ra[kc, l], lats, group)
        for l in range(lats):
            for q in range(members):
                f_buf[kc, q, l] = fields[l][q * width : (q + 1) * width]
        run = []
        for d in range(1, members):
            to = (m + d) % members
            copy = remote(
                f_buf.at[kc, member_of(own, to, members)], r_buf.at[m, kc], b_send.at[kc, d], b_recv.at[kc, d], (to, lat)
            )
            copy.start()
            run.append(copy)
        b_copies.append(run)
        r_buf[m, kc] = f_buf[kc, member_of(own, m, members)]
        if kc:
            arrive(kc - 1)
    arrive(chunks - 1)

    states = jnp.concatenate([xt[kc] for kc in range(chunks)], axis=1)
    mean = jnp.sum(states, axis=1, keepdims=True) * (1.0 / states.shape[1])
    at = states - mean
    at_buf[...] = at
    ah, al = split(at)
    right = jnp.concatenate([ah, al, ah], axis=1)

    def observed(slot):
        raw = jnp.concatenate([yt[slot, kc] for kc in range(chunks)], axis=1)
        centre = jnp.sum(raw, axis=1, keepdims=True) * (1.0 / raw.shape[1])
        return raw - centre, centre

    for copy in late[:2]:
        copy.wait_recv()
    all_meta = jnp.concatenate([meta[slot] for slot in range(3)], axis=1)
    nobs = cell_lane.shape[1]
    sure = lats // 4
    rest = lats - sure
    last = 1 - lat // (lats // 2)
    lasts = last.astype(jnp.float32)
    first_len = all_meta[4:5, nobs : nobs + 1]
    second_len = all_meta[4:5, nobs + 1 : nobs + 2]
    spans = []
    for which in (lasts, 1.0 - lasts):
        lower = which * first_len
        spans.append((lower, lower + (first_len + which * (second_len - first_len)) - 1.0))
    near_weights = [weigh(width, cells, 3 * nobs, *span, all_meta) for span in spans]
    own_spread, own_mean = observed(1)
    own_products(work, own_spread, right)
    for copy in late[2:]:
        copy.wait_recv()
    before, before_mean = observed(0)
    after, after_mean = observed(2)
    other_products(work, (before, after), right)
    innov = to_column(all_meta[0:1]) - jnp.concatenate([before_mean, own_mean, after_mean], axis=0)
    y_right, turned = work[2], work[9]

    def finish(tile, tiles, pick_cells, weights, change, factor):
        begin = tile * (rows * width)
        span = pl.ds(pl.multiple_of(begin, rows * width), tiles * rows * width)
        out = pick_cells(mean) + change + factor * at_buf[span, :] + dot(left_form(weights), y_right[...])
        for kc in range(chunks):
            lanes = out[:, kc * LANES : (kc + 1) * LANES]
            parts = [
                jnp.concatenate(
                    [lanes[(l * rows + r) * width : (l * rows + r + 1) * width] for l in range(tiles)], axis=0
                )
                for r in range(rows)
            ]
            for j, piece in enumerate(swap_blocks(parts, group)):
                for l in range(tiles):
                    t_buf[j, tile + l, kc] = piece[l * width : (l + 1) * width]

    def give(to):
        copy = remote(t_buf.at[to[0], to[1]], z_hbm.at[strip], z_send.at[len(z_copies)], z_recv.at[strip], to)
        copy.start()
        z_copies.append(copy)

    z_copies = []
    cut, tail = sure * rows * width, rest * rows * width
    early = last * rest
    change, factor = solve_patch(dims, work, 0, last, near_weights[0], innov)
    change_col = to_column(change)

    def far(column):
        return jnp.where(last == 1, column[tail:], column[:cut])

    def near(column):
        return jnp.where(last == 1, column[:tail], column[cut:])

    finish(early, sure, far, far(turned[0]), far(change_col), factor)
    for l in range(sure):
        for dm in range(members):
            give(((m + dm) % members, early + l))

    change2, factor2 = solve_patch(dims, work, 1, 1 - last, near_weights[1], innov)
    cell_row = (lax.broadcasted_iota(jnp.int32, (cells, 1), 0) // width).astype(jnp.float32)
    inside = near(jnp.logical_and(cell_row >= spans[0][0], cell_row <= spans[0][1]).astype(jnp.float32)) > 0.5
    base = (1 - last) * sure
    finish(
        base,
        rest,
        near,
        jnp.where(inside, near(turned[0]), near(turned[1])),
        jnp.where(inside, near(change_col), near(to_column(change2))),
        jnp.where(inside, factor, factor2),
    )
    for j in range(rest - 1):
        for dm in range(members):
            give(((m + dm) % members, base + (lat - base + 1 + j) % rest))
    for dm in range(1, members):
        give(((m + dm) % members, lat))
    kept = pltpu.make_async_copy(t_buf.at[m, lat], z_hbm.at[strip], own_sem)
    kept.start()

    for run in a_copies + b_copies + [late]:
        for copy in run:
            copy.wait_send()

    @pl.when(away)
    def _():
        obs_copy.wait_send()

    kept.wait()
    for copy in z_copies:
        copy.wait_send()
    for d in range(1, strips):
        other = (strip + d) % strips
        remote(
            t_buf.at[0, 0], z_hbm.at[other], z_send.at[0], z_recv.at[other], ((m + 1) % members, lat)
        ).wait_recv()


def engine(ensemble, obs_cell, obs_value, obs_var, patch_rows, dims):
    lats, members, chunks, rows, width, group = dims
    cells = lats * rows * width
    nobs = obs_cell.shape[1]
    strips = lats * members
    dma, f32 = pltpu.SemaphoreType.DMA, jnp.float32
    vmem, anywhere = pl.BlockSpec(memory_space=pltpu.VMEM), pl.BlockSpec(memory_space=pl.ANY)
    block = (chunks, lats, members * width + 2 * STEPS, LANES)
    return pl.pallas_call(
        functools.partial(engine_kernel, dims),
        out_shape=jax.ShapeDtypeStruct((strips, chunks, width, LANES), f32),
        in_specs=[anywhere, vmem, vmem, vmem, vmem],
        out_specs=anywhere,
        scratch_shapes=[
            pltpu.VMEM((chunks, group, rows, strips * width), f32),
            pltpu.VMEM(block, f32),
            pltpu.VMEM(block, f32),
            pltpu.VMEM((chunks, members, lats, width, LANES), f32),
            pltpu.VMEM((members, chunks, lats, width, LANES), f32),
            pltpu.VMEM((chunks, cells, LANES), f32),
            pltpu.VMEM((3, chunks, nobs, LANES), f32),
            pltpu.VMEM((3, 8, nobs), f32),
            pltpu.VMEM((8, nobs), f32),
            pltpu.VMEM((8, nobs), f32),
            pltpu.VMEM((members, lats, chunks, width, LANES), f32),
            pltpu.VMEM((cells, members * chunks * group), f32),
            dma((chunks,)),
            dma((chunks, lats)),
            dma((chunks, lats)),
            dma((chunks, members)),
            dma((chunks, members)),
            dma,
            dma,
            dma((3,)),
            dma((3,)),
            dma((3, chunks)),
            dma((3, chunks)),
            dma((strips,)),
            dma((strips,)),
            dma,
        ]
        + analysis_scratch(cells, members * chunks * group, 3 * nobs),
        compiler_params=pltpu.CompilerParams(
            collective_id=0, has_side_effects=True, vmem_limit_bytes=56 * 1024 * 1024
        ),
        name="engine",
    )(ensemble, obs_cell, obs_value, obs_var, patch_rows)


def settle_kernel(dims, z_hbm, out_hbm, z_buf, out_buf, in_sem, out_sem):
    lats, members, chunks, rows, width, group = dims
    reads = [pltpu.make_async_copy(z_hbm.at[:, kc], z_buf.at[kc], in_sem.at[kc]) for kc in range(chunks)]
    for read in reads:
        read.start()
    writes = []
    for kc in range(chunks):
        reads[kc].wait()
        turned = z_buf[kc].reshape(lats * members * width, LANES).T
        for r in range(rows):
            out_buf[kc, :, r, :] = turned[r * group : (r + 1) * group]
        write = pltpu.make_async_copy(out_buf.at[kc], out_hbm.at[pl.ds(kc * group, group)], out_sem.at[kc])
        write.start()
        writes.append(write)
    for write in writes:
        write.wait()


def settle(pieces, dims):
    lats, members, chunks, rows, width, group = dims
    strips = lats * members
    f32, anywhere = jnp.float32, pl.BlockSpec(memory_space=pl.ANY)
    return pl.pallas_call(
        functools.partial(settle_kernel, dims),
        out_shape=jax.ShapeDtypeStruct((chunks * group, rows, strips * width), f32),
        in_specs=[anywhere],
        out_specs=anywhere,
        scratch_shapes=[
            pltpu.VMEM((chunks, strips, width, LANES), f32),
            pltpu.VMEM((chunks, group, rows, strips * width), f32),
            pltpu.SemaphoreType.DMA((chunks,)),
            pltpu.SemaphoreType.DMA((chunks,)),
        ],
        name="settle",
    )(pieces)


def kernel_device(dims, ensemble, obs_cell, obs_value, obs_var, patch_rows):
    return settle(engine(ensemble, obs_cell, obs_value, obs_var, patch_rows, dims), dims)


def kernel_dims(mesh, ensemble, obs_cell, patch_rows):
    lats, members = mesh.shape["lat"], mesh.shape["member"]
    total, lat_all, lon = ensemble.shape
    own, rows = total // members, lat_all // lats
    width = lon // (lats * members)
    if LANES % rows:
        return None
    group = LANES // rows
    fits = (
        own % group == 0
        and (members * (own // group)) % rows == 0
        and width == 8
        and lats % 4 == 0
        and members % 2 == 0
        and obs_cell.shape[1] % LANES == 0
        and patch_rows.shape[1] == 2
    )
    return (lats, members, own // group, rows, width, group) if fits else None


def solution(mesh):
    specs = (P("member", "lat", None),) + (P(("member", "lat"), None),) * 4

    def run(ensemble, obs_cell, obs_value, obs_var, patch_rows):
        dims = kernel_dims(mesh, ensemble, obs_cell, patch_rows)
        body = general_device if dims is None else functools.partial(kernel_device, dims)
        mapped = jax.shard_map(
            body, mesh=mesh, in_specs=specs, out_specs=P("member", "lat", None), check_vma=False
        )
        return mapped(ensemble, obs_cell, obs_value, obs_var, patch_rows)

    return run
```
